32 devices in a mesh: seq: 4 (over x, core), head: 8 (over z, y).
Axes of the slice: x: 2, y: 2, z: 4, core: 2. Of those that a mesh axis runs over, the one named last changes fastest.
Arguments:
- residual_in: float32 [1, 4096, 1536], P(None, ('seq', 'head')), may hold values from -6 to 6
- norm_gain: float32 [1536], replicated, may hold values from 0.5 to 1.5
- gate_weight: float32 [3072, 1536], P('head'), may hold values from -0.15625 to 0.15625
- inner_weight: float32 [3072, 1536], P('head'), may hold values from -0.15625 to 0.15625
- bc_weight: float32 [1536, 256], replicated, may hold values from -0.15625 to 0.15625
- step_weight: float32 [48, 1536], P('head'), may hold values from -0.15625 to 0.15625
- conv_inner_weight: float32 [4, 3072], P(None, 'head'), may hold values from -3 to 3
- conv_inner_bias: float32 [3072], P('head'), may hold values from -0.5 to 0.5
- conv_bc_weight: float32 [4, 256], replicated, may hold values from -3 to 3
- conv_bc_bias: float32 [256], replicated, may hold values from -0.5 to 0.5
- step_bias: float32 [48], P('head'), may hold values from -4 to 0
- decay_log: float32 [48], P('head'), may hold values from -7 to -1
- skip_gain: float32 [48], P('head'), may hold values from 0.5 to 2
- gated_gain: float32 [3072], P('head'), may hold values from 0.5 to 1.5
- out_weight: float32 [3072, 1536], P('head'), may hold values from -0.109375 to 0.109375
- cotangent: float32 [1, 4096, 1536], P(None, ('seq', 'head')), may hold values from -6 to 6
Outputs:
- result: float32 [1, 4096, 1536], P(None, ('seq', 'head'))
- residual_grad: float32 [1, 4096, 1536], P(None, ('seq', 'head'))
- norm_gain_grad: float32 [1536], replicated
- gate_weight_grad: float32 [3072, 1536], P('head')
- inner_weight_grad: float32 [3072, 1536], P('head')
- bc_weight_grad: float32 [1536, 256], replicated
- step_weight_grad: float32 [48, 1536], P('head')
- conv_inner_weight_grad: float32 [4, 3072], P(None, 'head')
- conv_inner_bias_grad: float32 [3072], P('head')
- conv_bc_weight_grad: float32 [4, 256], replicated
- conv_bc_bias_grad: float32 [256], replicated
- step_bias_grad: float32 [48], P('head')
- decay_log_grad: float32 [48], P('head')
- skip_gain_grad: float32 [48], P('head')
- gated_gain_grad: float32 [3072], P('head')
- out_weight_grad: float32 [3072, 1536], P('head')
The draws below stay inside these ranges and needn't reach their ends.
All inputs are finite; a program needn't handle non-finite values.
Results may differ from the reference program's by a relative error of at most 0.0003.
Values sent between devices are 32-bit elements; how exact they have to be, the bound alone decides.
A program may use at most 192 MiB of HBM per device.

```python
import jax
import jax.numpy as jnp
from jax import lax

D = 1536
NHEADS = 48
HEADDIM = 64
NSTATE = 128
WIDTH = 4
BLOCK = 256
LEN = 4096
SEQS = 1
DI = 3072


def levels(key, dims, split, least, largest):
    gain = 1.0
    for dim, parts in split:
        heights = jax.random.uniform(jax.random.fold_in(jax.random.fold_in(key, 6), dim), (parts,), jnp.float32, least / len(split), largest / len(split))
        gain = gain * jnp.repeat(jnp.exp(heights), dims[dim] // parts).reshape((-1,) + (1,) * (len(dims) - 1 - dim))
    return gain


def normal_values(stream_key, dims, scale, limit, split=(), kind=jnp.bfloat16):
    loudness = levels(stream_key, dims, split, -0.22, 0.18) if split else 1.0
    array = jax.random.normal(stream_key, dims, jnp.float32) * scale * loudness
    return jnp.minimum(jnp.maximum(array, -limit), limit).astype(kind)


def setup_inputs(seed: int = 0) -> dict:
    streams_of = jax.random.split(jax.random.key(seed), 17)
    return {
        "residual_in": normal_values(streams_of[0], (SEQS, LEN, D), 1.0, 6.0, ((1, 32),), jnp.float32),
        "norm_gain": jnp.clip(1.0 + 0.1 * jax.random.normal(streams_of[1], (D,), jnp.float32), 0.5, 1.5),
        "gate_weight": normal_values(streams_of[2], (DI, D), D ** -0.5, 0.15625, ((0, 8),), jnp.float32),
        "inner_weight": normal_values(streams_of[3], (DI, D), D ** -0.5, 0.15625, ((0, 8),), jnp.float32),
        "bc_weight": normal_values(streams_of[4], (D, 2 * NSTATE), D ** -0.5, 0.15625, (), jnp.float32),
        "step_weight": normal_values(streams_of[5], (NHEADS, D), D ** -0.5, 0.15625, ((0, 8),), jnp.float32),
        "conv_inner_weight": normal_values(streams_of[6], (WIDTH, DI), WIDTH ** -0.5, 3.0, ((1, 8),), jnp.float32),
        "conv_inner_bias": jnp.clip(jax.random.uniform(streams_of[7], (DI,), jnp.float32, -0.5, 0.5) * levels(streams_of[7], (DI,), ((0, 8),), -0.4, 0.0), -0.5, 0.5),
        "conv_bc_weight": normal_values(streams_of[8], (WIDTH, 2 * NSTATE), WIDTH ** -0.5, 3.0, (), jnp.float32),
        "conv_bc_bias": jnp.clip(jax.random.uniform(streams_of[9], (2 * NSTATE,), jnp.float32, -0.5, 0.5), -0.5, 0.5),
        "step_bias": jnp.clip(-4.0 + 4.0 * jax.random.uniform(streams_of[10], (NHEADS,), jnp.float32) ** levels(streams_of[10], (NHEADS,), ((0, 8),), -0.2, 0.2), -4.0, 0.0),
        "decay_log": jnp.clip(-7.0 + 6.0 * jax.random.uniform(streams_of[11], (NHEADS,), jnp.float32) ** levels(streams_of[11], (NHEADS,), ((0, 8),), -0.2, 0.2), -7.0, -1.0),
        "skip_gain": jnp.clip(0.5 + 1.5 * jax.random.uniform(streams_of[12], (NHEADS,), jnp.float32) ** levels(streams_of[12], (NHEADS,), ((0, 8),), -0.2, 0.2), 0.5, 2.0),
        "gated_gain": jnp.clip(1.0 + 0.1 * jax.random.normal(streams_of[13], (DI,), jnp.float32), 0.5, 1.5),
        "out_weight": normal_values(streams_of[14], (DI, D), DI ** -0.5, 0.109375, ((0, 8),), jnp.float32),
        "cotangent": normal_values(streams_of[15], (SEQS, LEN, D), 1.0, 6.0, ((1, 32),), jnp.float32),
    }


@jax.custom_vjp
def low(v):
    return lax.optimization_barrier(v.astype(jnp.bfloat16)).astype(jnp.float32)

@jax.custom_vjp
def low_back(v):
    return v

def low_keep(v):
    return (low(v), None)

def low_pass(kept, grad):
    return (grad,)

def back_keep(v):
    return (v, None)

def back_low(kept, grad):
    return (low(grad),)
low.defvjp(low_keep, low_pass)
low_back.defvjp(back_keep, back_low)
EPSILON = 1e-05
HIGH = lax.Precision.HIGHEST

def product(left_side, right_side):
    return jnp.dot(left_side, right_side, precision=HIGH, preferred_element_type=jnp.float32)

def causal_conv(before, kernel, offset_bias):
    length = before.shape[0]
    padded = jnp.concatenate([jnp.zeros((WIDTH - 1, before.shape[1]), jnp.float32), before], 0)
    total = jnp.zeros_like(before) + offset_bias
    for offset in range(WIDTH):
        total = total + kernel[offset] * padded[offset:offset + length]
    return total

def mamba_layer(rows, norm_gain, gate_weight, inner_weight, bc_weight, step_weight, conv_inner_weight, conv_inner_bias, conv_bc_weight, conv_bc_bias, step_bias, decay_log, skip_gain, gated_gain, out_weight):
    length = rows.shape[0]
    row_scale = lax.rsqrt(lax.optimization_barrier(jnp.mean(rows * rows, axis=1, keepdims=True)) + EPSILON)
    normed = rows * row_scale * norm_gain
    gate_pre = product(normed, gate_weight.T)
    inner_pre = product(normed, inner_weight.T)
    bc_pre = product(normed, bc_weight)
    step_pre = product(normed, step_weight.T)
    inner_x = jax.nn.silu(causal_conv(inner_pre, conv_inner_weight, conv_inner_bias))
    bc_act = jax.nn.silu(causal_conv(bc_pre, conv_bc_weight, conv_bc_bias))
    step_size = jax.nn.softplus(step_pre + step_bias)
    rate_vec = -jnp.exp(decay_log)
    blocks_all = length // BLOCK
    causal = jnp.tril(jnp.ones((BLOCK, BLOCK), bool))[:, :, None]

    def block_step(state, pieces):
        inner_block, step_block, write_block, read_block = pieces
        cumulative = jnp.cumsum(step_block * rate_vec, axis=0)
        spread = cumulative[:, None, :] - cumulative[None, :, :]
        decay = jnp.where(causal, jnp.exp(jnp.where(causal, spread, 0.0)), 0.0)
        scores = product(read_block, write_block.T)
        weights = decay * scores[:, :, None] * step_block[None, :, :]
        intra = jnp.einsum('tsh,shp->thp', weights, inner_block, precision=HIGH)
        carried = jnp.einsum('tn,hpn->thp', read_block, state, precision=HIGH) * jnp.exp(cumulative)[:, :, None]
        tails = jnp.exp(cumulative[-1][None, :] - cumulative) * step_block
        fresh = jnp.einsum('sh,shp,sn->hpn', tails, inner_block, write_block, precision=HIGH)
        new_state = jnp.exp(cumulative[-1])[:, None, None] * state + fresh
        return (new_state, intra + carried)
    pieces = (inner_x.reshape(blocks_all, BLOCK, NHEADS, HEADDIM), step_size.reshape(blocks_all, BLOCK, NHEADS), bc_act[:, :NSTATE].reshape(blocks_all, BLOCK, NSTATE), bc_act[:, NSTATE:].reshape(blocks_all, BLOCK, NSTATE))
    start = jnp.zeros((NHEADS, HEADDIM, NSTATE), jnp.float32)
    final_state, outputs = lax.scan(jax.checkpoint(block_step), start, pieces)
    mixed = outputs.reshape(length, NHEADS, HEADDIM) + skip_gain[:, None] * inner_x.reshape(length, NHEADS, HEADDIM)
    gated = mixed.reshape(length, DI) * jax.nn.silu(gate_pre)
    gate_scale = lax.rsqrt(lax.optimization_barrier(jnp.mean(gated * gated, axis=1, keepdims=True)) + EPSILON)
    return rows + product(gated * gate_scale * gated_gain, out_weight)

def reference(residual_in, norm_gain, gate_weight, inner_weight, bc_weight, step_weight, conv_inner_weight, conv_inner_bias, conv_bc_weight, conv_bc_bias, step_bias, decay_log, skip_gain, gated_gain, out_weight, cotangent):
    weights_all = (norm_gain, gate_weight, inner_weight, bc_weight, step_weight, conv_inner_weight, conv_inner_bias, conv_bc_weight, conv_bc_bias, step_bias, decay_log, skip_gain, gated_gain, out_weight)

    def one_sequence(totals, item):
        rows, grad_rows = item
        output, pull = jax.vjp(mamba_layer, rows, *weights_all)
        grads = pull(grad_rows)
        summed = tuple((running + fresh_grad for running, fresh_grad in zip(totals, grads[1:])))
        return (summed, (output, grads[0]))
    zeros_all = tuple((jnp.zeros_like(weight_one) for weight_one in weights_all))
    totals, (outputs, input_grads) = lax.scan(one_sequence, zeros_all, (residual_in, cotangent))
    return (outputs, input_grads) + totals
```

```python
import functools

import jax
import jax.numpy as jnp
from jax import lax
from jax.experimental import pallas as pl
from jax.experimental.pallas import tpu as pltpu
from jax.sharding import PartitionSpec as P

HEADDIM = 64
NSTATE = 128
WIDTH = 4
BLOCK = 256
EPSILON = 1e-05
EXACT = lax.Precision.HIGHEST
MESH = pl.DeviceIdType.MESH
F32 = jnp.float32
BF16 = jnp.bfloat16
VMEM_LIMIT = 66000000


def dot3(left, right, left_dim, right_dim):
    dims = (((left_dim,), (right_dim,)), ((), ()))
    one = functools.partial(lax.dot_general, dimension_numbers=dims, preferred_element_type=F32)
    return one(left[0], right[0]) + (one(left[0], right[1]) + one(left[1], right[0]))


def remote(source, target, send_sem, recv_sem, seq, head):
    return pltpu.make_async_remote_copy(
        src_ref=source,
        dst_ref=target,
        send_sem=send_sem,
        recv_sem=recv_sem,
        device_id=(seq, head),
        device_id_type=MESH,
    )


def greet(seq, head, seqs, heads):
    barrier = pltpu.get_barrier_semaphore()
    for j in range(1, seqs):
        pl.semaphore_signal(
            barrier, inc=1, device_id=(lax.rem(seq + j, seqs), head), device_id_type=MESH
        )
    for j in range(1, heads):
        pl.semaphore_signal(
            barrier, inc=1, device_id=(seq, lax.rem(head + j, heads)), device_id_type=MESH
        )
    pl.semaphore_wait(barrier, seqs + heads - 2)


def inner_count(heads):
    return 2 if heads <= 8 else 4


def tail_kernel(dims, *refs):
    seqs, heads, chunk, chans, pad = dims
    (
        gp_hi, gp_lo, hat_hi, hat_lo, w_hi, w_lo, small_in, resid, cot, gain,
        resid_grad, gate_out, inner_out, bc_out, small_out,
        gph, gpl, hth, htl, wh, wl, grads, y_in, z_in, joined, keep, core_in, x_in,
        bc_part, bc_seq, bc_head, bc_full, small_all, small_head,
        load_sem, y_send, y_recv, z_send, z_recv, c_send, c_recv, x_send, x_recv,
        f_send, f_recv, o_sem, ba_s, ba_r, bb_s, bb_r, bc_s, bc_r, bd_s, bd_r,
        sa_s, sa_r, sb_s, sb_r,
    ) = refs
    width = gain.shape[1]
    ins = inner_count(heads)
    outs = heads // ins
    rounds = (seqs // 2).bit_length() - 1
    half = chans // 2
    span = 2 * chans
    seq, head = lax.axis_index("seq"), lax.axis_index("head")
    at_out, at_in = head // ins, lax.rem(head, ins)
    side = lax.rem(seq, 2)
    partner = seq + 1 - 2 * side

    loads = [
        pltpu.make_async_copy(a, b, load_sem.at[n])
        for n, (a, b) in enumerate(
            ((gp_hi, gph), (w_hi, wh), (gp_lo, gpl), (w_lo, wl), (hat_hi, hth), (hat_lo, htl))
        )
    ]
    for load in loads:
        load.start()
    mine = pl.ds(pl.multiple_of(side * half, 8), half)
    theirs = pl.ds(pl.multiple_of((1 - side) * half, 8), half)
    greet(seq, head, seqs, heads)

    core = [None] * 2
    for load in loads[:4]:
        load.wait()

    upper = at_out // (outs // 2)
    mirrored = at_out + upper * (outs - 1 - 2 * at_out)

    def target(step):
        last = (step + 1) // outs
        far = outs - 1 - step
        far = far - (mirrored - far + outs) // outs
        far = far + upper * (outs - 1 - 2 * far)
        return far + last * (at_out - far)

    def chunk_grad(step, inside):
        where = target(step) * ins + inside
        rows = pl.ds(pl.multiple_of(where * chunk, 8), chunk)
        grads[where] = dot3((gph[rows, :], gpl[rows, :]), (wh[...], wl[...]), 1, 0)
        return where

    def y_copy(step, j):
        to = lax.rem(at_in + 1 + j, ins)
        where = target(step) * ins + to
        slot = target(step) * (ins - 1) + j
        return remote(
            grads.at[where],
            y_in.at[slot],
            y_send.at[slot],
            y_recv.at[slot],
            seq,
            at_out * ins + to,
        )

    @pl.loop(0, outs)
    def _(step):
        for j in range(ins - 1):
            chunk_grad(step, lax.rem(at_in + 1 + j, ins))
            y_copy(step, j).start()

    x_copies = {}

    def x_start(n, source, turn):
        far = seq + (2 << turn) - 2 * (2 << turn) * lax.rem(seq // (2 << turn), 2)
        x_copies[n, turn] = remote(
            source, x_in.at[n, turn], x_send.at[n, turn], x_recv.at[n, turn], far, head
        )
        x_copies[n, turn].start()

    def after_core(n):
        core[n].wait()
        keep[n] = keep[n] + core_in[n]
        x_start(n, keep.at[n], 0)

    finals = {}
    puts = {}

    def after_x(n, result):
        now, new = keep, core_in
        for turn in range(rounds):
            x_copies[n, turn].wait()
            new[n] = now[n] + x_in[n, turn]
            now, new = new, now
            if turn + 1 < rounds:
                x_start(n, now.at[n], turn + 1)
        puts[n] = pltpu.make_async_copy(now.at[n], result.at[mine], o_sem.at[n])
        puts[n].start()
        finals[n] = remote(
            now.at[n], result.at[mine], f_send.at[n], f_recv.at[n], partner, head
        )
        finals[n].start()

    for load in loads[4:]:
        load.wait()
    joined[span:, :] = dot3(
        (gph[:, span:], gpl[:, span:]), (hth[...], htl[...]), 0, 0
    )
    gain_row = gain[...]
    pieces, _, lanes = bc_part.shape
    across = width // lanes

    def w_rows(lo, hi):
        return wh[lo:hi, :].astype(F32) + wl[lo:hi, :].astype(F32)

    gain_part = jnp.sum(joined[span:, :] * w_rows(span, pad), axis=0, keepdims=True)
    for row in range(pieces // across):
        for col in range(across):
            lane = slice(col * lanes, (col + 1) * lanes)
            block = joined[span + row * 8 : span + row * 8 + 8, lane] * gain_row[:, lane]
            bc_part[row * across + col] = block
    ba = []
    for j in range(1, seqs):
        to = lax.rem(seq + j, seqs)
        ba.append(
            remote(
                bc_part.at[pl.ds(to * heads, heads)],
                bc_seq.at[j - 1],
                ba_s.at[j - 1],
                ba_r.at[j - 1],
                to,
                head,
            )
        )
        ba[-1].start()

    @pl.loop(0, outs)
    def _(step):
        chunk_grad(step, at_in)

    def weight_rows(n):
        lo = n * chans
        if chans % 128 == 0:
            joined[lo : lo + chans, :] = dot3(
                (gph[:, lo : lo + chans], gpl[:, lo : lo + chans]), (hth[...], htl[...]), 0, 0
            )
        elif n == 0:
            joined[:span, :] = dot3((gph[:, :span], gpl[:, :span]), (hth[...], htl[...]), 0, 0)
        part = jnp.sum(joined[lo : lo + chans, :] * w_rows(lo, lo + chans), 0, keepdims=True)
        joined[lo : lo + chans, :] = joined[lo : lo + chans, :] * gain_row
        keep[n] = joined[pl.ds(pl.multiple_of(lo + side * half, 8), half), :]
        core[n] = remote(
            joined.at[pl.ds(pl.multiple_of(lo + (1 - side) * half, 8), half)],
            core_in.at[n],
            c_send.at[n],
            c_recv.at[n],
            partner,
            head,
        )
        core[n].start()
        return part

    def z_copy(where, step, up):
        goal = target(step)
        return remote(
            grads.at[where],
            z_in.at[goal + (1 if up else 0)],
            z_send.at[step],
            z_recv.at[goal + (1 if up else 0)],
            seq,
            (at_out + (1 if up else -1)) * ins + at_in,
        )

    def z_wait(slot):
        remote(
            grads.at[0], z_in.at[slot], z_send.at[0], z_recv.at[slot], partner, head
        ).wait_recv()

    def reduce_step(step):
        goal = target(step)
        where = goal * ins + at_in
        for j in range(ins - 1):
            y_copy(step, j).wait_recv()
            grads[where] = grads[where] + y_in[goal * (ins - 1) + j]
        if step == outs - 1:

            @pl.when(at_out > 0)
            def _():
                z_wait(goal + 1)
                grads[where] = grads[where] + z_in[goal + 1]

            @pl.when(at_out < outs - 1)
            def _():
                z_wait(goal)
                grads[where] = grads[where] + z_in[goal]

            return

        @pl.when(goal > at_out)
        def _():
            @pl.when(at_out > 0)
            def _():
                z_wait(goal + 1)
                grads[where] = grads[where] + z_in[goal + 1]

            z_copy(where, step, True).start()

        @pl.when(goal < at_out)
        def _():
            @pl.when(at_out < outs - 1)
            def _():
                z_wait(goal)
                grads[where] = grads[where] + z_in[goal]

            z_copy(where, step, False).start()

    gain_part = gain_part + weight_rows(0)
    reduce_step(0)
    gain_part = gain_part + weight_rows(1)
    after_core(0)

    small_all[seq] = small_in[...]
    small_all[seq, 0] = joined[span + 2 * NSTATE : span + 2 * NSTATE + 8, :] * gain_row
    small_all[seq, 2, 0:1, :] = gain_part
    sa = []
    for j in range(1, seqs):
        sa.append(
            remote(
                small_all.at[seq],
                small_all.at[seq],
                sa_s.at[j - 1],
                sa_r.at[j - 1],
                lax.rem(seq + j, seqs),
                head,
            )
        )
        sa[-1].start()
    after_core(1)

    for copy in ba:
        copy.wait_recv()
    own = pl.ds(seq * heads, heads)
    bc_part[own] = bc_part[own] + bc_seq[0]
    for j in range(1, seqs - 1):
        bc_part[own] = bc_part[own] + bc_seq[j]
    bb = []
    for j in range(1, heads):
        to = lax.rem(head + j, heads)
        bb.append(
            remote(
                bc_part.at[seq * heads + to],
                bc_head.at[j - 1],
                bb_s.at[j - 1],
                bb_r.at[j - 1],
                seq,
                to,
            )
        )
        bb[-1].start()

    def sent_from(j, count, at):
        return lax.rem(at - j + count, count)

    for j in range(1, seqs):
        came = sent_from(j, seqs, seq)
        remote(
            small_all.at[came], small_all.at[came], sa_s.at[j - 1], sa_r.at[j - 1], partner, head
        ).wait_recv()
    total = small_all[0]
    for j in range(1, seqs):
        total = total + small_all[j]
    small_out[...] = total
    small_head[head] = total[2]
    sb = []
    for j in range(1, heads):
        sb.append(
            remote(
                small_head.at[head],
                small_head.at[head],
                sb_s.at[j - 1],
                sb_r.at[j - 1],
                seq,
                lax.rem(head + j, heads),
            )
        )
        sb[-1].start()

    reduce_step(1)
    for copy in bb:
        copy.wait_recv()
    piece = bc_part[seq * heads + head]
    for j in range(heads - 1):
        piece = piece + bc_head[j]
    here = seq * heads + head
    bc_full[here] = piece
    bc = []
    for j in range(1, heads):
        bc.append(
            remote(
                bc_full.at[here],
                bc_full.at[here],
                bc_s.at[j - 1],
                bc_r.at[j - 1],
                seq,
                lax.rem(head + j, heads),
            )
        )
        bc[-1].start()
    for j in range(1, heads):
        came = sent_from(j, heads, head)
        remote(
            small_head.at[came], small_head.at[came], sb_s.at[j - 1], sb_r.at[j - 1], seq, came
        ).wait_recv()
    total = small_head[0]
    for j in range(1, heads):
        total = total + small_head[j]
    small_out[2] = total
    for j in range(1, heads):
        came = seq * heads + sent_from(j, heads, head)
        remote(
            bc_full.at[came], bc_full.at[came], bc_s.at[j - 1], bc_r.at[j - 1], partner, head
        ).wait_recv()
    bd = []
    for j in range(1, seqs):
        bd.append(
            remote(
                bc_full.at[own],
                bc_full.at[own],
                bd_s.at[j - 1],
                bd_r.at[j - 1],
                lax.rem(seq + j, seqs),
                head,
            )
        )
        bd[-1].start()
    for step in range(2, outs - 1):
        reduce_step(step)
    after_x(0, gate_out)
    reduce_step(outs - 1)
    where = at_out * ins + at_in
    grad_hat = grads[where] * gain_row
    rows = resid[...]
    scale = lax.rsqrt(jnp.mean(rows * rows, axis=1, keepdims=True) + EPSILON)
    row_cross = jnp.sum(grad_hat * rows, axis=1, keepdims=True)
    resid_grad[...] = (
        cot[...] + scale * grad_hat - rows * (scale * scale * scale * (row_cross / width))
    )
    after_x(1, inner_out)
    for j in range(1, seqs):
        came = pl.ds(sent_from(j, seqs, seq) * heads, heads)
        remote(
            bc_full.at[came], bc_full.at[came], bd_s.at[j - 1], bd_r.at[j - 1], partner, head
        ).wait_recv()
    bc_put = pltpu.make_async_copy(bc_full, bc_out, o_sem.at[2])
    bc_put.start()

    @pl.loop(0, outs)
    def _(step):
        for j in range(ins - 1):
            y_copy(step, j).wait_send()

    for step in range(outs - 1):
        remote(
            grads.at[0], z_in.at[0], z_send.at[step], z_recv.at[0], partner, head
        ).wait_send()
    for copy in ba + bb + bc + bd + sa + sb:
        copy.wait_send()
    for n in range(2):
        finals[n].wait_send()
        remote(
            keep.at[n],
            (gate_out, inner_out)[n].at[theirs],
            f_send.at[n],
            f_recv.at[n],
            partner,
            head,
        ).wait_recv()
        puts[n].wait()
    bc_put.wait()


def tail(gp, hat, weight, small, resid, cot, gain, seqs, heads, chans):
    tokens, width = hat[0].shape
    chunk = tokens // heads
    pad = gp[0].shape[1]
    ins = inner_count(heads)
    outs = heads // ins
    rounds = (seqs // 2).bit_length() - 1
    half = chans // 2
    lanes = 2 * NSTATE * width // (8 * seqs * heads)
    pieces = seqs * heads
    anywhere = pl.BlockSpec(memory_space=pl.ANY)
    local = pl.BlockSpec(memory_space=pltpu.VMEM)
    sems = pltpu.SemaphoreType.DMA
    weight_shape = jax.ShapeDtypeStruct((chans, width), F32)
    return pl.pallas_call(
        functools.partial(tail_kernel, (seqs, heads, chunk, chans, pad)),
        out_shape=(
            jax.ShapeDtypeStruct((chunk, width), F32),
            weight_shape,
            weight_shape,
            jax.ShapeDtypeStruct((pieces, 8, lanes), F32),
            jax.ShapeDtypeStruct((3, 8, width), F32),
        ),
        in_specs=[anywhere] * 6 + [local] * 4,
        out_specs=(local, anywhere, anywhere, anywhere, local),
        scratch_shapes=[
            pltpu.VMEM((tokens, pad), BF16),
            pltpu.VMEM((tokens, pad), BF16),
            pltpu.VMEM((tokens, width), BF16),
            pltpu.VMEM((tokens, width), BF16),
            pltpu.VMEM((pad, width), BF16),
            pltpu.VMEM((pad, width), BF16),
            pltpu.VMEM((heads, chunk, width), F32),
            pltpu.VMEM((outs * (ins - 1), chunk, width), F32),
            pltpu.VMEM((outs + 1, chunk, width), F32),
            pltpu.VMEM((pad, width), F32),
            pltpu.VMEM((2, half, width), F32),
            pltpu.VMEM((2, half, width), F32),
            pltpu.VMEM((2, rounds, half, width), F32),
            pltpu.VMEM((pieces, 8, lanes), F32),
            pltpu.VMEM((seqs - 1, heads, 8, lanes), F32),
            pltpu.VMEM((heads - 1, 8, lanes), F32),
            pltpu.VMEM((pieces, 8, lanes), F32),
            pltpu.VMEM((seqs, 3, 8, width), F32),
            pltpu.VMEM((heads, 8, width), F32),
            sems((6,)),
            sems((outs * (ins - 1),)),
            sems((outs * (ins - 1),)),
            sems((outs,)),
            sems((outs + 1,)),
            sems((2,)),
            sems((2,)),
            sems((2, rounds)),
            sems((2, rounds)),
            sems((2,)),
            sems((2,)),
            sems((3,)),
            sems((seqs - 1,)),
            sems((seqs - 1,)),
            sems((heads - 1,)),
            sems((heads - 1,)),
            sems((heads - 1,)),
            sems((heads - 1,)),
            sems((seqs - 1,)),
            sems((seqs - 1,)),
            sems((seqs - 1,)),
            sems((seqs - 1,)),
            sems((heads - 1,)),
            sems((heads - 1,)),
        ],
        compiler_params=pltpu.CompilerParams(
            collective_id=1, has_side_effects=True, vmem_limit_bytes=VMEM_LIMIT
        ),
        name="tail",
    )(*gp, *hat, *weight, small, resid, cot, gain)


def head_kernel(dims, *refs):
    heads, chunk, chans, pad = dims
    (
        rows, gain, gate_w, inner_w, bc_w, step_w,
        hat_hi, hat_lo, proj_out, w_hi, w_lo,
        parts, hth, htl, proj, raw, wh, wl, wth, wtl,
        load_sem, z_send, z_recv, y_send, y_recv, put_sem,
    ) = refs
    width = gain.shape[1]
    ins = inner_count(heads)
    outs = heads // ins
    span = 2 * chans
    seq, head = lax.axis_index("seq"), lax.axis_index("head")
    at_out, at_in = head // ins, lax.rem(head, ins)

    loads = [
        pltpu.make_async_copy(gate_w, raw.at[pl.ds(0, chans)], load_sem.at[0]),
        pltpu.make_async_copy(inner_w, raw.at[pl.ds(chans, chans)], load_sem.at[1]),
    ]
    for load in loads:
        load.start()
    greet(seq, head, 1, heads)
    values = rows[...]
    parts[head] = values * lax.rsqrt(
        jnp.mean(values * values, axis=1, keepdims=True) + EPSILON
    )

    def z_copy(where, up):
        return remote(
            parts.at[where],
            parts.at[where],
            z_send.at[where // ins, up],
            z_recv.at[where // ins],
            seq,
            (at_out + 2 * up - 1) * ins + at_in,
        )

    def y_copy(where, j, to):
        return remote(
            parts.at[where],
            parts.at[where],
            y_send.at[where // ins, j],
            y_recv.at[where // ins, j],
            seq,
            at_out * ins + to,
        )

    def arrived(place, distance, first):
        where = place * ins + at_in

        @pl.when(distance > 0)
        def _():
            z_copy(where, 0).wait_recv()

        @pl.when((place >= at_out) & (at_out > 0))
        def _():
            z_copy(where, 0).start()

        @pl.when((place <= at_out) & (at_out < outs - 1))
        def _():
            z_copy(where, 1).start()

        for j in range(ins - 1):
            y_copy(where, j, lax.rem(at_in + 1 + j, ins)).start()

    arrived(at_out, 0, True)

    raw[span : span + 2 * NSTATE, :] = bc_w[...].T
    raw[span + 2 * NSTATE :, :] = step_w[...]
    for load in loads:
        load.wait()
    gain_row = gain[...]

    @pl.loop(0, pad // 128)
    def _(block):
        here = pl.ds(pl.multiple_of(block * 128, 128), 128)
        piece = raw[here, :]
        top = piece.astype(BF16)
        wh[here, :] = top
        wl[here, :] = (piece - top.astype(F32)).astype(BF16)
        turned = (piece * gain_row).T
        top = turned.astype(BF16)
        wth[:, here] = top
        wtl[:, here] = (turned - top.astype(F32)).astype(BF16)

    puts = [
        pltpu.make_async_copy(wh, w_hi, put_sem.at[0]),
        pltpu.make_async_copy(wl, w_lo, put_sem.at[1]),
    ]
    for put in puts:
        put.start()

    def chunk_rows(where):
        return pl.ds(pl.multiple_of(where * chunk, 8), chunk)

    def chunk_puts(where):
        here = chunk_rows(where)
        return [
            pltpu.make_async_copy(hth.at[where], hat_hi.at[here], put_sem.at[2 + 3 * where]),
            pltpu.make_async_copy(htl.at[where], hat_lo.at[here], put_sem.at[3 + 3 * where]),
            pltpu.make_async_copy(proj.at[where], proj_out.at[here], put_sem.at[4 + 3 * where]),
        ]

    def project(where):
        piece = parts[where]
        top = piece.astype(BF16)
        low = (piece - top.astype(F32)).astype(BF16)
        hth[where] = top
        htl[where] = low
        proj[where] = dot3((top, low), (wth[...], wtl[...]), 1, 0)
        for put in chunk_puts(where):
            put.start()

    @pl.loop(0, outs + 1)
    def _(distance):
        for side in range(2):
            place = at_out + (2 * side - 1) * distance

            @pl.when((distance > 0) & (place >= 0) & (place < outs))
            def _():
                arrived(place, distance, False)

        @pl.loop(0, 2 * ins)
        def _(n):
            side, j = n // ins, lax.rem(n, ins)
            late = (j + ins - 1) // ins
            away = distance - late
            place = at_out + (2 * side - 1) * away

            @pl.when(
                (place >= 0) & (place < outs) & (away >= 0) & (away + 1 - side > 0)
            )
            def _():
                frm = lax.rem(at_in + ins - j, ins)
                where = place * ins + frm

                @pl.when(j > 0)
                def _():
                    y_copy(where, j - 1, lax.rem(at_in + 1, ins)).wait_recv()

                project(where)

    for place in range(outs):
        where = place * ins + at_in

        @pl.when((place >= at_out) & (at_out > 0))
        def _():
            z_copy(where, 0).wait_send()

        @pl.when((place <= at_out) & (at_out < outs - 1))
        def _():
            z_copy(where, 1).wait_send()

        for j in range(ins - 1):
            y_copy(where, j, lax.rem(at_in + 1 + j, ins)).wait_send()
    for put in puts:
        put.wait()

    @pl.loop(0, heads)
    def _(where):
        for put in chunk_puts(where):
            put.wait()


def gather_project(resid, gain, gate_w, inner_w, bc_w, step_w, heads):
    chunk, width = resid.shape
    chans = gate_w.shape[0]
    pad = 2 * chans + 2 * NSTATE + 128
    ins = inner_count(heads)
    outs = heads // ins
    tokens = chunk * heads
    anywhere = pl.BlockSpec(memory_space=pl.ANY)
    local = pl.BlockSpec(memory_space=pltpu.VMEM)
    sems = pltpu.SemaphoreType.DMA
    shape = jax.ShapeDtypeStruct
    return pl.pallas_call(
        functools.partial(head_kernel, (heads, chunk, chans, pad)),
        out_shape=(
            shape((tokens, width), BF16),
            shape((tokens, width), BF16),
            shape((tokens, pad), F32),
            shape((pad, width), BF16),
            shape((pad, width), BF16),
        ),
        in_specs=[local, local, anywhere, anywhere, local, local],
        out_specs=(anywhere,) * 5,
        scratch_shapes=[
            pltpu.VMEM((heads, chunk, width), F32),
            pltpu.VMEM((heads, chunk, width), BF16),
            pltpu.VMEM((heads, chunk, width), BF16),
            pltpu.VMEM((heads, chunk, pad), F32),
            pltpu.VMEM((pad, width), F32),
            pltpu.VMEM((pad, width), BF16),
            pltpu.VMEM((pad, width), BF16),
            pltpu.VMEM((width, pad), BF16),
            pltpu.VMEM((width, pad), BF16),
            sems((2,)),
            sems((outs, 2)),
            sems((outs,)),
            sems((outs, ins - 1)),
            sems((outs, ins - 1)),
            sems((2 + 3 * heads,)),
        ],
        compiler_params=pltpu.CompilerParams(
            collective_id=2, has_side_effects=True, vmem_limit_bytes=VMEM_LIMIT
        ),
        name="gather_project",
    )(resid, gain, gate_w, inner_w, bc_w, step_w)


def dotx(left, right, left_dim, right_dim):
    return lax.dot_general(
        left,
        right,
        (((left_dim,), (right_dim,)), ((), ())),
        precision=EXACT,
        preferred_element_type=F32,
    )


def halves(values):
    top = values.astype(BF16)
    return (top, (values - top.astype(F32)).astype(BF16))


class LineGather:
    def __init__(self, parts, sems, seq, head, heads):
        self.parts, self.seq, self.heads = parts, seq, heads
        self.z_send, self.z_recv, self.y_send, self.y_recv = sems
        self.ins = inner_count(heads)
        self.outs = heads // self.ins
        self.at_out, self.at_in = head // self.ins, lax.rem(head, self.ins)

    def z_copy(self, where, up):
        place = where // self.ins
        return remote(
            self.parts.at[where],
            self.parts.at[where],
            self.z_send.at[place, up],
            self.z_recv.at[place],
            self.seq,
            (self.at_out + 2 * up - 1) * self.ins + self.at_in,
        )

    def y_copy(self, where, j, to):
        place = where // self.ins
        return remote(
            self.parts.at[where],
            self.parts.at[where],
            self.y_send.at[place, j],
            self.y_recv.at[place, j],
            self.seq,
            self.at_out * self.ins + to,
        )

    def arrived(self, place, wait):
        where = place * self.ins + self.at_in
        if wait:
            self.z_copy(where, 0).wait_recv()

        @pl.when((place >= self.at_out) & (self.at_out > 0))
        def _():
            self.z_copy(where, 0).start()

        @pl.when((place <= self.at_out) & (self.at_out < self.outs - 1))
        def _():
            self.z_copy(where, 1).start()

        for j in range(self.ins - 1):
            self.y_copy(where, j, lax.rem(self.at_in + 1 + j, self.ins)).start()

    def start(self):
        self.arrived(self.at_out, False)

    def relay(self, distance):
        for side in range(2):
            place = self.at_out + (2 * side - 1) * distance

            @pl.when((place >= 0) & (place < self.outs))
            def _():
                self.arrived(place, True)

    def use(self, distance, consume):
        @pl.loop(0, 2 * self.ins)
        def _(n):
            side, j = n // self.ins, lax.rem(n, self.ins)
            late = (j + self.ins - 1) // self.ins
            away = distance - late
            place = self.at_out + (2 * side - 1) * away

            @pl.when(
                (place >= 0) & (place < self.outs) & (away >= 0) & (away + 1 - side > 0)
            )
            def _():
                where = place * self.ins + lax.rem(self.at_in + self.ins - j, self.ins)

                @pl.when(j > 0)
                def _():
                    self.y_copy(where, j - 1, lax.rem(self.at_in + 1, self.ins)).wait_recv()

                consume(where)

    def finish(self):
        for place in range(self.outs):
            where = place * self.ins + self.at_in

            @pl.when((place >= self.at_out) & (self.at_out > 0))
            def _():
                self.z_copy(where, 0).wait_send()

            @pl.when((place <= self.at_out) & (self.at_out < self.outs - 1))
            def _():
                self.z_copy(where, 1).wait_send()

            for j in range(self.ins - 1):
                self.y_copy(where, j, lax.rem(self.at_in + 1 + j, self.ins)).wait_send()


def lanes_of(chans):
    return [(lo, min(lo + 2 * HEADDIM, chans)) for lo in range(0, chans, 2 * HEADDIM)]


def row_scale(total_row, expand):
    wide = jnp.broadcast_to(jnp.exp(total_row), (128, 128)).T
    return dotx(expand, wide, 0, 0)


def logistic(values):
    return 1.0 / (1.0 + jnp.exp(-values))


def decay_of(cum, cum_turned, h, causal):
    gap = cum[:, h : h + 1] - cum_turned[h : h + 1, :]
    return jnp.where(causal, jnp.exp(jnp.where(causal, gap, 0.0)), 0.0)


def forward_kernel(dims, *refs):
    seqs, heads, chunk, chans, pad = dims
    (
        proj, cot, out_w, conv_p, head_p, chan_p, expand_in,
        cot_hi, cot_lo, conv_o, cum_o, step_o, state_o, mixed_o, cross_o, stat_o, edge_o,
        parts, hi, lo, pj, raw, owh, owl, scaled, enter, prefix, run, exch, stat_all, lows,
        z_send, z_recv, y_send, y_recv, load_sem, put_sem, e_send, e_recv,
        s_send, s_recv, t_send, t_recv,
    ) = refs
    tokens = chunk * heads
    blocks = tokens // BLOCK
    span = 2 * chans
    wide = chans + 2 * NSTATE
    here_heads = chans // HEADDIM
    seq, head = lax.axis_index("seq"), lax.axis_index("head")
    load = pltpu.make_async_copy(proj, pj.at[pl.ds(8, tokens)], load_sem.at[0])
    load.start()
    load_w = pltpu.make_async_copy(out_w, raw, load_sem.at[1])
    load_w.start()
    parts[head] = cot[...]
    greet(seq, head, seqs, heads)
    gather = LineGather(parts, (z_send, z_recv, y_send, y_recv), seq, head, heads)
    gather.start()
    edge = remote(
        proj.at[pl.ds(tokens - 8, 8)],
        pj.at[pl.ds(0, 8)],
        e_send,
        e_recv,
        lax.rem(seq + 1, seqs),
        head,
    )
    edge.start()
    load_w.wait()
    for lane, end in lanes_of(chans):
        owh[:, lane:end], owl[:, lane:end] = halves(raw[lane:end, :].T)
    expand = expand_in[...]
    load.wait()
    edge.wait()
    first = jnp.where(seq > 0, pj[0:8, :], 0.0)
    pj[0:8, :] = first
    edge_o[...] = first
    tri_r = lax.broadcasted_iota(jnp.int32, (BLOCK, BLOCK), 0)
    tri_c = lax.broadcasted_iota(jnp.int32, (BLOCK, BLOCK), 1)
    causal = tri_r >= tri_c
    lower = causal.astype(F32)
    run[...] = jnp.zeros_like(run)
    prefix[...] = jnp.zeros_like(prefix)

    @pl.loop(0, blocks)
    def _(b):
        at = pl.multiple_of(b * BLOCK, BLOCK)
        here = pl.ds(at, BLOCK)
        window = pj[pl.ds(at, BLOCK + 8), chans : span + 2 * NSTATE]
        conv = jnp.zeros((BLOCK, wide), F32) + conv_p[4:5, :]
        for k in range(WIDTH):
            conv = conv + conv_p[k : k + 1, :] * window[5 + k : 5 + k + BLOCK, :]
        conv_o[here, :] = conv
        act = conv * logistic(conv)
        arg = pj[pl.ds(at + 8, BLOCK), span + 2 * NSTATE : pad] + head_p[0:1, :]
        step = jnp.maximum(arg, 0.0) + jnp.log1p(jnp.exp(-jnp.abs(arg)))
        cum = dotx(lower, step * head_p[1:2, :], 1, 0)
        last = cum[BLOCK - 1 : BLOCK, :]
        step_o[here, :] = step
        cum_o[here, :] = cum
        fed = act[:, :chans] * dotx(step, expand, 1, 0)
        scaled[here, :] = fed
        fresh = dotx(
            fed * dotx(jnp.exp(last - cum), expand, 1, 0), act[:, chans : chans + NSTATE], 0, 0
        )
        enter[b] = run[...]
        run[...] = row_scale(last, expand) * run[...] + fresh
        prefix[pl.ds(b + 1, 1), :] = prefix[pl.ds(b, 1), :] + last

    gather.relay(1)
    exch[seq, 0:chans, :] = run[...]
    exch[seq, chans : chans + 8, :] = jnp.broadcast_to(prefix[blocks : blocks + 1, :], (8, 128))

    def state_copy(at, j, to):
        return remote(exch.at[at], exch.at[at], s_send.at[j - 1], s_recv.at[j - 1], to, head)

    for j in range(1, seqs):

        @pl.when(seq + j < seqs)
        def _():
            state_copy(seq, j, seq + j).start()

    @pl.loop(0, blocks)
    def _(b):
        at = pl.multiple_of(b * BLOCK, BLOCK)
        here = pl.ds(at, BLOCK)
        bc = conv_o[here, chans:wide]
        bc = bc * logistic(bc)
        scores = dotx(bc[:, NSTATE:], bc[:, :NSTATE], 1, 1)
        cum = cum_o[here, :]
        turned = cum.T
        for first_lane, end in lanes_of(chans):
            fed = scaled[here, first_lane:end]
            outs = [
                dotx(decay_of(cum, turned, lane // HEADDIM, causal) * scores, fed, 1, 0)
                for lane in range(first_lane, end, HEADDIM)
            ]
            out = outs[0]
            if len(outs) == 2:
                lane = lax.broadcasted_iota(jnp.int32, out.shape, 1)
                out = jnp.where(lane < HEADDIM, outs[0], outs[1])
            mixed_o[here, first_lane:end] = out

    if gather.outs > 2:
        gather.relay(2)
    run[...] = jnp.zeros_like(run)
    for earlier in range(seqs - 1):

        @pl.when(earlier < seq)
        def _():
            for j in range(1, seqs):

                @pl.when(seq - earlier == j)
                def _():
                    state_copy(earlier, j, lax.rem(seq + 1, seqs)).wait_recv()

            run[...] = (
                row_scale(exch[earlier, chans : chans + 1, :], expand) * run[...]
                + exch[earlier, 0:chans, :]
            )

    @pl.loop(0, blocks)
    def _(b):
        at = pl.multiple_of(b * BLOCK, BLOCK)
        here = pl.ds(at, BLOCK)
        state = enter[b] + row_scale(prefix[pl.ds(b, 1), :], expand) * run[...]
        state_o[b] = state
        conv = conv_o[here, :]
        act = conv * logistic(conv)
        gate = pj[pl.ds(at + 8, BLOCK), 0:chans]
        carried = dotx(act[:, chans + NSTATE :], state, 1, 1)
        mixed = (
            mixed_o[here, :]
            + carried * dotx(jnp.exp(cum_o[here, :]), expand, 1, 0)
            + chan_p[1:2, :] * act[:, :chans]
        )
        mixed_o[here, :] = mixed
        scaled[here, :] = mixed * gate * logistic(gate)

    for distance in range(3, gather.outs):
        gather.relay(distance)

    def chunk_puts(where):
        rows = pl.ds(pl.multiple_of(where * chunk, 8), chunk)
        return [
            pltpu.make_async_copy(hi.at[where], cot_hi.at[rows], put_sem.at[2 * where]),
            pltpu.make_async_copy(lo.at[where], cot_lo.at[rows], put_sem.at[2 * where + 1]),
        ]

    def consume(where):
        rows = pl.ds(pl.multiple_of(where * chunk, 8), chunk)
        top, low = halves(parts[where])
        hi[where] = top
        lo[where] = low
        cross_o[rows, :] = dot3((top, low), (owh[...], owl[...]), 1, 0)
        for put in chunk_puts(where):
            put.start()

    for distance in range(gather.outs + 1):
        gather.use(distance, consume)

    ones = jnp.ones((8, chans), F32)
    groups = tokens // 128
    for n in range(groups):
        here = slice(n * 128, n * 128 + 128)
        gated = scaled[here, :]
        lows[n : n + 1, :] = dotx(ones, gated * gated, 1, 1)[0:1, :]
        lows[groups + n : groups + n + 1, :] = dotx(
            ones, cross_o[here, :] * chan_p[0:1, :] * gated, 1, 1
        )[0:1, :]
    stat_all[head] = lows[...]
    sends = []
    for j in range(1, heads):
        sends.append(
            remote(
                stat_all.at[head],
                stat_all.at[head],
                t_send.at[j - 1],
                t_recv.at[j - 1],
                seq,
                lax.rem(head + j, heads),
            )
        )
        sends[-1].start()
    gather.finish()

    @pl.loop(0, heads)
    def _(where):
        for put in chunk_puts(where):
            put.wait()

    for j in range(1, seqs):

        @pl.when(seq + j < seqs)
        def _():
            state_copy(seq, j, seq + j).wait_send()

    for j in range(1, heads):
        came = lax.rem(head - j + heads, heads)
        remote(
            stat_all.at[came], stat_all.at[came], t_send.at[j - 1], t_recv.at[j - 1], seq, came
        ).wait_recv()
    total = stat_all[0]
    for j in range(1, heads):
        total = total + stat_all[j]
    stat_o[...] = total
    for copy in sends:
        copy.wait_send()


def forward(proj, cot, out_w, conv_p, head_p, chan_p, expand, seqs, heads):
    tokens, pad = proj.shape
    chunk, width = cot.shape
    chans = out_w.shape[0]
    ins = inner_count(heads)
    outs = heads // ins
    wide = chans + 2 * NSTATE
    blocks = tokens // BLOCK
    groups = 2 * tokens // 128
    anywhere = pl.BlockSpec(memory_space=pl.ANY)
    local = pl.BlockSpec(memory_space=pltpu.VMEM)
    sems = pltpu.SemaphoreType.DMA
    shape = jax.ShapeDtypeStruct
    return pl.pallas_call(
        functools.partial(forward_kernel, (seqs, heads, chunk, chans, pad)),
        out_shape=(
            shape((tokens, width), BF16),
            shape((tokens, width), BF16),
            shape((tokens, wide), F32),
            shape((tokens, 128), F32),
            shape((tokens, 128), F32),
            shape((blocks, chans, NSTATE), F32),
            shape((tokens, chans), F32),
            shape((tokens, chans), F32),
            shape((groups, 128), F32),
            shape((8, pad), F32),
        ),
        in_specs=[anywhere, local, anywhere, local, local, local, local],
        out_specs=(anywhere, anywhere) + (local,) * 8,
        scratch_shapes=[
            pltpu.VMEM((heads, chunk, width), F32),
            pltpu.VMEM((heads, chunk, width), BF16),
            pltpu.VMEM((heads, chunk, width), BF16),
            pltpu.VMEM((8 + tokens, pad), F32),
            pltpu.VMEM((chans, width), F32),
            pltpu.VMEM((width, chans), BF16),
            pltpu.VMEM((width, chans), BF16),
            pltpu.VMEM((tokens, chans), F32),
            pltpu.VMEM((blocks, chans, NSTATE), F32),
            pltpu.VMEM((8, 128), F32),
            pltpu.VMEM((chans, NSTATE), F32),
            pltpu.VMEM((seqs, chans + 8, NSTATE), F32),
            pltpu.VMEM((heads, groups, 128), F32),
            pltpu.VMEM((groups, 128), F32),
            sems((outs, 2)),
            sems((outs,)),
            sems((outs, ins - 1)),
            sems((outs, ins - 1)),
            sems((2,)),
            sems((2 * heads,)),
            sems,
            sems,
            sems((seqs - 1,)),
            sems((seqs - 1,)),
            sems((heads - 1,)),
            sems((heads - 1,)),
        ],
        compiler_params=pltpu.CompilerParams(
            collective_id=3, has_side_effects=True, vmem_limit_bytes=VMEM_LIMIT
        ),
        name="forward",
    )(proj, cot, out_w, conv_p, head_p, chan_p, expand)


class LineReduce:
    def __init__(self, parts, y_in, z_in, sems, seq, head, heads, partner):
        self.parts, self.y_in, self.z_in = parts, y_in, z_in
        self.y_send, self.y_recv, self.z_send, self.z_recv = sems
        self.seq, self.partner = seq, partner
        self.ins = inner_count(heads)
        self.outs = heads // self.ins
        self.at_out, self.at_in = head // self.ins, lax.rem(head, self.ins)
        self.upper = self.at_out // (self.outs // 2)
        self.mirrored = self.at_out + self.upper * (self.outs - 1 - 2 * self.at_out)

    def target(self, step):
        last = (step + 1) // self.outs
        far = self.outs - 1 - step
        far = far - (self.mirrored - far + self.outs) // self.outs
        far = far + self.upper * (self.outs - 1 - 2 * far)
        return far + last * (self.at_out - far)

    def y_copy(self, step, j):
        to = lax.rem(self.at_in + 1 + j, self.ins)
        slot = self.target(step) * (self.ins - 1) + j
        return remote(
            self.parts.at[self.target(step) * self.ins + to],
            self.y_in.at[slot],
            self.y_send.at[slot],
            self.y_recv.at[slot],
            self.seq,
            self.at_out * self.ins + to,
        )

    def give(self, make):
        @pl.loop(0, self.outs)
        def _(step):
            for j in range(self.ins - 1):
                make(self.target(step) * self.ins + lax.rem(self.at_in + 1 + j, self.ins))
                self.y_copy(step, j).start()

    def own(self, make):
        @pl.loop(0, self.outs)
        def _(step):
            make(self.target(step) * self.ins + self.at_in)

    def take(self, where, slot):
        remote(
            self.parts.at[0],
            self.z_in.at[slot],
            self.z_send.at[0],
            self.z_recv.at[slot],
            self.partner,
            self.at_out * self.ins + self.at_in,
        ).wait_recv()
        self.parts[where] = self.parts[where] + self.z_in[slot]

    def pass_on(self, where, step, up):
        slot = self.target(step) + up
        remote(
            self.parts.at[where],
            self.z_in.at[slot],
            self.z_send.at[step],
            self.z_recv.at[slot],
            self.seq,
            (self.at_out + 2 * up - 1) * self.ins + self.at_in,
        ).start()

    def reduce(self, step):
        goal = self.target(step)
        where = goal * self.ins + self.at_in
        for j in range(self.ins - 1):
            self.y_copy(step, j).wait_recv()
            self.parts[where] = self.parts[where] + self.y_in[goal * (self.ins - 1) + j]
        from_below, from_above = self.at_out > 0, self.at_out < self.outs - 1

        @pl.when((goal >= self.at_out) & from_below)
        def _():
            self.take(where, goal + 1)

        @pl.when((goal <= self.at_out) & from_above)
        def _():
            self.take(where, goal)

        if step < self.outs - 1:

            @pl.when(goal > self.at_out)
            def _():
                self.pass_on(where, step, 1)

            @pl.when(goal < self.at_out)
            def _():
                self.pass_on(where, step, 0)

    def finish(self):
        @pl.loop(0, self.outs)
        def _(step):
            for j in range(self.ins - 1):
                self.y_copy(step, j).wait_send()

        for step in range(self.outs - 1):
            remote(
                self.parts.at[0],
                self.z_in.at[0],
                self.z_send.at[step],
                self.z_recv.at[0],
                self.partner,
                self.at_out * self.ins + self.at_in,
            ).wait_send()


def backward_kernel(dims, *refs):
    seqs, heads, chunk, chans, pad = dims
    (
        proj, edge_in, cot_hi, cot_lo, conv_in, cum_in, step_in, state_in, mixed_in, cross_in,
        stat_in, out_w, resid, conv_p, head_p, chan_p, expand_in,
        result_o, gp_hi, gp_lo, out_o, wide_o, chan_o, head_o,
        pj, ngh, ngl, owh, owl, gmix, fedg, adj, run, exch, gconv,
        parts, y_in, z_in, chi, clo, oparts, keep, core_in, x_in, head_acc,
        y_send, y_recv, z_send, z_recv, load_sem, s_send, s_recv, e_send, e_recv,
        c_send, c_recv, x_send, x_recv, f_send, f_recv, o_sem,
    ) = refs
    tokens = chunk * heads
    blocks = tokens // BLOCK
    span = 2 * chans
    wide = chans + 2 * NSTATE
    half = chans // 2
    rounds = (seqs // 2).bit_length() - 1
    split_at = resid.shape[1] // 2
    seq, head = lax.axis_index("seq"), lax.axis_index("head")
    side = lax.rem(seq, 2)
    partner = seq + 1 - 2 * side
    loads = [
        pltpu.make_async_copy(a, b, load_sem.at[n])
        for n, (a, b) in enumerate(
            (
                (proj, pj.at[pl.ds(8, tokens)]),
                (edge_in, pj.at[pl.ds(0, 8)]),
                (cot_hi.at[:, pl.ds(0, split_at)], chi),
                (cot_lo.at[:, pl.ds(0, split_at)], clo),
                (out_w, oparts),
            )
        )
    ]
    for load in loads:
        load.start()
    greet(seq, head, seqs, heads)
    loads[4].wait()
    owh[...], owl[...] = halves(oparts[...])
    expand = expand_in[...]
    tri_r = lax.broadcasted_iota(jnp.int32, (BLOCK, BLOCK), 0)
    tri_c = lax.broadcasted_iota(jnp.int32, (BLOCK, BLOCK), 1)
    causal = tri_r >= tri_c
    upper = (tri_r <= tri_c).astype(F32)
    wide_o[...] = jnp.zeros_like(wide_o)
    chan_o[...] = jnp.zeros_like(chan_o)
    head_acc[...] = jnp.zeros_like(head_acc)
    run[...] = jnp.zeros_like(run)
    for load in loads[:2]:
        load.wait()
    per = BLOCK // 128
    groups = tokens // 128
    turned_stats = stat_in[...].T
    inner_total = DI_TOTAL(heads, chans)
    gain_row, skip_row = chan_p[0:1, :], chan_p[1:2, :]

    for b in range(blocks - 1, -1, -1):
        at = b * BLOCK
        here = slice(at, at + BLOCK)
        squares = jnp.concatenate(
            [turned_stats[:, b * per + n : b * per + n + 1] for n in range(per)], 0
        )
        cross = jnp.concatenate(
            [
                turned_stats[:, groups + b * per + n : groups + b * per + n + 1]
                for n in range(per)
            ],
            0,
        )
        scale = lax.rsqrt(squares / inner_total + EPSILON)
        factor = scale * scale * scale * (cross / inner_total)
        gate = pj[at + 8 : at + 8 + BLOCK, 0:chans]
        sig = logistic(gate)
        gate_act = gate * sig
        mixed = mixed_in[here, :]
        gated = mixed * gate_act
        grad_ng = cross_in[here, :]
        grad_gated = scale * (grad_ng * gain_row) - gated * factor
        scaled = gated * scale
        ngh[here, :], ngl[here, :] = halves(scaled * gain_row)
        grad_mixed = grad_gated * gate_act
        gmix[here, :] = grad_mixed
        gp_hi[here, 0:chans], gp_lo[here, 0:chans] = halves(
            grad_gated * mixed * (sig * (1.0 + gate * (1.0 - sig)))
        )
        conv = conv_in[here, :]
        act = conv * logistic(conv)
        chan_o[0:1, :] = chan_o[0:1, :] + jnp.sum(grad_ng * scaled, 0, keepdims=True)
        chan_o[1:2, :] = chan_o[1:2, :] + jnp.sum(grad_mixed * act[:, :chans], 0, keepdims=True)
        early = grad_mixed * dotx(jnp.exp(cum_in[here, :]), expand, 1, 0)
        adj[b] = run[...]
        run[...] = row_scale(cum_in[at + BLOCK - 1 : at + BLOCK, :], expand) * run[...] + dotx(
            early, act[:, chans + NSTATE :], 0, 0
        )
        gconv[here, chans + NSTATE :] = dotx(early, state_in[b], 1, 0)

    total = jnp.zeros((1, 128), F32)
    for b in range(blocks):
        total = total + cum_in[(b + 1) * BLOCK - 1 : (b + 1) * BLOCK, :]
    exch[seq, 0:chans, :] = run[...]
    exch[seq, chans : chans + 8, :] = jnp.broadcast_to(total, (8, 128))

    def state_copy(at, j, to):
        return remote(exch.at[at], exch.at[at], s_send.at[j - 1], s_recv.at[j - 1], to, head)

    for j in range(1, seqs):

        @pl.when(seq - j >= 0)
        def _():
            state_copy(seq, j, seq - j).start()

    reduce = LineReduce(
        parts, y_in, z_in, (y_send, y_recv, z_send, z_recv), seq, head, heads, partner
    )

    def product_chunk(where):
        rows = pl.ds(pl.multiple_of(where * chunk, 8), chunk)
        parts[where] = dot3((ngh[rows, :], ngl[rows, :]), (owh[...], owl[...]), 1, 0)

    reduce.give(product_chunk)
    for load in loads[2:4]:
        load.wait()
    oparts[:, :split_at] = dot3((ngh[...], ngl[...]), (chi[...], clo[...]), 0, 0)
    rest = [
        pltpu.make_async_copy(a.at[:, pl.ds(split_at, split_at)], b, load_sem.at[n])
        for n, (a, b) in enumerate(((cot_hi, chi), (cot_lo, clo)))
    ]
    for load in rest:
        load.start()
    reduce.own(product_chunk)
    for load in rest:
        load.wait()
    oparts[:, split_at:] = dot3((ngh[...], ngl[...]), (chi[...], clo[...]), 0, 0)
    mine = pl.ds(pl.multiple_of(side * half, 8), half)
    theirs = pl.ds(pl.multiple_of((1 - side) * half, 8), half)
    keep[...] = oparts[mine, :]
    core = remote(oparts.at[theirs], core_in, c_send, c_recv, partner, head)
    core.start()

    @pl.loop(0, blocks)
    def _(b):
        at = pl.multiple_of(b * BLOCK, BLOCK)
        here = pl.ds(at, BLOCK)
        conv = conv_in[here, :]
        act = conv * logistic(conv)
        writes, reads = act[:, chans : chans + NSTATE], act[:, chans + NSTATE :]
        scores = dotx(reads, writes, 1, 1)
        cum = cum_in[here, :]
        turned = cum.T
        fed_all = act[:, :chans] * dotx(step_in[here, :], expand, 1, 0)
        grad_scores = jnp.zeros((BLOCK, BLOCK), F32)
        for first_lane, end in lanes_of(chans):
            fed = fed_all[:, first_lane:end]
            grad = gmix[here, first_lane:end]
            lane = lax.broadcasted_iota(jnp.int32, fed.shape, 1)
            outs = []
            for start in range(first_lane, end, HEADDIM):
                decay = decay_of(cum, turned, start // HEADDIM, causal)
                inside = (lane // HEADDIM) == (start - first_lane) // HEADDIM
                grad_scores = grad_scores + decay * dotx(jnp.where(inside, grad, 0.0), fed, 1, 1)
                outs.append(dotx(decay * scores, grad, 0, 0))
            out = outs[0]
            if len(outs) == 2:
                out = jnp.where(lane < HEADDIM, outs[0], outs[1])
            fedg[here, first_lane:end] = out
        gconv[here, chans : chans + NSTATE] = dotx(grad_scores, reads, 0, 0)
        gconv[here, chans + NSTATE :] = gconv[here, chans + NSTATE :] + dotx(grad_scores, writes, 1, 0)

    core.wait()
    keep[...] = keep[...] + core_in[...]
    x_copies = []

    def x_start(source, turn):
        far = seq + (2 << turn) - 2 * (2 << turn) * lax.rem(seq // (2 << turn), 2)
        x_copies.append(
            remote(source, x_in.at[turn], x_send.at[turn], x_recv.at[turn], far, head)
        )
        x_copies[-1].start()

    x_start(keep, 0)
    reduce.reduce(0)
    run[...] = jnp.zeros_like(run)
    for back in range(seqs - 1):
        later = seqs - 1 - back

        @pl.when(later > seq)
        def _():
            for j in range(1, seqs):

                @pl.when(later - seq == j)
                def _():
                    state_copy(later, j, partner).wait_recv()

            run[...] = (
                row_scale(exch[later, chans : chans + 1, :], expand) * run[...]
                + exch[later, 0:chans, :]
            )

    for b in range(blocks - 1, -1, -1):
        adj[b] = adj[b] + run[...]
        run[...] = row_scale(cum_in[(b + 1) * BLOCK - 1 : (b + 1) * BLOCK, :], expand) * run[...]

    lane_ones = jnp.ones((8, NSTATE), F32)

    @pl.loop(0, blocks)
    def _(b):
        at = pl.multiple_of(b * BLOCK, BLOCK)
        here = pl.ds(at, BLOCK)
        conv = conv_in[here, :]
        sig = logistic(conv)
        act = conv * sig
        slope = sig * (1.0 + conv * (1.0 - sig))
        inner, writes = act[:, :chans], act[:, chans : chans + NSTATE]
        cum = cum_in[here, :]
        step = step_in[here, :]
        last = cum[BLOCK - 1 : BLOCK, :]
        step_wide = dotx(step, expand, 1, 0)
        tails = dotx(jnp.exp(last - cum), expand, 1, 0)
        fed = inner * step_wide
        grad_state = adj[b]
        from_state = tails * dotx(writes, grad_state, 1, 1)
        grad_fed = fedg[here, :] + from_state
        grad_mixed = gmix[here, :]
        grad_writes = gconv[here, chans : chans + NSTATE] + dotx(fed * tails, grad_state, 1, 0)
        direct = dotx(inner * grad_fed, expand, 1, 1)
        scanned = mixed_in[here, :] - skip_row * inner
        grad_cum = dotx(grad_mixed * scanned - fed * grad_fed, expand, 1, 1)
        kept = dotx(expand, grad_state * state_in[b], 1, 0)
        kept = dotx(lane_ones, kept, 1, 1)[0:1, :] * jnp.exp(last)
        grad_last = kept + jnp.sum(dotx(fed * from_state, expand, 1, 1), 0, keepdims=True)
        grad_log = dotx(upper, grad_cum, 1, 0) + grad_last
        rate = head_p[1:2, :]
        head_acc[1:2, :] = head_acc[1:2, :] + jnp.sum(step * grad_log, 0, keepdims=True) * rate
        arg = pj[pl.ds(at + 8, BLOCK), span + 2 * NSTATE : pad] + head_p[0:1, :]
        grad_arg = (direct + rate * grad_log) * logistic(arg) * head_p[2:3, :]
        head_acc[0:1, :] = head_acc[0:1, :] + jnp.sum(grad_arg, 0, keepdims=True)
        gp_hi[here, span + 2 * NSTATE : pad], gp_lo[here, span + 2 * NSTATE : pad] = halves(
            grad_arg
        )
        gconv[here, 0:chans] = (step_wide * grad_fed + skip_row * grad_mixed) * slope[:, :chans]
        gconv[here, chans : chans + NSTATE] = grad_writes * slope[:, chans : chans + NSTATE]
        gconv[here, chans + NSTATE :] = gconv[here, chans + NSTATE :] * slope[:, chans + NSTATE :]

    reduce.reduce(1)
    edge = remote(
        gconv.at[pl.ds(0, 8)],
        gconv.at[pl.ds(tokens, 8)],
        e_send,
        e_recv,
        lax.rem(seq + seqs - 1, seqs),
        head,
    )
    edge.start()
    head_o[...] = head_acc[...]

    def conv_back(b):
        at = pl.multiple_of(b * BLOCK, BLOCK)
        here = pl.ds(at, BLOCK)
        window = pj[pl.ds(at, BLOCK + 8), chans : span + 2 * NSTATE]
        ahead = gconv[pl.ds(at, BLOCK + 8), :]
        grad = ahead[0:BLOCK, :]
        grad_pre = jnp.zeros((BLOCK, wide), F32)
        for k in range(WIDTH):
            grad_pre = grad_pre + conv_p[k : k + 1, :] * ahead[3 - k : 3 - k + BLOCK, :]
            wide_o[k : k + 1, :] = wide_o[k : k + 1, :] + jnp.sum(
                grad * window[5 + k : 5 + k + BLOCK, :], 0, keepdims=True
            )
        wide_o[4:5, :] = wide_o[4:5, :] + jnp.sum(grad, 0, keepdims=True)
        (
            gp_hi[here, chans : span + 2 * NSTATE],
            gp_lo[here, chans : span + 2 * NSTATE],
        ) = halves(grad_pre)

    @pl.loop(0, blocks - 1)
    def _(b):
        conv_back(b)

    edge.wait()
    gconv[tokens : tokens + 8, :] = jnp.where(seq < seqs - 1, gconv[tokens : tokens + 8, :], 0.0)

    @pl.loop(blocks - 1, blocks)
    def _(b):
        conv_back(b)

    for step in range(2, reduce.outs - 1):
        reduce.reduce(step)
    now, new = keep, core_in
    for turn in range(rounds):
        x_copies[turn].wait()
        new[...] = now[...] + x_in[turn]
        now, new = new, now
        if turn + 1 < rounds:
            x_start(now, turn + 1)
    put = pltpu.make_async_copy(now, out_o.at[mine], o_sem)
    put.start()
    final = remote(now, out_o.at[mine], f_send, f_recv, partner, head)
    final.start()
    reduce.reduce(reduce.outs - 1)
    result_o[...] = resid[...] + parts[head]
    reduce.finish()
    for j in range(1, seqs):

        @pl.when(seq - j >= 0)
        def _():
            state_copy(seq, j, seq - j).wait_send()

    final.wait_send()
    remote(now, out_o.at[theirs], f_send, f_recv, partner, head).wait_recv()
    put.wait()


def DI_TOTAL(heads, chans):
    return float(heads * chans)


def backward(proj, kept, out_w, resid, conv_p, head_p, chan_p, expand, seqs, heads):
    (cot_hi, cot_lo, conv, cum, step, state, mixed, cross, stat, edge) = kept
    tokens, pad = proj.shape
    chunk, width = resid.shape
    chans = out_w.shape[0]
    ins = inner_count(heads)
    outs = heads // ins
    wide = chans + 2 * NSTATE
    blocks = tokens // BLOCK
    half = chans // 2
    rounds = (seqs // 2).bit_length() - 1
    anywhere = pl.BlockSpec(memory_space=pl.ANY)
    local = pl.BlockSpec(memory_space=pltpu.VMEM)
    sems = pltpu.SemaphoreType.DMA
    shape = jax.ShapeDtypeStruct
    return pl.pallas_call(
        functools.partial(backward_kernel, (seqs, heads, chunk, chans, pad)),
        out_shape=(
            shape((chunk, width), F32),
            shape((tokens, pad), BF16),
            shape((tokens, pad), BF16),
            shape((chans, width), F32),
            shape((8, wide), F32),
            shape((8, chans), F32),
            shape((8, 128), F32),
        ),
        in_specs=[anywhere] * 4 + [local] * 7 + [anywhere] + [local] * 5,
        out_specs=(local, local, local, anywhere, local, local, local),
        scratch_shapes=[
            pltpu.VMEM((8 + tokens, pad), F32),
            pltpu.VMEM((tokens, chans), BF16),
            pltpu.VMEM((tokens, chans), BF16),
            pltpu.VMEM((chans, width), BF16),
            pltpu.VMEM((chans, width), BF16),
            pltpu.VMEM((tokens, chans), F32),
            pltpu.VMEM((tokens, chans), F32),
            pltpu.VMEM((blocks, chans, NSTATE), F32),
            pltpu.VMEM((chans, NSTATE), F32),
            pltpu.VMEM((seqs, chans + 8, NSTATE), F32),
            pltpu.VMEM((tokens + 8, wide), F32),
            pltpu.VMEM((heads, chunk, width), F32),
            pltpu.VMEM((outs * (ins - 1), chunk, width), F32),
            pltpu.VMEM((outs + 1, chunk, width), F32),
            pltpu.VMEM((tokens, width // 2), BF16),
            pltpu.VMEM((tokens, width // 2), BF16),
            pltpu.VMEM((chans, width), F32),
            pltpu.VMEM((half, width), F32),
            pltpu.VMEM((half, width), F32),
            pltpu.VMEM((rounds, half, width), F32),
            pltpu.VMEM((8, 128), F32),
            sems((outs * (ins - 1),)),
            sems((outs * (ins - 1),)),
            sems((outs,)),
            sems((outs + 1,)),
            sems((5,)),
            sems((seqs - 1,)),
            sems((seqs - 1,)),
            sems,
            sems,
            sems,
            sems,
            sems((rounds,)),
            sems((rounds,)),
            sems,
            sems,
            sems,
        ],
        compiler_params=pltpu.CompilerParams(
            collective_id=4, has_side_effects=True, vmem_limit_bytes=VMEM_LIMIT
        ),
        name="backward",
    )(
        proj, edge, cot_hi, cot_lo, conv, cum, step, state, mixed, cross, stat,
        out_w, resid, conv_p, head_p, chan_p, expand,
    )


def on_device(
    residual_in,
    norm_gain,
    gate_weight,
    inner_weight,
    bc_weight,
    step_weight,
    conv_inner_weight,
    conv_inner_bias,
    conv_bc_weight,
    conv_bc_bias,
    step_bias,
    decay_log,
    skip_gain,
    gated_gain,
    out_weight,
    cotangent,
):
    seqs, heads = lax.axis_size("seq"), lax.axis_size("head")
    width = residual_in.shape[2]
    chans = gate_weight.shape[0]
    heads_here = step_weight.shape[0]
    spare = 128 - heads_here
    resid = residual_in.reshape(-1, width)
    cot = cotangent.reshape(-1, width)
    gain = norm_gain.reshape(1, width)

    def eight(part):
        return jnp.pad(part, ((0, 8 - part.shape[0]), (0, 0)))

    def by_head(*parts):
        return eight(jnp.pad(jnp.stack(parts), ((0, 0), (0, spare))))

    conv_p = eight(
        jnp.concatenate(
            [
                jnp.concatenate([conv_inner_weight, conv_bc_weight], 1),
                jnp.concatenate([conv_inner_bias, conv_bc_bias])[None],
            ],
            0,
        )
    )
    head_p = by_head(step_bias, -jnp.exp(decay_log), jnp.ones_like(step_bias))
    chan_p = eight(jnp.stack([gated_gain, jnp.repeat(skip_gain, HEADDIM)]))
    expand = (
        lax.broadcasted_iota(jnp.int32, (128, chans), 0)
        == lax.broadcasted_iota(jnp.int32, (128, chans), 1) // HEADDIM
    ).astype(F32)
    hat_hi, hat_lo, projected, weight_hi, weight_lo = gather_project(
        resid,
        gain,
        gate_weight,
        inner_weight,
        bc_weight,
        jnp.pad(step_weight, ((0, spare), (0, 0))),
        heads,
    )
    kept = forward(projected, cot, out_weight, conv_p, head_p, chan_p, expand, seqs, heads)
    result, grad_hi, grad_lo, out_weight_grad, wide_sums, chan_sums, head_sums = backward(
        projected, kept, out_weight, resid, conv_p, head_p, chan_p, expand, seqs, heads
    )

    def packed(*parts):
        flat = jnp.concatenate([part.reshape(-1) for part in parts])
        count = -(-flat.shape[0] // width)
        return jnp.pad(flat, (0, count * width - flat.shape[0])).reshape(count, width)

    seq_small = packed(
        wide_sums[:WIDTH, :chans],
        wide_sums[WIDTH, :chans],
        chan_sums[0],
        head_sums[0, :heads_here],
        head_sums[1, :heads_here],
        jnp.sum(chan_sums[1].reshape(heads_here, HEADDIM), axis=1),
    )
    all_small = packed(wide_sums[: WIDTH + 1, chans:])
    small = jnp.stack(
        [
            jnp.zeros((8, width), F32),
            eight(seq_small),
            eight(jnp.concatenate([jnp.zeros((1, width), F32), all_small], 0)),
        ]
    )
    residual_grad, gate_weight_grad, inner_weight_grad, bc_pieces, sums = tail(
        (grad_hi, grad_lo),
        (hat_hi, hat_lo),
        (weight_hi, weight_lo),
        small,
        resid,
        cot,
        gain,
        seqs,
        heads,
        chans,
    )
    across = width // bc_pieces.shape[2]
    bc_weight_grad = jnp.transpose(
        bc_pieces.reshape(2 * NSTATE // 8, across, 8, width // across), (1, 3, 0, 2)
    ).reshape(width, 2 * NSTATE)
    flat = sums[1].reshape(-1)

    def take(count):
        nonlocal flat
        first, flat = flat[:count], flat[count:]
        return first

    conv_inner_weight_grad = take(WIDTH * chans).reshape(WIDTH, chans)
    conv_inner_bias_grad = take(chans)
    gated_gain_grad = take(chans)
    step_bias_grad = take(heads_here)
    decay_log_grad = take(heads_here)
    skip_gain_grad = take(heads_here)
    flat = sums[2, 1:].reshape(-1)
    conv_bc_weight_grad = take(WIDTH * 2 * NSTATE).reshape(WIDTH, 2 * NSTATE)
    conv_bc_bias_grad = take(2 * NSTATE)
    return (
        result.reshape(residual_in.shape),
        residual_grad.reshape(residual_in.shape),
        sums[2, 0],
        gate_weight_grad,
        inner_weight_grad,
        bc_weight_grad,
        sums[0, :heads_here],
        conv_inner_weight_grad,
        conv_inner_bias_grad,
        conv_bc_weight_grad,
        conv_bc_bias_grad,
        step_bias_grad,
        decay_log_grad,
        skip_gain_grad,
        gated_gain_grad,
        out_weight_grad,
    )


def solution(mesh):
    placed = (
        P(None, ("seq", "head"), None),
        P(),
        P("head", None),
        P("head", None),
        P(),
        P("head", None),
        P(None, "head"),
        P("head"),
        P(),
        P(),
        P("head"),
        P("head"),
        P("head"),
        P("head"),
        P("head", None),
        P(None, ("seq", "head"), None),
    )
    return jax.shard_map(
        on_device,
        mesh=mesh,
        in_specs=placed,
        out_specs=(
            P(None, ("seq", "head"), None),
            P(None, ("seq", "head"), None),
            P(),
            P("head", None),
            P("head", None),
            P(),
            P("head", None),
            P(None, "head"),
            P("head"),
            P(),
            P(),
            P("head"),
            P("head"),
            P("head"),
            P("head"),
            P("head", None),
        ),
        check_vma=False,
    )
```

```python
import functools

import jax
import jax.numpy as jnp
from jax import lax
from jax.experimental import pallas as pl
from jax.experimental.pallas import tpu as pltpu
from jax.sharding import PartitionSpec as P

HEADDIM = 64
NSTATE = 128
WIDTH = 4
BLOCK = 256
EPSILON = 1e-05
EXACT = lax.Precision.HIGHEST
MESH = pl.DeviceIdType.MESH
F32 = jnp.float32
BF16 = jnp.bfloat16
VMEM_LIMIT = 66000000


def dot3(left, right, left_dim, right_dim):
    dims = (((left_dim,), (right_dim,)), ((), ()))
    one = functools.partial(lax.dot_general, dimension_numbers=dims, preferred_element_type=F32)
    return one(left[0], right[0]) + (one(left[0], right[1]) + one(left[1], right[0]))


def remote(source, target, send_sem, recv_sem, seq, head):
    return pltpu.make_async_remote_copy(
        src_ref=source,
        dst_ref=target,
        send_sem=send_sem,
        recv_sem=recv_sem,
        device_id=(seq, head),
        device_id_type=MESH,
    )


def greet(seq, head, seqs, heads):
    barrier = pltpu.get_barrier_semaphore()
    for j in range(1, seqs):
        pl.semaphore_signal(
            barrier, inc=1, device_id=(lax.rem(seq + j, seqs), head), device_id_type=MESH
        )
    for j in range(1, heads):
        pl.semaphore_signal(
            barrier, inc=1, device_id=(seq, lax.rem(head + j, heads)), device_id_type=MESH
        )
    pl.semaphore_wait(barrier, seqs + heads - 2)


def inner_count(heads):
    return 2 if heads <= 8 else 4


class SeqSum:
    def __init__(self, source, base, keep, core_in, x_in, sems, result, seq, head, seqs):
        self.source, self.base, self.keep, self.core_in, self.x_in = source, base, keep, core_in, x_in
        self.sems, self.result, self.seq, self.head = sems, result, seq, head
        self.rounds = (seqs // 2).bit_length() - 1
        self.half = keep.shape[0]
        self.side = lax.rem(seq, 2)
        self.partner = seq + 1 - 2 * self.side
        self.crossing = []

    def rows(self, side, base):
        return pl.ds(pl.multiple_of(base + side * self.half, 8), self.half)

    def begin(self):
        self.keep[...] = self.source[self.rows(self.side, self.base), :]
        self.core = remote(
            self.source.at[self.rows(1 - self.side, self.base)],
            self.core_in,
            self.sems.at[0],
            self.sems.at[1],
            self.partner,
            self.head,
        )
        self.core.start()

    def cross(self, source, turn):
        away = 2 << turn
        far = self.seq + away - 2 * away * lax.rem(self.seq // away, 2)
        self.crossing.append(
            remote(
                source,
                self.x_in.at[turn],
                self.sems.at[5 + 2 * turn],
                self.sems.at[6 + 2 * turn],
                far,
                self.head,
            )
        )
        self.crossing[-1].start()

    def pair(self):
        self.core.wait()
        self.keep[...] = self.keep[...] + self.core_in[...]
        self.cross(self.keep, 0)

    def total(self):
        now, new = self.keep, self.core_in
        for turn in range(self.rounds):
            self.crossing[turn].wait()
            new[...] = now[...] + self.x_in[turn]
            now, new = new, now
            if turn + 1 < self.rounds:
                self.cross(now, turn + 1)
        mine = self.result.at[self.rows(self.side, 0)]
        self.now = now
        self.put = pltpu.make_async_copy(now, mine, self.sems.at[2])
        self.put.start()
        self.final = remote(
            now, mine, self.sems.at[3], self.sems.at[4], self.partner, self.head
        )
        self.final.start()

    def end(self):
        self.final.wait_send()
        remote(
            self.now,
            self.result.at[self.rows(1 - self.side, 0)],
            self.sems.at[3],
            self.sems.at[4],
            self.partner,
            self.head,
        ).wait_recv()
        self.put.wait()


def seq_sum_scratch(half, width, rounds):
    return [
        pltpu.VMEM((half, width), F32),
        pltpu.VMEM((half, width), F32),
        pltpu.VMEM((rounds, half, width), F32),
        pltpu.SemaphoreType.DMA((5 + 2 * rounds,)),
    ]


def tail_kernel(dims, *refs):
    seqs, heads, chunk, chans, pad = dims
    (
        gp_hi, gp_lo, hat_hi, hat_lo, w_hi, w_lo, small_in, resid, cot, gain,
        resid_grad, inner_out, bc_out, small_out,
        gph, gpl, hth, htl, wh, wl, parts, y_in, z_in, joined, keep, core_in, x_in, i_sems,
        bc_part, bc_half, bc_seq, bc_quart, bc_head, bc_full,
        small_mine, small_pair, small_far, small_head,
        load_sem, y_send, y_recv, z_send, z_recv,
        a_sem, b_send, b_recv, c_send, c_recv, m_sem, h_send, h_recv, put_sem,
    ) = refs
    width = gain.shape[1]
    span = 2 * chans
    fars = seqs // 2
    seq, head = lax.axis_index("seq"), lax.axis_index("head")
    side, far = lax.rem(seq, 2), seq // 2
    partner = seq + 1 - 2 * side
    loads = [
        pltpu.make_async_copy(a, b, load_sem.at[n])
        for n, (a, b) in enumerate(
            ((gp_hi, gph), (w_hi, wh), (gp_lo, gpl), (w_lo, wl), (hat_hi, hth), (hat_lo, htl))
        )
    ]
    for load in loads:
        load.start()
    greet(seq, head, seqs, heads)
    reduce = LineReduce(
        parts, y_in, z_in, (y_send, y_recv, z_send, z_recv), seq, head, heads, partner
    )
    for load in loads[:4]:
        load.wait()

    def chunk_rows(where):
        return pl.ds(pl.multiple_of(where * chunk, 8), chunk)

    ins = reduce.ins

    def produce(step):
        first = reduce.target(step) * ins
        rows = pl.ds(pl.multiple_of(first * chunk, 8), ins * chunk)
        out = dot3((gph[rows, :], gpl[rows, :]), (wh[...], wl[...]), 1, 0)
        for n in range(ins):
            parts[first + n] = out[n * chunk : (n + 1) * chunk]

    produce(jnp.int32(0))
    reduce.give(jnp.int32(0))
    reduce.give(jnp.int32(1))
    gain_row = gain[...]
    for load in loads[4:]:
        load.wait()

    joined[span:, :] = (
        dot3((gph[:, span:], gpl[:, span:]), (hth[...], htl[...]), 0, 0) * gain_row
    )
    pieces, _, lanes = bc_part.shape
    across = width // lanes
    for row in range(pieces // across):
        for col in range(across):
            bc_part[row * across + col] = joined[
                span + row * 8 : span + row * 8 + 8, col * lanes : (col + 1) * lanes
            ]
    mine = pl.ds(side * (pieces // 2), pieces // 2)
    theirs = pl.ds((1 - side) * (pieces // 2), pieces // 2)
    bc_core = remote(
        bc_part.at[theirs], bc_half, a_sem.at[0], a_sem.at[1], partner, head
    )
    bc_core.start()
    low = chans if chans % 128 == 0 else 0
    rows = dot3((gph[:, low:span], gpl[:, low:span]), (hth[...], htl[...]), 0, 0)
    joined[low:span, :] = rows * gain_row
    inner = SeqSum(
        joined, chans, keep, core_in, x_in, i_sems, inner_out, seq, head, seqs
    )
    inner.begin()
    bc_core.wait()
    bc_half[...] = bc_half[...] + bc_part[mine]

    def others(make):
        copies = []
        for j in range(1, fars):
            copies.append(make(j, lax.rem(far + j, fars)))
            copies[-1].start()
        return copies

    cross_bc = others(
        lambda j, to: remote(
            bc_half.at[pl.ds(to * heads, heads)],
            bc_seq.at[j - 1],
            b_send.at[0, j - 1],
            b_recv.at[0, j - 1],
            2 * to + side,
            head,
        )
    )
    @pl.loop(1, reduce.outs)
    def _(step):
        produce(step)

    inner.pair()

    small_mine[...] = small_in[...]

    @pl.loop(0, heads)
    def _(where):
        rows = chunk_rows(where)
        hat = hth[rows, :].astype(F32) + htl[rows, :].astype(F32)
        small_mine[2, 0:1, :] = small_mine[2, 0:1, :] + jnp.sum(
            parts[where] * hat, 0, keepdims=True
        )

    reduce.reduce(0)
    small_mine[0] = joined[span + 2 * NSTATE : span + 2 * NSTATE + 8, :]
    small_core = remote(
        small_mine, small_pair, a_sem.at[2], a_sem.at[3], partner, head
    )
    small_core.start()
    for copy in cross_bc:
        copy.wait()
    quarter = bc_half[pl.ds(far * heads, heads)]
    for j in range(fars - 1):
        quarter = quarter + bc_seq[j]
    bc_quart[...] = quarter

    def to_heads(make):
        copies = []
        for j in range(1, heads):
            copies.append(make(j, lax.rem(head + j, heads)))
            copies[-1].start()
        return copies

    spread_bc = to_heads(
        lambda j, to: remote(
            bc_quart.at[to], bc_head.at[j - 1], c_send.at[0, j - 1], c_recv.at[0, j - 1], seq, to
        )
    )
    reduce.reduce(1)
    small_core.wait()
    small_far[far] = small_mine[...] + small_pair[...]
    cross_small = others(
        lambda j, to: remote(
            small_far.at[far],
            small_far.at[far],
            m_sem.at[0, j - 1],
            m_sem.at[1, j - 1],
            2 * to + side,
            head,
        )
    )
    reduce.reduce(2)
    reduce.reduce(3)
    for copy in spread_bc:
        copy.wait()
    piece = bc_quart[head]
    for j in range(heads - 1):
        piece = piece + bc_head[j]
    block = side * (pieces // 2) + far * heads
    bc_full[block + head] = piece
    gather_bc = to_heads(
        lambda j, to: remote(
            bc_full.at[block + head],
            bc_full.at[block + head],
            c_send.at[1, j - 1],
            c_recv.at[1, j - 1],
            seq,
            to,
        )
    )
    for j in range(1, fars):
        came = lax.rem(far - j + fars, fars)
        remote(
            small_far.at[came], small_far.at[came], m_sem.at[0, j - 1], m_sem.at[1, j - 1],
            partner, head,
        ).wait_recv()
    total = small_far[0]
    for j in range(1, fars):
        total = total + small_far[j]
    small_out[...] = total
    small_head[head] = total[2]
    spread_small = to_heads(
        lambda j, to: remote(
            small_head.at[head], small_head.at[head], h_send.at[j - 1], h_recv.at[j - 1], seq, to
        )
    )
    reduce.reduce(4)
    reduce.reduce(5)
    for j in range(1, heads):
        came = lax.rem(head - j + heads, heads)
        remote(
            bc_full.at[block + came], bc_full.at[block + came],
            c_send.at[1, j - 1], c_recv.at[1, j - 1], partner, head,
        ).wait_recv()
    reduce.reduce(6)
    own_block = pl.ds(block, heads)
    join_bc = others(
        lambda j, to: remote(
            bc_full.at[own_block],
            bc_full.at[own_block],
            b_send.at[1, j - 1],
            b_recv.at[1, j - 1],
            2 * to + side,
            head,
        )
    )
    for j in range(1, heads):
        came = lax.rem(head - j + heads, heads)
        remote(
            small_head.at[came], small_head.at[came], h_send.at[j - 1], h_recv.at[j - 1], seq, came
        ).wait_recv()
    total = small_head[0]
    for j in range(1, heads):
        total = total + small_head[j]
    small_out[2] = total
    for j in range(1, fars):
        came = side * (pieces // 2) + lax.rem(far - j + fars, fars) * heads
        came = pl.ds(came, heads)
        remote(
            bc_full.at[came], bc_full.at[came], b_send.at[1, j - 1], b_recv.at[1, j - 1],
            partner, head,
        ).wait_recv()
    join_core = remote(
        bc_full.at[mine], bc_full.at[mine], a_sem.at[4], a_sem.at[5], partner, head
    )
    join_core.start()
    inner.total()
    reduce.reduce(7)
    reduce.last()
    grad_hat = parts[head] * gain_row
    values = resid[...]
    scale = lax.rsqrt(jnp.mean(values * values, axis=1, keepdims=True) + EPSILON)
    row_cross = jnp.sum(grad_hat * values, axis=1, keepdims=True)
    resid_grad[...] = (
        cot[...] + scale * grad_hat - values * (scale * scale * scale * (row_cross / width))
    )
    remote(
        bc_full.at[theirs], bc_full.at[theirs], a_sem.at[4], a_sem.at[5], partner, head
    ).wait_recv()
    bc_put = pltpu.make_async_copy(bc_full, bc_out, put_sem)
    bc_put.start()
    reduce.finish()
    for copy in gather_bc + cross_small + spread_small + join_bc + [join_core]:
        copy.wait_send()
    inner.end()
    bc_put.wait()


def tail(gp, hat, weight, small, resid, cot, gain, seqs, heads, chans):
    tokens, width = hat[0].shape
    chunk = tokens // heads
    pad = gp[0].shape[1]
    ins = inner_count(heads)
    outs = heads // ins
    rounds = (seqs // 2).bit_length() - 1
    fars = seqs // 2
    lanes = 2 * NSTATE * width // (8 * seqs * heads)
    pieces = seqs * heads
    anywhere = pl.BlockSpec(memory_space=pl.ANY)
    local = pl.BlockSpec(memory_space=pltpu.VMEM)
    sems = pltpu.SemaphoreType.DMA
    return pl.pallas_call(
        functools.partial(tail_kernel, (seqs, heads, chunk, chans, pad)),
        out_shape=(
            jax.ShapeDtypeStruct((chunk, width), F32),
            jax.ShapeDtypeStruct((chans, width), F32),
            jax.ShapeDtypeStruct((pieces, 8, lanes), F32),
            jax.ShapeDtypeStruct((3, 8, width), F32),
        ),
        in_specs=[anywhere] * 6 + [local] * 4,
        out_specs=(local, anywhere, anywhere, local),
        scratch_shapes=[
            pltpu.VMEM((tokens, pad), BF16),
            pltpu.VMEM((tokens, pad), BF16),
            pltpu.VMEM((tokens, width), BF16),
            pltpu.VMEM((tokens, width), BF16),
            pltpu.VMEM((pad, width), BF16),
            pltpu.VMEM((pad, width), BF16),
            pltpu.VMEM((heads, chunk, width), F32),
            pltpu.VMEM((outs * (ins - 1), chunk, width), F32),
            pltpu.VMEM((outs + 1, chunk, width), F32),
            pltpu.VMEM((pad, width), F32),
            *seq_sum_scratch(chans // 2, width, rounds),
            pltpu.VMEM((pieces, 8, lanes), F32),
            pltpu.VMEM((pieces // 2, 8, lanes), F32),
            pltpu.VMEM((fars - 1, heads, 8, lanes), F32),
            pltpu.VMEM((heads, 8, lanes), F32),
            pltpu.VMEM((heads - 1, 8, lanes), F32),
            pltpu.VMEM((pieces, 8, lanes), F32),
            pltpu.VMEM((3, 8, width), F32),
            pltpu.VMEM((3, 8, width), F32),
            pltpu.VMEM((fars, 3, 8, width), F32),
            pltpu.VMEM((heads, 8, width), F32),
            sems((6,)),
            *line_reduce_sems(ins, outs),
            sems((6,)),
            sems((2, fars - 1)),
            sems((2, fars - 1)),
            sems((2, heads - 1)),
            sems((2, heads - 1)),
            sems((2, fars - 1)),
            sems((heads - 1,)),
            sems((heads - 1,)),
            sems,
        ],
        compiler_params=pltpu.CompilerParams(
            collective_id=1, has_side_effects=True, vmem_limit_bytes=VMEM_LIMIT
        ),
        name="tail",
    )(*gp, *hat, *weight, small, resid, cot, gain)


def head_kernel(dims, *refs):
    heads, chunk, chans, pad = dims
    (
        rows, gain, gate_w, inner_w, bc_w, step_w,
        hat_hi, hat_lo, proj_out, w_hi, w_lo,
        parts, hth, htl, proj, raw, wh, wl, wth, wtl,
        load_sem, z_send, z_recv, y_send, y_recv, put_sem,
    ) = refs
    width = gain.shape[1]
    ins = inner_count(heads)
    outs = heads // ins
    span = 2 * chans
    seq, head = lax.axis_index("seq"), lax.axis_index("head")
    at_out, at_in = head // ins, lax.rem(head, ins)

    loads = [
        pltpu.make_async_copy(gate_w, raw.at[pl.ds(0, chans)], load_sem.at[0]),
        pltpu.make_async_copy(inner_w, raw.at[pl.ds(chans, chans)], load_sem.at[1]),
    ]
    for load in loads:
        load.start()
    greet(seq, head, 1, heads)
    values = rows[...]
    parts[head] = values * lax.rsqrt(
        jnp.mean(values * values, axis=1, keepdims=True) + EPSILON
    )

    def z_copy(where, up):
        return remote(
            parts.at[where],
            parts.at[where],
            z_send.at[where // ins, up],
            z_recv.at[where // ins],
            seq,
            (at_out + 2 * up - 1) * ins + at_in,
        )

    def y_copy(where, j, to):
        return remote(
            parts.at[where],
            parts.at[where],
            y_send.at[where // ins, j],
            y_recv.at[where // ins, j],
            seq,
            at_out * ins + to,
        )

    def arrived(place, distance, first):
        where = place * ins + at_in

        @pl.when(distance > 0)
        def _():
            z_copy(where, 0).wait_recv()

        @pl.when((place >= at_out) & (at_out > 0))
        def _():
            z_copy(where, 0).start()

        @pl.when((place <= at_out) & (at_out < outs - 1))
        def _():
            z_copy(where, 1).start()

        for j in range(ins - 1):
            y_copy(where, j, lax.rem(at_in + 1 + j, ins)).start()

    arrived(at_out, 0, True)

    raw[span : span + 2 * NSTATE, :] = bc_w[...].T
    raw[span + 2 * NSTATE :, :] = step_w[...]
    for load in loads:
        load.wait()
    gain_row = gain[...]

    @pl.loop(0, pad // 128)
    def _(block):
        here = pl.ds(pl.multiple_of(block * 128, 128), 128)
        piece = raw[here, :]
        top = piece.astype(BF16)
        wh[here, :] = top
        wl[here, :] = (piece - top.astype(F32)).astype(BF16)
        turned = (piece * gain_row).T
        top = turned.astype(BF16)
        wth[:, here] = top
        wtl[:, here] = (turned - top.astype(F32)).astype(BF16)

    puts = [
        pltpu.make_async_copy(wh, w_hi, put_sem.at[0]),
        pltpu.make_async_copy(wl, w_lo, put_sem.at[1]),
    ]
    for put in puts:
        put.start()

    def chunk_rows(where):
        return pl.ds(pl.multiple_of(where * chunk, 8), chunk)

    def chunk_puts(where):
        here = chunk_rows(where)
        return [
            pltpu.make_async_copy(hth.at[where], hat_hi.at[here], put_sem.at[2 + 3 * where]),
            pltpu.make_async_copy(htl.at[where], hat_lo.at[here], put_sem.at[3 + 3 * where]),
            pltpu.make_async_copy(proj.at[where], proj_out.at[here], put_sem.at[4 + 3 * where]),
        ]

    def project(where):
        piece = parts[where]
        top = piece.astype(BF16)
        low = (piece - top.astype(F32)).astype(BF16)
        hth[where] = top
        htl[where] = low
        proj[where] = dot3((top, low), (wth[...], wtl[...]), 1, 0)
        for put in chunk_puts(where):
            put.start()

    @pl.loop(0, outs + 1)
    def _(distance):
        for side in range(2):
            place = at_out + (2 * side - 1) * distance

            @pl.when((distance > 0) & (place >= 0) & (place < outs))
            def _():
                arrived(place, distance, False)

        @pl.loop(0, 2 * ins)
        def _(n):
            side, j = n // ins, lax.rem(n, ins)
            late = (j + ins - 1) // ins
            away = distance - late
            place = at_out + (2 * side - 1) * away

            @pl.when(
                (place >= 0) & (place < outs) & (away >= 0) & (away + 1 - side > 0)
            )
            def _():
                frm = lax.rem(at_in + ins - j, ins)
                where = place * ins + frm

                @pl.when(j > 0)
                def _():
                    y_copy(where, j - 1, lax.rem(at_in + 1, ins)).wait_recv()

                project(where)

    for place in range(outs):
        where = place * ins + at_in

        @pl.when((place >= at_out) & (at_out > 0))
        def _():
            z_copy(where, 0).wait_send()

        @pl.when((place <= at_out) & (at_out < outs - 1))
        def _():
            z_copy(where, 1).wait_send()

        for j in range(ins - 1):
            y_copy(where, j, lax.rem(at_in + 1 + j, ins)).wait_send()
    for put in puts:
        put.wait()

    @pl.loop(0, heads)
    def _(where):
        for put in chunk_puts(where):
            put.wait()


def gather_project(resid, gain, gate_w, inner_w, bc_w, step_w, heads):
    chunk, width = resid.shape
    chans = gate_w.shape[0]
    pad = 2 * chans + 2 * NSTATE + 128
    ins = inner_count(heads)
    outs = heads // ins
    tokens = chunk * heads
    anywhere = pl.BlockSpec(memory_space=pl.ANY)
    local = pl.BlockSpec(memory_space=pltpu.VMEM)
    sems = pltpu.SemaphoreType.DMA
    shape = jax.ShapeDtypeStruct
    return pl.pallas_call(
        functools.partial(head_kernel, (heads, chunk, chans, pad)),
        out_shape=(
            shape((tokens, width), BF16),
            shape((tokens, width), BF16),
            shape((tokens, pad), F32),
            shape((pad, width), BF16),
            shape((pad, width), BF16),
        ),
        in_specs=[local, local, anywhere, anywhere, local, local],
        out_specs=(anywhere,) * 5,
        scratch_shapes=[
            pltpu.VMEM((heads, chunk, width), F32),
            pltpu.VMEM((heads, chunk, width), BF16),
            pltpu.VMEM((heads, chunk, width), BF16),
            pltpu.VMEM((heads, chunk, pad), F32),
            pltpu.VMEM((pad, width), F32),
            pltpu.VMEM((pad, width), BF16),
            pltpu.VMEM((pad, width), BF16),
            pltpu.VMEM((width, pad), BF16),
            pltpu.VMEM((width, pad), BF16),
            sems((2,)),
            sems((outs, 2)),
            sems((outs,)),
            sems((outs, ins - 1)),
            sems((outs, ins - 1)),
            sems((2 + 3 * heads,)),
        ],
        compiler_params=pltpu.CompilerParams(
            collective_id=2, has_side_effects=True, vmem_limit_bytes=VMEM_LIMIT
        ),
        name="gather_project",
    )(resid, gain, gate_w, inner_w, bc_w, step_w)


def dotx(left, right, left_dim, right_dim):
    return lax.dot_general(
        left,
        right,
        (((left_dim,), (right_dim,)), ((), ())),
        precision=EXACT,
        preferred_element_type=F32,
    )


def halves(values):
    top = values.astype(BF16)
    return (top, (values - top.astype(F32)).astype(BF16))


class LineGather:
    def __init__(self, parts, sems, seq, head, heads):
        self.parts, self.seq, self.heads = parts, seq, heads
        self.z_send, self.z_recv, self.y_send, self.y_recv = sems
        self.ins = inner_count(heads)
        self.outs = heads // self.ins
        self.at_out, self.at_in = head // self.ins, lax.rem(head, self.ins)

    def z_copy(self, where, up):
        place = where // self.ins
        return remote(
            self.parts.at[where],
            self.parts.at[where],
            self.z_send.at[place, up],
            self.z_recv.at[place],
            self.seq,
            (self.at_out + 2 * up - 1) * self.ins + self.at_in,
        )

    def y_copy(self, where, j, to):
        place = where // self.ins
        return remote(
            self.parts.at[where],
            self.parts.at[where],
            self.y_send.at[place, j],
            self.y_recv.at[place, j],
            self.seq,
            self.at_out * self.ins + to,
        )

    def arrived(self, place, wait):
        where = place * self.ins + self.at_in
        if wait:
            self.z_copy(where, 0).wait_recv()

        @pl.when((place >= self.at_out) & (self.at_out > 0))
        def _():
            self.z_copy(where, 0).start()

        @pl.when((place <= self.at_out) & (self.at_out < self.outs - 1))
        def _():
            self.z_copy(where, 1).start()

        for j in range(self.ins - 1):
            self.y_copy(where, j, lax.rem(self.at_in + 1 + j, self.ins)).start()

    def start(self):
        self.arrived(self.at_out, False)

    def relay(self, distance):
        for side in range(2):
            place = self.at_out + (2 * side - 1) * distance

            @pl.when((place >= 0) & (place < self.outs))
            def _():
                self.arrived(place, True)

    def use(self, distance, consume):
        @pl.loop(0, 2 * self.ins)
        def _(n):
            side, j = n // self.ins, lax.rem(n, self.ins)
            late = (j + self.ins - 1) // self.ins
            away = distance - late
            place = self.at_out + (2 * side - 1) * away

            @pl.when(
                (place >= 0) & (place < self.outs) & (away >= 0) & (away + 1 - side > 0)
            )
            def _():
                where = place * self.ins + lax.rem(self.at_in + self.ins - j, self.ins)

                @pl.when(j > 0)
                def _():
                    self.y_copy(where, j - 1, lax.rem(self.at_in + 1, self.ins)).wait_recv()

                consume(where)

    def finish(self):
        for place in range(self.outs):
            where = place * self.ins + self.at_in

            @pl.when((place >= self.at_out) & (self.at_out > 0))
            def _():
                self.z_copy(where, 0).wait_send()

            @pl.when((place <= self.at_out) & (self.at_out < self.outs - 1))
            def _():
                self.z_copy(where, 1).wait_send()

            for j in range(self.ins - 1):
                self.y_copy(where, j, lax.rem(self.at_in + 1 + j, self.ins)).wait_send()


def lanes_of(chans):
    return [(lo, min(lo + 2 * HEADDIM, chans)) for lo in range(0, chans, 2 * HEADDIM)]


def spread(values, expand):
    top, low = halves(values)
    expand = expand.astype(BF16)
    dims = (((1,), (0,)), ((), ()))
    one = functools.partial(lax.dot_general, dimension_numbers=dims, preferred_element_type=F32)
    return one(top, expand) + one(low, expand)


def gather_heads(values, expand):
    top, low = halves(values)
    expand = expand.astype(BF16)
    dims = (((1,), (1,)), ((), ()))
    one = functools.partial(lax.dot_general, dimension_numbers=dims, preferred_element_type=F32)
    return one(top, expand) + one(low, expand)


def row_scale(total_row, expand):
    wide = jnp.broadcast_to(jnp.exp(total_row), (128, 128)).T
    return dotx(expand, wide, 0, 0)


def logistic(values):
    return 1.0 / (1.0 + jnp.exp(-values))


def decay_of(cum, cum_turned, h, causal):
    gap = cum[:, h : h + 1] - cum_turned[h : h + 1, :]
    return jnp.where(causal, jnp.exp(jnp.where(causal, gap, 0.0)), 0.0)


def forward_kernel(dims, *refs):
    seqs, heads, chunk, chans, pad = dims
    (
        proj, cot, out_w, conv_p, head_p, chan_p, expand_in,
        cot_hi, cot_lo, conv_hbm, cum_o, step_o, state_o, mixed_o, cross_o, stat_o, edge_o,
        parts, hi, lo, pj, conv_o, raw, owh, owl, scaled, enter, prefix, run, exch, stat_all, lows,
        z_send, z_recv, y_send, y_recv, load_sem, put_sem, e_send, e_recv,
        s_send, s_recv, t_send, t_recv,
    ) = refs
    tokens = chunk * heads
    blocks = tokens // BLOCK
    span = 2 * chans
    wide = chans + 2 * NSTATE
    here_heads = chans // HEADDIM
    seq, head = lax.axis_index("seq"), lax.axis_index("head")
    load = pltpu.make_async_copy(proj, pj.at[pl.ds(8, tokens)], load_sem.at[0])
    load.start()
    load_w = pltpu.make_async_copy(out_w, raw, load_sem.at[1])
    load_w.start()
    parts[head] = cot[...]
    greet(seq, head, seqs, heads)
    gather = LineGather(parts, (z_send, z_recv, y_send, y_recv), seq, head, heads)
    gather.start()
    edge = remote(
        proj.at[pl.ds(tokens - 8, 8)],
        pj.at[pl.ds(0, 8)],
        e_send,
        e_recv,
        lax.rem(seq + 1, seqs),
        head,
    )
    edge.start()
    load_w.wait()
    for lane, end in lanes_of(chans):
        owh[:, lane:end], owl[:, lane:end] = halves(raw[lane:end, :].T)
    expand = expand_in[...]
    load.wait()
    edge.wait()
    first = jnp.where(seq > 0, pj[0:8, :], 0.0)
    pj[0:8, :] = first
    edge_o[...] = first
    tri_r = lax.broadcasted_iota(jnp.int32, (BLOCK, BLOCK), 0)
    tri_c = lax.broadcasted_iota(jnp.int32, (BLOCK, BLOCK), 1)
    causal = tri_r >= tri_c
    lower = causal.astype(F32)
    run[...] = jnp.zeros_like(run)
    prefix[...] = jnp.zeros_like(prefix)

    @pl.loop(0, blocks)
    def _(b):
        at = pl.multiple_of(b * BLOCK, BLOCK)
        here = pl.ds(at, BLOCK)
        window = pj[pl.ds(at, BLOCK + 8), chans : span + 2 * NSTATE]
        conv = jnp.zeros((BLOCK, wide), F32) + conv_p[4:5, :]
        for k in range(WIDTH):
            conv = conv + conv_p[k : k + 1, :] * window[5 + k : 5 + k + BLOCK, :]
        conv_o[here, :] = conv
        act = conv * logistic(conv)
        arg = pj[pl.ds(at + 8, BLOCK), span + 2 * NSTATE : pad] + head_p[0:1, :]
        step = jnp.maximum(arg, 0.0) + jnp.log1p(jnp.exp(-jnp.abs(arg)))
        cum = dotx(lower, step * head_p[1:2, :], 1, 0)
        last = cum[BLOCK - 1 : BLOCK, :]
        step_o[here, :] = step
        cum_o[here, :] = cum
        fed = act[:, :chans] * spread(step, expand)
        scaled[here, :] = fed
        fresh = dotx(
            fed * spread(jnp.exp(last - cum), expand), act[:, chans : chans + NSTATE], 0, 0
        )
        enter[b] = run[...]
        run[...] = row_scale(last, expand) * run[...] + fresh
        prefix[pl.ds(b + 1, 1), :] = prefix[pl.ds(b, 1), :] + last

    gather.relay(1)
    conv_put = pltpu.make_async_copy(conv_o, conv_hbm, put_sem.at[2 * heads])
    conv_put.start()
    exch[seq, 0:chans, :] = run[...]
    exch[seq, chans : chans + 8, :] = jnp.broadcast_to(prefix[blocks : blocks + 1, :], (8, 128))

    def state_copy(at, j, to):
        return remote(exch.at[at], exch.at[at], s_send.at[j - 1], s_recv.at[j - 1], to, head)

    for j in range(1, seqs):

        @pl.when(seq + j < seqs)
        def _():
            state_copy(seq, j, seq + j).start()

    @pl.loop(0, blocks)
    def _(b):
        at = pl.multiple_of(b * BLOCK, BLOCK)
        here = pl.ds(at, BLOCK)
        bc = conv_o[here, chans:wide]
        bc = bc * logistic(bc)
        scores = dotx(bc[:, NSTATE:], bc[:, :NSTATE], 1, 1)
        cum = cum_o[here, :]
        turned = cum.T
        for first_lane, end in lanes_of(chans):
            fed = scaled[here, first_lane:end]
            outs = [
                dotx(decay_of(cum, turned, lane // HEADDIM, causal) * scores, fed, 1, 0)
                for lane in range(first_lane, end, HEADDIM)
            ]
            out = outs[0]
            if len(outs) == 2:
                lane = lax.broadcasted_iota(jnp.int32, out.shape, 1)
                out = jnp.where(lane < HEADDIM, outs[0], outs[1])
            mixed_o[here, first_lane:end] = out

    if gather.outs > 2:
        gather.relay(2)
    run[...] = jnp.zeros_like(run)
    for earlier in range(seqs - 1):

        @pl.when(earlier < seq)
        def _():
            for j in range(1, seqs):

                @pl.when(seq - earlier == j)
                def _():
                    state_copy(earlier, j, lax.rem(seq + 1, seqs)).wait_recv()

            run[...] = (
                row_scale(exch[earlier, chans : chans + 1, :], expand) * run[...]
                + exch[earlier, 0:chans, :]
            )

    @pl.loop(0, blocks)
    def _(b):
        at = pl.multiple_of(b * BLOCK, BLOCK)
        here = pl.ds(at, BLOCK)
        state = enter[b] + row_scale(prefix[pl.ds(b, 1), :], expand) * run[...]
        state_o[b] = state
        conv = conv_o[here, :]
        act = conv * logistic(conv)
        gate = pj[pl.ds(at + 8, BLOCK), 0:chans]
        carried = dotx(act[:, chans + NSTATE :], state, 1, 1)
        mixed = (
            mixed_o[here, :]
            + carried * spread(jnp.exp(cum_o[here, :]), expand)
            + chan_p[1:2, :] * act[:, :chans]
        )
        mixed_o[here, :] = mixed
        scaled[here, :] = mixed * gate * logistic(gate)

    for distance in range(3, gather.outs):
        gather.relay(distance)

    def chunk_puts(where):
        rows = pl.ds(pl.multiple_of(where * chunk, 8), chunk)
        return [
            pltpu.make_async_copy(hi.at[where], cot_hi.at[rows], put_sem.at[2 * where]),
            pltpu.make_async_copy(lo.at[where], cot_lo.at[rows], put_sem.at[2 * where + 1]),
        ]

    def consume(where):
        rows = pl.ds(pl.multiple_of(where * chunk, 8), chunk)
        top, low = halves(parts[where])
        hi[where] = top
        lo[where] = low
        cross_o[rows, :] = dot3((top, low), (owh[...], owl[...]), 1, 0)
        for put in chunk_puts(where):
            put.start()

    for distance in range(gather.outs + 1):
        gather.use(distance, consume)

    ones = jnp.ones((8, chans), F32)
    groups = tokens // 128
    for n in range(groups):
        here = slice(n * 128, n * 128 + 128)
        gated = scaled[here, :]
        lows[n : n + 1, :] = dotx(ones, gated * gated, 1, 1)[0:1, :]
        lows[groups + n : groups + n + 1, :] = dotx(
            ones, cross_o[here, :] * chan_p[0:1, :] * gated, 1, 1
        )[0:1, :]
    stat_all[head] = lows[...]
    sends = []
    for j in range(1, heads):
        sends.append(
            remote(
                stat_all.at[head],
                stat_all.at[head],
                t_send.at[j - 1],
                t_recv.at[j - 1],
                seq,
                lax.rem(head + j, heads),
            )
        )
        sends[-1].start()
    gather.finish()
    conv_put.wait()

    @pl.loop(0, heads)
    def _(where):
        for put in chunk_puts(where):
            put.wait()

    for j in range(1, seqs):

        @pl.when(seq + j < seqs)
        def _():
            state_copy(seq, j, seq + j).wait_send()

    for j in range(1, heads):
        came = lax.rem(head - j + heads, heads)
        remote(
            stat_all.at[came], stat_all.at[came], t_send.at[j - 1], t_recv.at[j - 1], seq, came
        ).wait_recv()
    total = stat_all[0]
    for j in range(1, heads):
        total = total + stat_all[j]
    stat_o[...] = total
    for copy in sends:
        copy.wait_send()


def forward(proj, cot, out_w, conv_p, head_p, chan_p, expand, seqs, heads):
    tokens, pad = proj.shape
    chunk, width = cot.shape
    chans = out_w.shape[0]
    ins = inner_count(heads)
    outs = heads // ins
    wide = chans + 2 * NSTATE
    blocks = tokens // BLOCK
    groups = 2 * tokens // 128
    anywhere = pl.BlockSpec(memory_space=pl.ANY)
    local = pl.BlockSpec(memory_space=pltpu.VMEM)
    sems = pltpu.SemaphoreType.DMA
    shape = jax.ShapeDtypeStruct
    return pl.pallas_call(
        functools.partial(forward_kernel, (seqs, heads, chunk, chans, pad)),
        out_shape=(
            shape((tokens, width), BF16),
            shape((tokens, width), BF16),
            shape((tokens, wide), F32),
            shape((tokens, 128), F32),
            shape((tokens, 128), F32),
            shape((blocks, chans, NSTATE), F32),
            shape((tokens, chans), F32),
            shape((tokens, chans), F32),
            shape((groups, 128), F32),
            shape((8, pad), F32),
        ),
        in_specs=[anywhere, local, anywhere, local, local, local, local],
        out_specs=(anywhere, anywhere, anywhere) + (local,) * 7,
        scratch_shapes=[
            pltpu.VMEM((heads, chunk, width), F32),
            pltpu.VMEM((heads, chunk, width), BF16),
            pltpu.VMEM((heads, chunk, width), BF16),
            pltpu.VMEM((8 + tokens, pad), F32),
            pltpu.VMEM((tokens, wide), F32),
            pltpu.VMEM((chans, width), F32),
            pltpu.VMEM((width, chans), BF16),
            pltpu.VMEM((width, chans), BF16),
            pltpu.VMEM((tokens, chans), F32),
            pltpu.VMEM((blocks, chans, NSTATE), F32),
            pltpu.VMEM((8, 128), F32),
            pltpu.VMEM((chans, NSTATE), F32),
            pltpu.VMEM((seqs, chans + 8, NSTATE), F32),
            pltpu.VMEM((heads, groups, 128), F32),
            pltpu.VMEM((groups, 128), F32),
            sems((outs, 2)),
            sems((outs,)),
            sems((outs, ins - 1)),
            sems((outs, ins - 1)),
            sems((2,)),
            sems((2 * heads + 1,)),
            sems,
            sems,
            sems((seqs - 1,)),
            sems((seqs - 1,)),
            sems((heads - 1,)),
            sems((heads - 1,)),
        ],
        compiler_params=pltpu.CompilerParams(
            collective_id=3, has_side_effects=True, vmem_limit_bytes=VMEM_LIMIT
        ),
        name="forward",
    )(proj, cot, out_w, conv_p, head_p, chan_p, expand)


class LineReduce:
    def __init__(self, parts, y_in, z_in, sems, seq, head, heads, partner):
        self.parts, self.y_in, self.z_in = parts, y_in, z_in
        self.y_send, self.y_recv, self.z_send, self.z_recv = sems
        self.seq, self.partner = seq, partner
        self.ins = inner_count(heads)
        self.outs = heads // self.ins
        self.half = parts.shape[1] // 2
        self.turns = 2 * self.outs
        self.at_out, self.at_in = head // self.ins, lax.rem(head, self.ins)
        self.upper = self.at_out // (self.outs // 2)
        self.mirrored = self.at_out + self.upper * (self.outs - 1 - 2 * self.at_out)

    def target(self, step):
        last = (step + 1) // self.outs
        far = self.outs - 1 - step
        far = far - (self.mirrored - far + self.outs) // self.outs
        far = far + self.upper * (self.outs - 1 - 2 * far)
        return far + last * (self.at_out - far)

    def rows(self, turn):
        return pl.ds(pl.multiple_of(lax.rem(turn, 2) * self.half, 8), self.half)

    def y_copy(self, turn, j):
        goal = self.target(turn // 2)
        to = lax.rem(self.at_in + 1 + j, self.ins)
        rows = self.rows(turn)
        return remote(
            self.parts.at[goal * self.ins + to, rows],
            self.y_in.at[goal * (self.ins - 1) + j, rows],
            self.y_send.at[turn, j],
            self.y_recv.at[turn, j],
            self.seq,
            self.at_out * self.ins + to,
        )

    def give(self, turn):
        for j in range(self.ins - 1):
            self.y_copy(turn, j).start()

    def take(self, turn, slot):
        rows = self.rows(turn)
        where = self.target(turn // 2) * self.ins + self.at_in
        remote(
            self.parts.at[0, rows],
            self.z_in.at[slot, rows],
            self.z_send.at[0],
            self.z_recv.at[slot, lax.rem(turn, 2)],
            self.partner,
            self.at_out * self.ins + self.at_in,
        ).wait_recv()
        self.parts[where, rows, :] = self.parts[where, rows, :] + self.z_in[slot, rows, :]

    def pass_on(self, turn, up):
        goal, rows = self.target(turn // 2), self.rows(turn)
        remote(
            self.parts.at[goal * self.ins + self.at_in, rows],
            self.z_in.at[goal + up, rows],
            self.z_send.at[turn],
            self.z_recv.at[goal + up, lax.rem(turn, 2)],
            self.seq,
            (self.at_out + 2 * up - 1) * self.ins + self.at_in,
        ).start()

    def across(self, turn):
        goal = self.target(turn // 2)
        rows = self.rows(turn)
        where = goal * self.ins + self.at_in
        for j in range(self.ins - 1):
            self.y_copy(turn, j).wait_recv()

        @pl.when(turn + 2 < self.turns)
        def _():
            self.give(turn + 2)

        for j in range(self.ins - 1):
            self.parts[where, rows, :] = (
                self.parts[where, rows, :] + self.y_in[goal * (self.ins - 1) + j, rows, :]
            )

        @pl.when((goal > self.at_out) & (self.at_out == 0))
        def _():
            self.pass_on(turn, 1)

        @pl.when((goal < self.at_out) & (self.at_out == self.outs - 1))
        def _():
            self.pass_on(turn, 0)

    def along(self, turn):
        goal = self.target(turn // 2)

        @pl.when((goal >= self.at_out) & (self.at_out > 0))
        def _():
            self.take(turn, goal + 1)

        @pl.when((goal <= self.at_out) & (self.at_out < self.outs - 1))
        def _():
            self.take(turn, goal)

        @pl.when((goal > self.at_out) & (self.at_out > 0))
        def _():
            self.pass_on(turn, 1)

        @pl.when((goal < self.at_out) & (self.at_out < self.outs - 1))
        def _():
            self.pass_on(turn, 0)

    def reduce(self, turn):
        turn = jnp.int32(turn)
        self.across(turn)

        @pl.when(turn > 0)
        def _():
            self.along(turn - 1)

    def last(self):
        self.along(jnp.int32(self.turns - 1))

    def finish(self):
        @pl.loop(0, self.turns)
        def _(turn):
            for j in range(self.ins - 1):
                self.y_copy(turn, j).wait_send()

        @pl.loop(0, self.turns - 2)
        def _(turn):
            rows = pl.ds(0, self.half)
            remote(
                self.parts.at[0, rows],
                self.z_in.at[0, rows],
                self.z_send.at[turn],
                self.z_recv.at[0, 0],
                self.partner,
                self.at_out * self.ins + self.at_in,
            ).wait_send()


def line_reduce_sems(ins, outs):
    sems = pltpu.SemaphoreType.DMA
    return [
        sems((2 * outs, ins - 1)),
        sems((2 * outs, ins - 1)),
        sems((2 * outs,)),
        sems((outs + 1, 2)),
    ]


def backward_kernel(dims, *refs):
    seqs, heads, chunk, chans, pad = dims
    (
        proj, edge_in, cot_hi, cot_lo, hat_hi, hat_lo, conv_in, cum_in, step_in, state_in, mixed_in, cross_in,
        stat_in, out_w, resid, conv_p, head_p, chan_p, gain, expand_in,
        result_o, gp_hi, gp_lo, out_o, gate_o, wide_o, chan_o, head_o,
        pj, ngh, ngl, owh, owl, gmix, fedg, adj, run, exch, gconv,
        parts, y_in, z_in, chi, clo, oparts, columns, conv_buf, head_acc,
        keep_o, core_o, x_o, o_sems, keep_g, core_g, x_g, g_sems,
        y_send, y_recv, z_send, z_recv, load_sem, s_send, s_recv, e_send, e_recv, conv_sem,
    ) = refs
    tokens = chunk * heads
    blocks = tokens // BLOCK
    span = 2 * chans
    wide = chans + 2 * NSTATE
    split_at = resid.shape[1] // 2
    seq, head = lax.axis_index("seq"), lax.axis_index("head")
    side = lax.rem(seq, 2)
    partner = seq + 1 - 2 * side
    loads = [
        pltpu.make_async_copy(a, b, load_sem.at[n])
        for n, (a, b) in enumerate(
            (
                (proj, pj.at[pl.ds(8, tokens)]),
                (edge_in, pj.at[pl.ds(0, 8)]),
                (cot_hi.at[:, pl.ds(0, split_at)], chi),
                (cot_lo.at[:, pl.ds(0, split_at)], clo),
                (out_w, oparts),
            )
        )
    ]
    for load in loads:
        load.start()
    greet(seq, head, seqs, heads)
    loads[4].wait()
    owh[...], owl[...] = halves(oparts[...])
    expand = expand_in[...]
    tri_r = lax.broadcasted_iota(jnp.int32, (BLOCK, BLOCK), 0)
    tri_c = lax.broadcasted_iota(jnp.int32, (BLOCK, BLOCK), 1)
    causal = tri_r >= tri_c
    upper = (tri_r <= tri_c).astype(F32)
    wide_o[...] = jnp.zeros_like(wide_o)
    chan_o[...] = jnp.zeros_like(chan_o)
    head_acc[...] = jnp.zeros_like(head_acc)
    run[...] = jnp.zeros_like(run)
    for load in loads[:2]:
        load.wait()
    groups = tokens // 128
    turned_stats = stat_in[...].T
    inner_total = float(heads * chans)
    gain_row, skip_row = chan_p[0:1, :], chan_p[1:2, :]
    for n in range(groups):
        here = slice(n * 128, n * 128 + 128)
        scale = lax.rsqrt(turned_stats[:, n : n + 1] / inner_total + EPSILON)
        cross = turned_stats[:, groups + n : groups + n + 1]
        columns[here, 0:1] = scale
        columns[here, 1:2] = scale * scale * scale * (cross / inner_total)

    def conv_load(b, slot):
        return pltpu.make_async_copy(
            conv_in.at[pl.ds(pl.multiple_of(b * BLOCK, BLOCK), BLOCK)],
            conv_buf.at[slot],
            conv_sem.at[slot],
        )

    def conv_of(n, b, following):
        slot = lax.rem(n, 2)
        conv_load(b, slot).wait()
        conv_load(following, 1 - slot).start()
        return conv_buf[slot]

    conv_load(blocks - 1, 0).start()

    @pl.loop(0, blocks)
    def _(b):
        at = pl.multiple_of(b * BLOCK, BLOCK)
        here = pl.ds(at, BLOCK)
        gate = pj[pl.ds(at + 8, BLOCK), 0:chans]
        ngh[here, :], ngl[here, :] = halves(
            mixed_in[here, :] * (gate * logistic(gate)) * columns[here, 0:1] * gain_row
        )

    reduce = LineReduce(
        parts, y_in, z_in, (y_send, y_recv, z_send, z_recv), seq, head, heads, partner
    )

    ins = reduce.ins

    def produce(step):
        first = reduce.target(step) * ins
        rows = pl.ds(pl.multiple_of(first * chunk, 8), ins * chunk)
        out = dot3((ngh[rows, :], ngl[rows, :]), (owh[...], owl[...]), 1, 0)
        for n in range(ins):
            parts[first + n] = out[n * chunk : (n + 1) * chunk]

    @pl.loop(0, reduce.outs)
    def _(step):
        produce(step)

        @pl.when(step == 0)
        def _():
            reduce.give(jnp.int32(0))
            reduce.give(jnp.int32(1))

    for load in loads[2:4]:
        load.wait()

    def weight_parts(left_hi, left_lo, hi, lo, then):
        for n in range(2):
            cols = pl.ds(n * split_at, split_at)
            oparts[:, n * split_at : (n + 1) * split_at] = dot3(
                (left_hi[...], left_lo[...]), (chi[...], clo[...]), 0, 0
            )
            source, cols = ((hi, lo), pl.ds(split_at, split_at)) if n == 0 else (then, None)
            if source is None:
                continue
            cols = pl.ds(split_at, split_at) if n == 0 else pl.ds(0, split_at)
            more = [
                pltpu.make_async_copy(a.at[:, cols], b, load_sem.at[2 + m])
                for m, (a, b) in enumerate(zip(source, (chi, clo)))
            ]
            for load in more:
                load.start()
            if n == 0:
                for load in more:
                    load.wait()
        return more

    hat_load = weight_parts(ngh, ngl, cot_hi, cot_lo, (hat_hi, hat_lo))
    out_sum = SeqSum(oparts, 0, keep_o, core_o, x_o, o_sems, out_o, seq, head, seqs)
    out_sum.begin()
    reduce.reduce(0)
    out_sum.pair()

    def poll(n, base):
        @pl.when(lax.rem(n, pace) == pace - 1)
        def _():
            reduce.reduce(base + n // pace)

    pace = max(1, blocks // 2)

    @pl.loop(0, blocks)
    def _(back):
        b = blocks - 1 - back
        at = pl.multiple_of(b * BLOCK, BLOCK)
        here = pl.ds(at, BLOCK)
        scale = columns[here, 0:1]
        gate = pj[pl.ds(at + 8, BLOCK), 0:chans]
        sig = logistic(gate)
        gate_act = gate * sig
        mixed = mixed_in[here, :]
        gated = mixed * gate_act
        grad_ng = cross_in[here, :]
        grad_gated = scale * (grad_ng * gain_row) - gated * columns[here, 1:2]
        grad_mixed = grad_gated * gate_act
        gmix[here, :] = grad_mixed
        gp_hi[here, 0:chans], gp_lo[here, 0:chans] = halves(
            grad_gated * mixed * (sig * (1.0 + gate * (1.0 - sig)))
        )
        conv = conv_of(back, b, jnp.maximum(b - 1, 0))
        act = conv * logistic(conv)
        chan_o[0:1, :] = chan_o[0:1, :] + jnp.sum(grad_ng * (gated * scale), 0, keepdims=True)
        chan_o[1:2, :] = chan_o[1:2, :] + jnp.sum(grad_mixed * act[:, :chans], 0, keepdims=True)
        early = grad_mixed * spread(jnp.exp(cum_in[here, :]), expand)
        adj[b] = run[...]
        run[...] = row_scale(cum_in[pl.ds(at + BLOCK - 1, 1), :], expand) * run[...] + dotx(
            early, act[:, chans + NSTATE :], 0, 0
        )
        gconv[here, chans + NSTATE :] = dotx(early, state_in[b], 1, 0)
        poll(back, 1)

    total = jnp.zeros((1, 128), F32)
    for b in range(blocks):
        total = total + cum_in[(b + 1) * BLOCK - 1 : (b + 1) * BLOCK, :]
    exch[seq, 0:chans, :] = run[...]
    exch[seq, chans : chans + 8, :] = jnp.broadcast_to(total, (8, 128))

    def state_copy(at, j, to):
        return remote(exch.at[at], exch.at[at], s_send.at[j - 1], s_recv.at[j - 1], to, head)

    for j in range(1, seqs):

        @pl.when(seq - j >= 0)
        def _():
            state_copy(seq, j, seq - j).start()

    for load in hat_load:
        load.wait()
    weight_parts(gp_hi.at[:, 0:chans], gp_lo.at[:, 0:chans], hat_hi, hat_lo, None)
    oparts[...] = oparts[...] * gain[...]
    gate_sum = SeqSum(oparts, 0, keep_g, core_g, x_g, g_sems, gate_o, seq, head, seqs)
    gate_sum.begin()
    reduce.reduce(3)

    @pl.loop(0, blocks)
    def _(b):
        at = pl.multiple_of(b * BLOCK, BLOCK)
        here = pl.ds(at, BLOCK)
        conv = conv_of(b, b, lax.rem(b + 1, blocks))
        act = conv * logistic(conv)
        writes, reads = act[:, chans : chans + NSTATE], act[:, chans + NSTATE :]
        scores = dotx(reads, writes, 1, 1)
        cum = cum_in[here, :]
        turned = cum.T
        fed_all = act[:, :chans] * spread(step_in[here, :], expand)
        grad_scores = jnp.zeros((BLOCK, BLOCK), F32)
        for first_lane, end in lanes_of(chans):
            fed = fed_all[:, first_lane:end]
            grad = gmix[here, first_lane:end]
            fed_parts, grad_parts = halves(fed), halves(grad)
            lane = lax.broadcasted_iota(jnp.int32, fed.shape, 1)
            outs = []
            for start in range(first_lane, end, HEADDIM):
                decay = decay_of(cum, turned, start // HEADDIM, causal)
                inside = (lane // HEADDIM) == (start - first_lane) // HEADDIM
                grad_scores = grad_scores + decay * dot3(halves(jnp.where(inside, grad, 0.0)), fed_parts, 1, 1)
                outs.append(dot3(halves(decay * scores), grad_parts, 0, 0))
            out = outs[0]
            if len(outs) == 2:
                out = jnp.where(lane < HEADDIM, outs[0], outs[1])
            fedg[here, first_lane:end] = out
        gconv[here, chans : chans + NSTATE] = dotx(grad_scores, reads, 0, 0)
        gconv[here, chans + NSTATE :] = gconv[here, chans + NSTATE :] + dotx(grad_scores, writes, 1, 0)
        poll(b, 4)

    gate_sum.pair()
    run[...] = jnp.zeros_like(run)
    for back in range(seqs - 1):
        later = seqs - 1 - back

        @pl.when(later > seq)
        def _():
            for j in range(1, seqs):

                @pl.when(later - seq == j)
                def _():
                    state_copy(later, j, partner).wait_recv()

            run[...] = (
                row_scale(exch[later, chans : chans + 1, :], expand) * run[...]
                + exch[later, 0:chans, :]
            )

    for b in range(blocks - 1, -1, -1):
        adj[b] = adj[b] + run[...]
        run[...] = row_scale(cum_in[(b + 1) * BLOCK - 1 : (b + 1) * BLOCK, :], expand) * run[...]

    lane_ones = jnp.ones((8, NSTATE), F32)

    @pl.loop(0, blocks)
    def _(b):
        at = pl.multiple_of(b * BLOCK, BLOCK)
        here = pl.ds(at, BLOCK)
        conv = conv_of(b, b, lax.rem(b + 1, blocks))
        sig = logistic(conv)
        act = conv * sig
        slope = sig * (1.0 + conv * (1.0 - sig))
        inner, writes = act[:, :chans], act[:, chans : chans + NSTATE]
        cum = cum_in[here, :]
        step = step_in[here, :]
        last = cum[BLOCK - 1 : BLOCK, :]
        step_wide = spread(step, expand)
        tails = spread(jnp.exp(last - cum), expand)
        fed = inner * step_wide
        grad_state = adj[b]
        from_state = tails * dotx(writes, grad_state, 1, 1)
        grad_fed = fedg[here, :] + from_state
        grad_mixed = gmix[here, :]
        grad_writes = gconv[here, chans : chans + NSTATE] + dotx(fed * tails, grad_state, 1, 0)
        direct = gather_heads(inner * grad_fed, expand)
        scanned = mixed_in[here, :] - skip_row * inner
        grad_cum = dotx(grad_mixed * scanned - fed * grad_fed, expand, 1, 1)
        kept = dotx(expand, grad_state * state_in[b], 1, 0)
        kept = dotx(lane_ones, kept, 1, 1)[0:1, :] * jnp.exp(last)
        grad_last = kept + jnp.sum(gather_heads(fed * from_state, expand), 0, keepdims=True)
        grad_log = dotx(upper, grad_cum, 1, 0) + grad_last
        rate = head_p[1:2, :]
        head_acc[1:2, :] = head_acc[1:2, :] + jnp.sum(step * grad_log, 0, keepdims=True) * rate
        arg = pj[pl.ds(at + 8, BLOCK), span + 2 * NSTATE : pad] + head_p[0:1, :]
        grad_arg = (direct + rate * grad_log) * logistic(arg) * head_p[2:3, :]
        head_acc[0:1, :] = head_acc[0:1, :] + jnp.sum(grad_arg, 0, keepdims=True)
        gp_hi[here, span + 2 * NSTATE : pad], gp_lo[here, span + 2 * NSTATE : pad] = halves(
            grad_arg
        )
        gconv[here, 0:chans] = (step_wide * grad_fed + skip_row * grad_mixed) * slope[:, :chans]
        gconv[here, chans : chans + NSTATE] = grad_writes * slope[:, chans : chans + NSTATE]
        gconv[here, chans + NSTATE :] = gconv[here, chans + NSTATE :] * slope[:, chans + NSTATE :]

    out_sum.total()
    reduce.reduce(6)
    edge = remote(
        gconv.at[pl.ds(0, 8)],
        gconv.at[pl.ds(tokens, 8)],
        e_send,
        e_recv,
        lax.rem(seq + seqs - 1, seqs),
        head,
    )
    edge.start()
    head_o[...] = head_acc[...]

    def conv_back(b):
        at = pl.multiple_of(b * BLOCK, BLOCK)
        here = pl.ds(at, BLOCK)
        window = pj[pl.ds(at, BLOCK + 8), chans : span + 2 * NSTATE]
        ahead = gconv[pl.ds(at, BLOCK + 8), :]
        grad = ahead[0:BLOCK, :]
        grad_pre = jnp.zeros((BLOCK, wide), F32)
        for k in range(WIDTH):
            grad_pre = grad_pre + conv_p[k : k + 1, :] * ahead[3 - k : 3 - k + BLOCK, :]
            wide_o[k : k + 1, :] = wide_o[k : k + 1, :] + jnp.sum(
                grad * window[5 + k : 5 + k + BLOCK, :], 0, keepdims=True
            )
        wide_o[4:5, :] = wide_o[4:5, :] + jnp.sum(grad, 0, keepdims=True)
        (
            gp_hi[here, chans : span + 2 * NSTATE],
            gp_lo[here, chans : span + 2 * NSTATE],
        ) = halves(grad_pre)

    @pl.loop(0, blocks - 1)
    def _(b):
        conv_back(b)

    edge.wait()
    gconv[tokens : tokens + 8, :] = jnp.where(seq < seqs - 1, gconv[tokens : tokens + 8, :], 0.0)

    @pl.loop(blocks - 1, blocks)
    def _(b):
        conv_back(b)

    gate_sum.total()
    reduce.reduce(7)
    reduce.last()
    result_o[...] = resid[...] + parts[head]
    conv_load(0, 0).wait()
    reduce.finish()
    for j in range(1, seqs):

        @pl.when(seq - j >= 0)
        def _():
            state_copy(seq, j, seq - j).wait_send()

    out_sum.end()
    gate_sum.end()


def backward(proj, hat, kept, out_w, resid, conv_p, head_p, chan_p, gain, expand, seqs, heads):
    (cot_hi, cot_lo, conv, cum, step, state, mixed, cross, stat, edge) = kept
    tokens, pad = proj.shape
    chunk, width = resid.shape
    chans = out_w.shape[0]
    ins = inner_count(heads)
    outs = heads // ins
    wide = chans + 2 * NSTATE
    blocks = tokens // BLOCK
    half = chans // 2
    rounds = (seqs // 2).bit_length() - 1
    anywhere = pl.BlockSpec(memory_space=pl.ANY)
    local = pl.BlockSpec(memory_space=pltpu.VMEM)
    sems = pltpu.SemaphoreType.DMA
    shape = jax.ShapeDtypeStruct
    return pl.pallas_call(
        functools.partial(backward_kernel, (seqs, heads, chunk, chans, pad)),
        out_shape=(
            shape((chunk, width), F32),
            shape((tokens, pad), BF16),
            shape((tokens, pad), BF16),
            shape((chans, width), F32),
            shape((chans, width), F32),
            shape((8, wide), F32),
            shape((8, chans), F32),
            shape((8, 128), F32),
        ),
        in_specs=[anywhere] * 7 + [local] * 6 + [anywhere] + [local] * 6,
        out_specs=(local, local, local, anywhere, anywhere, local, local, local),
        scratch_shapes=[
            pltpu.VMEM((8 + tokens, pad), F32),
            pltpu.VMEM((tokens, chans), BF16),
            pltpu.VMEM((tokens, chans), BF16),
            pltpu.VMEM((chans, width), BF16),
            pltpu.VMEM((chans, width), BF16),
            pltpu.VMEM((tokens, chans), F32),
            pltpu.VMEM((tokens, chans), F32),
            pltpu.VMEM((blocks, chans, NSTATE), F32),
            pltpu.VMEM((chans, NSTATE), F32),
            pltpu.VMEM((seqs, chans + 8, NSTATE), F32),
            pltpu.VMEM((tokens + 8, wide), F32),
            pltpu.VMEM((heads, chunk, width), F32),
            pltpu.VMEM((outs * (ins - 1), chunk, width), F32),
            pltpu.VMEM((outs + 1, chunk, width), F32),
            pltpu.VMEM((tokens, width // 2), BF16),
            pltpu.VMEM((tokens, width // 2), BF16),
            pltpu.VMEM((chans, width), F32),
            pltpu.VMEM((tokens, 128), F32),
            pltpu.VMEM((2, BLOCK, wide), F32),
            pltpu.VMEM((8, 128), F32),
            *seq_sum_scratch(half, width, rounds),
            *seq_sum_scratch(half, width, rounds),
            *line_reduce_sems(ins, outs),
            sems((5,)),
            sems((seqs - 1,)),
            sems((seqs - 1,)),
            sems,
            sems,
            sems((2,)),
        ],
        compiler_params=pltpu.CompilerParams(
            collective_id=4, has_side_effects=True, vmem_limit_bytes=VMEM_LIMIT
        ),
        name="backward",
    )(
        proj, edge, cot_hi, cot_lo, *hat, conv, cum, step, state, mixed, cross, stat,
        out_w, resid, conv_p, head_p, chan_p, gain, expand,
    )


def on_device(
    residual_in,
    norm_gain,
    gate_weight,
    inner_weight,
    bc_weight,
    step_weight,
    conv_inner_weight,
    conv_inner_bias,
    conv_bc_weight,
    conv_bc_bias,
    step_bias,
    decay_log,
    skip_gain,
    gated_gain,
    out_weight,
    cotangent,
):
    seqs, heads = lax.axis_size("seq"), lax.axis_size("head")
    width = residual_in.shape[2]
    chans = gate_weight.shape[0]
    heads_here = step_weight.shape[0]
    spare = 128 - heads_here
    resid = residual_in.reshape(-1, width)
    cot = cotangent.reshape(-1, width)
    gain = norm_gain.reshape(1, width)

    def eight(part):
        return jnp.pad(part, ((0, 8 - part.shape[0]), (0, 0)))

    def by_head(*parts):
        return eight(jnp.pad(jnp.stack(parts), ((0, 0), (0, spare))))

    conv_p = eight(
        jnp.concatenate(
            [
                jnp.concatenate([conv_inner_weight, conv_bc_weight], 1),
                jnp.concatenate([conv_inner_bias, conv_bc_bias])[None],
            ],
            0,
        )
    )
    head_p = by_head(step_bias, -jnp.exp(decay_log), jnp.ones_like(step_bias))
    chan_p = eight(jnp.stack([gated_gain, jnp.repeat(skip_gain, HEADDIM)]))
    expand = (
        lax.broadcasted_iota(jnp.int32, (128, chans), 0)
        == lax.broadcasted_iota(jnp.int32, (128, chans), 1) // HEADDIM
    ).astype(F32)
    hat_hi, hat_lo, projected, weight_hi, weight_lo = gather_project(
        resid,
        gain,
        gate_weight,
        inner_weight,
        bc_weight,
        jnp.pad(step_weight, ((0, spare), (0, 0))),
        heads,
    )
    kept = forward(projected, cot, out_weight, conv_p, head_p, chan_p, expand, seqs, heads)
    (
        result,
        grad_hi,
        grad_lo,
        out_weight_grad,
        gate_weight_grad,
        wide_sums,
        chan_sums,
        head_sums,
    ) = backward(
        projected,
        (hat_hi, hat_lo),
        kept,
        out_weight,
        resid,
        conv_p,
        head_p,
        chan_p,
        gain,
        expand,
        seqs,
        heads,
    )

    def packed(*parts):
        flat = jnp.concatenate([part.reshape(-1) for part in parts])
        count = -(-flat.shape[0] // width)
        return jnp.pad(flat, (0, count * width - flat.shape[0])).reshape(count, width)

    seq_small = packed(
        wide_sums[:WIDTH, :chans],
        wide_sums[WIDTH, :chans],
        chan_sums[0],
        head_sums[0, :heads_here],
        head_sums[1, :heads_here],
        jnp.sum(chan_sums[1].reshape(heads_here, HEADDIM), axis=1),
    )
    all_small = packed(wide_sums[: WIDTH + 1, chans:])
    small = jnp.stack(
        [
            jnp.zeros((8, width), F32),
            eight(seq_small),
            eight(jnp.concatenate([jnp.zeros((1, width), F32), all_small], 0)),
        ]
    )
    residual_grad, inner_weight_grad, bc_pieces, sums = tail(
        (grad_hi, grad_lo),
        (hat_hi, hat_lo),
        (weight_hi, weight_lo),
        small,
        resid,
        cot,
        gain,
        seqs,
        heads,
        chans,
    )
    across = width // bc_pieces.shape[2]
    bc_weight_grad = jnp.transpose(
        bc_pieces.reshape(2 * NSTATE // 8, across, 8, width // across), (1, 3, 0, 2)
    ).reshape(width, 2 * NSTATE)
    flat = sums[1].reshape(-1)

    def take(count):
        nonlocal flat
        first, flat = flat[:count], flat[count:]
        return first

    conv_inner_weight_grad = take(WIDTH * chans).reshape(WIDTH, chans)
    conv_inner_bias_grad = take(chans)
    gated_gain_grad = take(chans)
    step_bias_grad = take(heads_here)
    decay_log_grad = take(heads_here)
    skip_gain_grad = take(heads_here)
    flat = sums[2, 1:].reshape(-1)
    conv_bc_weight_grad = take(WIDTH * 2 * NSTATE).reshape(WIDTH, 2 * NSTATE)
    conv_bc_bias_grad = take(2 * NSTATE)
    return (
        result.reshape(residual_in.shape),
        residual_grad.reshape(residual_in.shape),
        sums[2, 0],
        gate_weight_grad,
        inner_weight_grad,
        bc_weight_grad,
        sums[0, :heads_here],
        conv_inner_weight_grad,
        conv_inner_bias_grad,
        conv_bc_weight_grad,
        conv_bc_bias_grad,
        step_bias_grad,
        decay_log_grad,
        skip_gain_grad,
        gated_gain_grad,
        out_weight_grad,
    )


def solution(mesh):
    placed = (
        P(None, ("seq", "head"), None),
        P(),
        P("head", None),
        P("head", None),
        P(),
        P("head", None),
        P(None, "head"),
        P("head"),
        P(),
        P(),
        P("head"),
        P("head"),
        P("head"),
        P("head"),
        P("head", None),
        P(None, ("seq", "head"), None),
    )
    return jax.shard_map(
        on_device,
        mesh=mesh,
        in_specs=placed,
        out_specs=(
            P(None, ("seq", "head"), None),
            P(None, ("seq", "head"), None),
            P(),
            P("head", None),
            P("head", None),
            P(),
            P("head", None),
            P(None, "head"),
            P("head"),
            P(),
            P(),
            P("head"),
            P("head"),
            P("head"),
            P("head"),
            P("head", None),
        ),
        check_vma=False,
    )
```

```python
import functools

import jax
import jax.numpy as jnp
from jax import lax
from jax.experimental import pallas as pl
from jax.experimental.pallas import tpu as pltpu
from jax.sharding import PartitionSpec as P

HEADDIM = 64
NSTATE = 128
WIDTH = 4
BLOCK = 256
EPSILON = 1e-05
EXACT = lax.Precision.HIGHEST
MESH = pl.DeviceIdType.MESH
F32 = jnp.float32
BF16 = jnp.bfloat16
VMEM_LIMIT = 66000000


def dot3(left, right, left_dim, right_dim):
    dims = (((left_dim,), (right_dim,)), ((), ()))
    one = functools.partial(lax.dot_general, dimension_numbers=dims, preferred_element_type=F32)
    return one(left[0], right[0]) + (one(left[0], right[1]) + one(left[1], right[0]))


def remote(source, target, send_sem, recv_sem, seq, head):
    return pltpu.make_async_remote_copy(
        src_ref=source,
        dst_ref=target,
        send_sem=send_sem,
        recv_sem=recv_sem,
        device_id=(seq, head),
        device_id_type=MESH,
    )


def greet(seq, head, seqs, heads):
    barrier = pltpu.get_barrier_semaphore()
    for j in range(1, seqs):
        pl.semaphore_signal(
            barrier, inc=1, device_id=(lax.rem(seq + j, seqs), head), device_id_type=MESH
        )
    for j in range(1, heads):
        pl.semaphore_signal(
            barrier, inc=1, device_id=(seq, lax.rem(head + j, heads)), device_id_type=MESH
        )
    pl.semaphore_wait(barrier, seqs + heads - 2)


def inner_count(heads):
    return 2 if heads <= 8 else 4


class SeqSum:
    def __init__(self, source, base, keep, core_in, x_in, sems, result, seq, head, seqs):
        self.source, self.base, self.keep, self.core_in, self.x_in = source, base, keep, core_in, x_in
        self.sems, self.result, self.seq, self.head = sems, result, seq, head
        self.rounds = (seqs // 2).bit_length() - 1
        self.half = keep.shape[0]
        self.side = lax.rem(seq, 2)
        self.partner = seq + 1 - 2 * self.side

    def rows(self, side, base):
        return pl.ds(pl.multiple_of(base + side * self.half, 8), self.half)

    def begin(self):
        self.keep[...] = self.source[self.rows(self.side, self.base), :]
        self.core = remote(
            self.source.at[self.rows(1 - self.side, self.base)],
            self.core_in,
            self.sems.at[0],
            self.sems.at[1],
            self.partner,
            self.head,
        )
        self.core.start()

    def cross(self, source, turn):
        away = 2 << turn
        far = self.seq + away - 2 * away * lax.rem(self.seq // away, 2)
        return remote(
            source,
            self.x_in.at[turn],
            self.sems.at[5 + 2 * turn],
            self.sems.at[6 + 2 * turn],
            far,
            self.head,
        )

    def pair(self):
        self.core.wait()
        self.keep[...] = self.keep[...] + self.core_in[...]
        self.cross(self.keep, 0).start()

    def total(self):
        now, new = self.keep, self.core_in
        for turn in range(self.rounds):
            self.cross(now, turn).wait()
            new[...] = now[...] + self.x_in[turn]
            now, new = new, now
            if turn + 1 < self.rounds:
                self.cross(now, turn + 1).start()
        mine = self.result.at[self.rows(self.side, 0)]
        self.now = now
        self.put = pltpu.make_async_copy(now, mine, self.sems.at[2])
        self.put.start()
        self.final = remote(
            now, mine, self.sems.at[3], self.sems.at[4], self.partner, self.head
        )
        self.final.start()

    def end(self):
        self.final.wait_send()
        remote(
            self.now,
            self.result.at[self.rows(1 - self.side, 0)],
            self.sems.at[3],
            self.sems.at[4],
            self.partner,
            self.head,
        ).wait_recv()
        self.put.wait()


def seq_sum_scratch(half, width, rounds):
    return [
        pltpu.VMEM((half, width), F32),
        pltpu.VMEM((half, width), F32),
        pltpu.VMEM((rounds, half, width), F32),
        pltpu.SemaphoreType.DMA((5 + 2 * rounds,)),
    ]


def tail_kernel(dims, *refs):
    seqs, heads, chunk, chans, pad = dims
    (
        gp_hi, gp_lo, hat_hi, hat_lo, w_hi, w_lo, wide_in, chan_in, head_in, resid, cot, gain,
        resid_grad, inner_out, bc_out, small_out, glob_out,
        gph, gpl, hth, htl, wh, wl, parts, y_in, z_in, joined, keep, core_in, x_in, i_sems,
        bc_part, bc_half, bc_seq, bc_quart, bc_head, bc_full,
        small_mine, small_pair, small_far, glob_mine, glob_pair, glob_far, small_head, gain_sum,
        load_sem, y_send, y_recv, z_send, z_recv,
        a_sem, b_send, b_recv, c_send, c_recv, m_sem, h_send, h_recv, put_sem,
    ) = refs
    width = gain.shape[1]
    span = 2 * chans
    fars = seqs // 2
    seq, head = lax.axis_index("seq"), lax.axis_index("head")
    side, far = lax.rem(seq, 2), seq // 2
    partner = seq + 1 - 2 * side
    loads = [
        pltpu.make_async_copy(a, b, load_sem.at[n])
        for n, (a, b) in enumerate(
            ((gp_hi, gph), (w_hi, wh), (gp_lo, gpl), (w_lo, wl), (hat_hi, hth), (hat_lo, htl))
        )
    ]
    for load in loads:
        load.start()
    greet(seq, head, seqs, heads)
    reduce = LineReduce(
        parts, y_in, z_in, (y_send, y_recv, z_send, z_recv), seq, head, heads, partner, 2
    )
    for load in loads[:4]:
        load.wait()

    def chunk_rows(where):
        return pl.ds(pl.multiple_of(where * chunk, 8), chunk)

    ins = reduce.ins

    def produce(step):
        first = reduce.target(step) * ins
        rows = pl.ds(pl.multiple_of(first * chunk, 8), ins * chunk)
        out = dot3((gph[rows, :], gpl[rows, :]), (wh[...], wl[...]), 1, 0)
        for n in range(ins):
            parts[first + n] = out[n * chunk : (n + 1) * chunk]

    produce(jnp.int32(0))
    reduce.give(jnp.int32(0))
    gain_row = gain[...]
    for load in loads[4:]:
        load.wait()

    small_mine[...] = jnp.zeros_like(small_mine)
    offset = 0
    for block in (wide_in, chan_in, head_in):
        small_mine[1, :, offset : offset + block.shape[1]] = block[...]
        offset += full_lanes(block.shape[1])
    gain_sum[...] = jnp.zeros_like(gain_sum)

    def gain_part(step):
        first = reduce.target(step) * ins
        rows = pl.ds(pl.multiple_of(first * chunk, 8), ins * chunk)
        hat = hth[rows, :].astype(F32) + htl[rows, :].astype(F32)
        for n in range(ins):
            gain_sum[...] = gain_sum[...] + jnp.sum(
                parts[first + n] * hat[n * chunk : (n + 1) * chunk], 0, keepdims=True
            )

    gain_part(jnp.int32(0))

    joined[span:, :] = (
        dot3((gph[:, span:], gpl[:, span:]), (hth[...], htl[...]), 0, 0) * gain_row
    )
    pieces, _, lanes = bc_part.shape
    across = width // lanes
    for row in range(pieces // across):
        for col in range(across):
            bc_part[row * across + col] = joined[
                span + row * 8 : span + row * 8 + 8, col * lanes : (col + 1) * lanes
            ]
    mine = pl.ds(side * (pieces // 2), pieces // 2)
    theirs = pl.ds((1 - side) * (pieces // 2), pieces // 2)
    bc_core = remote(
        bc_part.at[theirs], bc_half, a_sem.at[0], a_sem.at[1], partner, head
    )
    bc_core.start()
    reduce.give(jnp.int32(1))

    @pl.loop(1, reduce.outs)
    def _(step):
        produce(step)
        gain_part(step)

    def others(make):
        copies = []
        for j in range(1, fars):
            copies.append(make(j, lax.rem(far + j, fars)))
            copies[-1].start()
        return copies

    bc_core.wait()
    bc_half[...] = bc_half[...] + bc_part[mine]
    cross_bc = others(
        lambda j, to: remote(
            bc_half.at[pl.ds(to * heads, heads)],
            bc_seq.at[j - 1],
            b_send.at[0, j - 1],
            b_recv.at[0, j - 1],
            2 * to + side,
            head,
        )
    )
    reduce.reduce(0)
    low = chans if chans % 128 == 0 else 0
    rows = dot3((gph[:, low:span], gpl[:, low:span]), (hth[...], htl[...]), 0, 0)
    joined[low:span, :] = rows * gain_row
    inner = SeqSum(
        joined, chans, keep, core_in, x_in, i_sems, inner_out, seq, head, seqs
    )
    inner.begin()
    small_mine[0] = joined[span + 2 * NSTATE : span + 2 * NSTATE + 8, :]
    glob_mine[...] = jnp.zeros_like(glob_mine)
    quarter = glob_mine.shape[1]
    for n in range(width // quarter):
        glob_mine[n : n + 1, :] = gain_sum[:, n * quarter : (n + 1) * quarter]
    glob_mine[8:16, 0 : 2 * NSTATE] = wide_in[:, chans:]
    reduce.reduce(1)
    for copy in cross_bc:
        copy.wait()
    quarter = bc_half[pl.ds(far * heads, heads)]
    for j in range(fars - 1):
        quarter = quarter + bc_seq[j]
    bc_quart[...] = quarter

    def to_heads(make):
        copies = []
        for j in range(1, heads):
            copies.append(make(j, lax.rem(head + j, heads)))
            copies[-1].start()
        return copies

    spread_bc = to_heads(
        lambda j, to: remote(
            bc_quart.at[to], bc_head.at[j - 1], c_send.at[0, j - 1], c_recv.at[0, j - 1], seq, to
        )
    )
    inner.pair()
    small_core = [
        remote(small_mine, small_pair, a_sem.at[2], a_sem.at[3], partner, head),
        remote(glob_mine, glob_pair, a_sem.at[6], a_sem.at[7], partner, head),
    ]
    for copy in small_core:
        copy.start()
    reduce.reduce(2)
    for copy in small_core:
        copy.wait()
    small_far[far] = small_mine[...] + small_pair[...]
    glob_far[far] = glob_mine[...] + glob_pair[...]
    cross_small = others(
        lambda j, to: remote(
            small_far.at[far],
            small_far.at[far],
            m_sem.at[0, j - 1],
            m_sem.at[1, j - 1],
            2 * to + side,
            head,
        )
    ) + others(
        lambda j, to: remote(
            glob_far.at[far],
            glob_far.at[far],
            m_sem.at[2, j - 1],
            m_sem.at[3, j - 1],
            2 * to + side,
            head,
        )
    )
    reduce.reduce(3)
    for copy in spread_bc:
        copy.wait()
    piece = bc_quart[head]
    for j in range(heads - 1):
        piece = piece + bc_head[j]
    block = side * (pieces // 2) + far * heads
    bc_full[block + head] = piece
    gather_bc = to_heads(
        lambda j, to: remote(
            bc_full.at[block + head],
            bc_full.at[block + head],
            c_send.at[1, j - 1],
            c_recv.at[1, j - 1],
            seq,
            to,
        )
    )
    for j in range(1, fars):
        came = lax.rem(far - j + fars, fars)
        remote(
            small_far.at[came], small_far.at[came], m_sem.at[0, j - 1], m_sem.at[1, j - 1],
            partner, head,
        ).wait_recv()
        remote(
            glob_far.at[came], glob_far.at[came], m_sem.at[2, j - 1], m_sem.at[3, j - 1],
            partner, head,
        ).wait_recv()
    total, glob = small_far[0], glob_far[0]
    for j in range(1, fars):
        total = total + small_far[j]
        glob = glob + glob_far[j]
    small_out[...] = total
    small_head[head] = glob
    spread_small = to_heads(
        lambda j, to: remote(
            small_head.at[head], small_head.at[head], h_send.at[j - 1], h_recv.at[j - 1], seq, to
        )
    )
    reduce.reduce(4)
    reduce.reduce(5)
    for j in range(1, heads):
        came = lax.rem(head - j + heads, heads)
        remote(
            bc_full.at[block + came], bc_full.at[block + came],
            c_send.at[1, j - 1], c_recv.at[1, j - 1], partner, head,
        ).wait_recv()
    own_block = pl.ds(block, heads)
    join_bc = others(
        lambda j, to: remote(
            bc_full.at[own_block],
            bc_full.at[own_block],
            b_send.at[1, j - 1],
            b_recv.at[1, j - 1],
            2 * to + side,
            head,
        )
    )
    for j in range(1, heads):
        came = lax.rem(head - j + heads, heads)
        remote(
            small_head.at[came], small_head.at[came], h_send.at[j - 1], h_recv.at[j - 1], seq, came
        ).wait_recv()
    total = small_head[0]
    for j in range(1, heads):
        total = total + small_head[j]
    glob_out[...] = total
    reduce.reduce(6)
    for j in range(1, fars):
        came = side * (pieces // 2) + lax.rem(far - j + fars, fars) * heads
        came = pl.ds(came, heads)
        remote(
            bc_full.at[came], bc_full.at[came], b_send.at[1, j - 1], b_recv.at[1, j - 1],
            partner, head,
        ).wait_recv()
    join_core = remote(
        bc_full.at[mine], bc_full.at[mine], a_sem.at[4], a_sem.at[5], partner, head
    )
    join_core.start()
    inner.total()
    reduce.reduce(7)
    reduce.last()
    grad_hat = parts[head] * gain_row
    values = resid[...]
    scale = lax.rsqrt(jnp.mean(values * values, axis=1, keepdims=True) + EPSILON)
    row_cross = jnp.sum(grad_hat * values, axis=1, keepdims=True)
    resid_grad[...] = (
        cot[...] + scale * grad_hat - values * (scale * scale * scale * (row_cross / width))
    )
    remote(
        bc_full.at[theirs], bc_full.at[theirs], a_sem.at[4], a_sem.at[5], partner, head
    ).wait_recv()
    bc_put = pltpu.make_async_copy(bc_full, bc_out, put_sem)
    bc_put.start()
    reduce.finish()
    for copy in gather_bc + cross_small + spread_small + join_bc + [join_core]:
        copy.wait_send()
    inner.end()
    bc_put.wait()


def tail(gp, hat, weight, sums, resid, cot, gain, seqs, heads, chans):
    tokens, width = hat[0].shape
    chunk = tokens // heads
    pad = gp[0].shape[1]
    ins = inner_count(heads)
    outs = heads // ins
    rounds = (seqs // 2).bit_length() - 1
    fars = seqs // 2
    lanes = 2 * NSTATE * width // (8 * seqs * heads)
    pieces = seqs * heads
    anywhere = pl.BlockSpec(memory_space=pl.ANY)
    local = pl.BlockSpec(memory_space=pltpu.VMEM)
    sems = pltpu.SemaphoreType.DMA
    return pl.pallas_call(
        functools.partial(tail_kernel, (seqs, heads, chunk, chans, pad)),
        out_shape=(
            jax.ShapeDtypeStruct((chunk, width), F32),
            jax.ShapeDtypeStruct((chans, width), F32),
            jax.ShapeDtypeStruct((pieces, 8, lanes), F32),
            jax.ShapeDtypeStruct((2, 8, width), F32),
            jax.ShapeDtypeStruct((16, width // 4), F32),
        ),
        in_specs=[anywhere] * 6 + [local] * 6,
        out_specs=(local, anywhere, anywhere, local, local),
        scratch_shapes=[
            pltpu.VMEM((tokens, pad), BF16),
            pltpu.VMEM((tokens, pad), BF16),
            pltpu.VMEM((tokens, width), BF16),
            pltpu.VMEM((tokens, width), BF16),
            pltpu.VMEM((pad, width), BF16),
            pltpu.VMEM((pad, width), BF16),
            pltpu.VMEM((heads, chunk, width), F32),
            pltpu.VMEM((outs * (ins - 1), chunk, width), F32),
            pltpu.VMEM((outs + 1, chunk, width), F32),
            pltpu.VMEM((pad, width), F32),
            *seq_sum_scratch(chans // 2, width, rounds),
            pltpu.VMEM((pieces, 8, lanes), F32),
            pltpu.VMEM((pieces // 2, 8, lanes), F32),
            pltpu.VMEM((fars - 1, heads, 8, lanes), F32),
            pltpu.VMEM((heads, 8, lanes), F32),
            pltpu.VMEM((heads - 1, 8, lanes), F32),
            pltpu.VMEM((pieces, 8, lanes), F32),
            pltpu.VMEM((2, 8, width), F32),
            pltpu.VMEM((2, 8, width), F32),
            pltpu.VMEM((fars, 2, 8, width), F32),
            pltpu.VMEM((16, width // 4), F32),
            pltpu.VMEM((16, width // 4), F32),
            pltpu.VMEM((fars, 16, width // 4), F32),
            pltpu.VMEM((heads, 16, width // 4), F32),
            pltpu.VMEM((1, width), F32),
            sems((6,)),
            *line_reduce_sems(ins, outs),
            sems((8,)),
            sems((2, fars - 1)),
            sems((2, fars - 1)),
            sems((2, heads - 1)),
            sems((2, heads - 1)),
            sems((4, fars - 1)),
            sems((heads - 1,)),
            sems((heads - 1,)),
            sems,
        ],
        compiler_params=pltpu.CompilerParams(
            collective_id=1, has_side_effects=True, vmem_limit_bytes=VMEM_LIMIT
        ),
        name="tail",
    )(*gp, *hat, *weight, *sums, resid, cot, gain)


def dotx(left, right, left_dim, right_dim):
    return lax.dot_general(
        left,
        right,
        (((left_dim,), (right_dim,)), ((), ())),
        precision=EXACT,
        preferred_element_type=F32,
    )


def halves(values):
    top = values.astype(BF16)
    return (top, (values - top.astype(F32)).astype(BF16))


def head_lanes(chans):
    row = lax.broadcasted_iota(jnp.int32, (128, chans), 0)
    col = lax.broadcasted_iota(jnp.int32, (128, chans), 1)
    return (row == col // HEADDIM).astype(F32)


def lanes_of(chans):
    return [(lo, min(lo + 2 * HEADDIM, chans)) for lo in range(0, chans, 2 * HEADDIM)]


def spread(values, expand):
    top, low = halves(values)
    expand = expand.astype(BF16)
    dims = (((1,), (0,)), ((), ()))
    one = functools.partial(lax.dot_general, dimension_numbers=dims, preferred_element_type=F32)
    return one(top, expand) + one(low, expand)


def gather_heads(values, expand):
    top, low = halves(values)
    expand = expand.astype(BF16)
    dims = (((1,), (1,)), ((), ()))
    one = functools.partial(lax.dot_general, dimension_numbers=dims, preferred_element_type=F32)
    return one(top, expand) + one(low, expand)


def row_scale(total_row, expand):
    wide = jnp.broadcast_to(jnp.exp(total_row), (128, 128)).T
    return dotx(expand, wide, 0, 0)


def logistic(values):
    return 1.0 / (1.0 + jnp.exp(-values))


def decay_of(cum, cum_turned, h, causal):
    return jnp.where(causal, jnp.exp(cum[:, h : h + 1] - cum_turned[h : h + 1, :]), 0.0)


def decay_turned(cum, cum_turned, h, anticausal):
    return jnp.where(anticausal, jnp.exp(cum_turned[h : h + 1, :] - cum[:, h : h + 1]), 0.0)


class LineGather:
    def __init__(self, parts, sems, seq, head, heads):
        self.parts, self.seq = parts, seq
        self.z_send, self.z_recv, self.y_send, self.y_recv = sems
        self.ins = inner_count(heads)
        self.outs = heads // self.ins
        self.at_out, self.at_in = head // self.ins, lax.rem(head, self.ins)
        chunk = parts.shape[1]
        half, early = chunk // 2, max(8, chunk // 8)
        self.halves = {0: pl.ds(0, half), self.ins: pl.ds(half, half)}
        self.sides = (pl.ds(0, half), pl.ds(chunk - early, early), pl.ds(half, half - early))

    def z_copy(self, place, j, up):
        where = place * self.ins + lax.rem(self.at_in + j, self.ins)
        piece = self.parts.at[where, self.halves.get(j, self.sides[1])]
        return remote(
            piece,
            piece,
            self.z_send.at[place, up, j],
            self.z_recv.at[place, j],
            self.seq,
            (self.at_out + 2 * up - 1) * self.ins + self.at_in,
        )

    def y_copy(self, where, j, part):
        place = where // self.ins
        piece = self.parts.at[where, self.sides[part]]
        return remote(
            piece,
            piece,
            self.y_send.at[place, j, part],
            self.y_recv.at[place, j, part],
            self.seq,
            self.at_out * self.ins + lax.rem(self.at_in + 1 + j, self.ins),
        )

    def onward(self, place, j, act):
        @pl.when((place >= self.at_out) & (self.at_out > 0))
        def _():
            act(self.z_copy(place, j, 0))

        @pl.when((place <= self.at_out) & (self.at_out < self.outs - 1))
        def _():
            act(self.z_copy(place, j, 1))

    def half(self, place, half):
        self.onward(place, half, lambda copy: copy.start())
        for j in range(self.ins - 1):
            self.y_copy(place * self.ins + self.at_in, j, 2 if half else 0).start()

    def start(self):
        for j in range(self.ins - 1):
            self.y_copy(self.at_out * self.ins + self.at_in, j, 1).start()
        self.half(self.at_out, 0)

    def second(self):
        self.half(self.at_out, self.ins)

    def early(self):
        for j in range(self.ins - 1):
            where = self.at_out * self.ins + lax.rem(self.at_in + self.ins - 1 - j, self.ins)
            self.y_copy(where, j, 1).wait_recv()
            self.onward(self.at_out, self.ins - 1 - j, lambda copy: copy.start())

    def relay(self, distance, part):
        for side in range(2):
            place = self.at_out + (2 * side - 1) * distance

            @pl.when((place >= 0) & (place < self.outs))
            def _():
                self.z_copy(place, part * self.ins, 0).wait_recv()
                self.half(place, part * self.ins)
                for j in range(1, self.ins if part else 1):
                    self.z_copy(place, j, 0).wait_recv()
                    self.onward(place, j, lambda copy: copy.start())

    def use(self, distance, consume):
        @pl.loop(0, 2 * self.ins)
        def _(n):
            side, j = n // self.ins, lax.rem(n, self.ins)
            late = (j + self.ins - 1) // self.ins
            away = distance - late
            place = self.at_out + (2 * side - 1) * away

            @pl.when(
                (place >= 0) & (place < self.outs) & (away >= 0) & (away + 1 - side > 0)
            )
            def _():
                where = place * self.ins + lax.rem(self.at_in + self.ins - j, self.ins)

                @pl.when(j > 0)
                def _():
                    self.y_copy(where, j - 1, 0).wait_recv()
                    self.y_copy(where, j - 1, 2).wait_recv()

                consume(where)

    def finish(self):
        mine = self.at_out * self.ins + self.at_in
        for place in range(self.outs):
            for j in range(self.ins + 1):
                self.onward(place, j, lambda copy: copy.wait_send())
            for j in range(self.ins - 1):
                self.y_copy(place * self.ins + self.at_in, j, 0).wait_send()
                self.y_copy(place * self.ins + self.at_in, j, 2).wait_send()
        for j in range(self.ins - 1):
            self.y_copy(mine, j, 1).wait_send()


def line_gather_sems(ins, outs):
    sems = pltpu.SemaphoreType.DMA
    return [
        sems((outs, 2, ins + 1)),
        sems((outs, ins + 1)),
        sems((outs, ins - 1, 3)),
        sems((outs, ins - 1, 3)),
    ]


def full_lanes(count):
    return -(-count // 128) * 128


def front_kernel(dims, *refs):
    seqs, heads, chunk, chans, pad = dims
    (
        rows, cot, gain, gate_w, inner_w, bc_w, step_w, out_w, conv_p, head_p, chan_p,
        hat_hi, hat_lo, pj_o, w_hi, w_lo,
        cot_hi, cot_lo, conv_hbm, cum_o, step_o, state_o, mixed_o, cross_o, stat_o,
        parts, cot_parts, hi, lo, pj, raw, wh, wl, wth, wtl, owh, owl,
        enter, prefix, run, exch, stat_all, lows,
        za_send, za_recv, ya_send, ya_recv, zb_send, zb_recv, yb_send, yb_recv,
        load_sem, put_sem, e_send, e_recv, s_send, s_recv, t_send, t_recv,
    ) = refs
    tokens = chunk * heads
    blocks = tokens // BLOCK
    span = 2 * chans
    wide = chans + 2 * NSTATE
    seq, head = lax.axis_index("seq"), lax.axis_index("head")
    convs = slice(0, wide)
    scaled = slice(768, 768 + chans)

    loads = [
        pltpu.make_async_copy(gate_w, raw.at[pl.ds(0, chans)], load_sem.at[0]),
        pltpu.make_async_copy(inner_w, raw.at[pl.ds(chans, chans)], load_sem.at[1]),
    ]
    for load in loads:
        load.start()
    values = rows[...]
    parts[head] = values * lax.rsqrt(
        jnp.mean(values * values, axis=1, keepdims=True) + EPSILON
    )
    cot_parts[head] = cot[...]
    greet(seq, head, seqs, heads)
    gather = LineGather(parts, (za_send, za_recv, ya_send, ya_recv), seq, head, heads)
    cotan = LineGather(cot_parts, (zb_send, zb_recv, yb_send, yb_recv), seq, head, heads)
    gather.start()

    raw[span : span + 2 * NSTATE, :] = bc_w[...].T
    raw[span + 2 * NSTATE :, :] = jnp.zeros((raw.shape[0] - span - 2 * NSTATE, raw.shape[1]), F32)
    raw[span + 2 * NSTATE : span + 2 * NSTATE + step_w.shape[0], :] = step_w[...]
    for load in loads:
        load.wait()
    gain_row = gain[...]

    def turn_weights(block):
        here = pl.ds(pl.multiple_of(block * 128, 128), 128)
        piece = raw[here, :]
        wh[here, :], wl[here, :] = halves(piece)
        wth[:, here], wtl[:, here] = halves((piece * gain_row).T)

    @pl.loop(0, pad // 256)
    def _(block):
        turn_weights(block)

    gather.second()
    gather.early()

    @pl.loop(pad // 256, pad // 128)
    def _(block):
        turn_weights(block)

    puts = [
        pltpu.make_async_copy(wh, w_hi, put_sem.at[0]),
        pltpu.make_async_copy(wl, w_lo, put_sem.at[1]),
    ]
    load_w = pltpu.make_async_copy(out_w, raw.at[pl.ds(0, chans)], load_sem.at[0])
    for copy in puts + [load_w]:
        copy.start()

    def chunk_rows(where):
        return pl.ds(pl.multiple_of(where * chunk, 8), chunk)

    def chunk_puts(where, top, low):
        here = chunk_rows(where)
        return [
            pltpu.make_async_copy(hi.at[where], top.at[here], put_sem.at[2 + 2 * where]),
            pltpu.make_async_copy(lo.at[where], low.at[here], put_sem.at[3 + 2 * where]),
        ]

    def project(where):
        top, low = halves(parts[where])
        hi[where] = top
        lo[where] = low
        here = pl.ds(pl.multiple_of(8 + where * chunk, 8), chunk)
        pj[here, :] = dot3((top, low), (wth[...], wtl[...]), 1, 0)
        for put in chunk_puts(where, hat_hi, hat_lo):
            put.start()

    assert gather.outs == 4
    gather.relay(1, 0)
    gather.use(0, project)
    load_w.wait()
    for lane, end in lanes_of(chans):
        owh[:, lane:end], owl[:, lane:end] = halves(raw[lane:end, :].T)
    gather.relay(1, 1)
    gather.relay(2, 0)
    expand = head_lanes(chans)
    gather.use(1, project)
    gather.relay(2, 1)
    gather.relay(3, 0)
    gather.use(2, project)
    gather.relay(3, 1)
    cotan.start()
    gather.use(3, project)
    cotan.second()
    cotan.early()
    gather.use(4, project)
    edge = remote(
        pj.at[pl.ds(tokens, 8)],
        pj.at[pl.ds(0, 8)],
        e_send,
        e_recv,
        lax.rem(seq + 1, seqs),
        head,
    )
    edge.start()
    cotan.relay(1, 0)
    edge.wait()
    pj[0:8, :] = jnp.where(seq > 0, pj[0:8, :], 0.0)
    pj_put = pltpu.make_async_copy(pj, pj_o, put_sem.at[2 + 2 * heads])
    pj_put.start()
    cotan.relay(1, 1)
    cotan.relay(2, 0)
    tri_r = lax.broadcasted_iota(jnp.int32, (BLOCK, BLOCK), 0)
    tri_c = lax.broadcasted_iota(jnp.int32, (BLOCK, BLOCK), 1)
    causal = tri_r >= tri_c
    lower = causal.astype(F32)
    run[...] = jnp.zeros_like(run)
    prefix[...] = jnp.zeros_like(prefix)

    @pl.loop(0, blocks)
    def _(b):
        at = pl.multiple_of(b * BLOCK, BLOCK)
        here = pl.ds(at, BLOCK)
        window = pj[pl.ds(at, BLOCK + 8), chans : span + 2 * NSTATE]
        conv = jnp.zeros((BLOCK, wide), F32) + conv_p[4:5, :]
        for k in range(WIDTH):
            conv = conv + conv_p[k : k + 1, :] * window[5 + k : 5 + k + BLOCK, :]
        raw[here, convs] = conv
        act = conv * logistic(conv)
        arg = pj[pl.ds(at + 8, BLOCK), span + 2 * NSTATE : pad] + head_p[0:1, :]
        step = jnp.maximum(arg, 0.0) + jnp.log1p(jnp.exp(-jnp.abs(arg)))
        cum = dotx(lower, step * head_p[1:2, :], 1, 0)
        last = cum[BLOCK - 1 : BLOCK, :]
        step_o[here, :] = step
        cum_o[here, :] = cum
        fed = act[:, :chans] * spread(step, expand)
        raw[here, scaled] = fed
        fresh = dotx(
            fed * spread(jnp.exp(last - cum), expand), act[:, chans : chans + NSTATE], 0, 0
        )
        enter[b] = run[...]
        run[...] = row_scale(last, expand) * run[...] + fresh
        prefix[pl.ds(b + 1, 1), :] = prefix[pl.ds(b, 1), :] + last

        @pl.when(b == blocks // 2)
        def _():
            cotan.relay(2, 1)

    conv_put = pltpu.make_async_copy(
        raw.at[pl.ds(0, tokens), pl.ds(0, full_lanes(wide))], conv_hbm, put_sem.at[3 + 2 * heads]
    )
    conv_put.start()
    exch[seq, 0:chans, :] = run[...]
    exch[seq, chans : chans + 8, :] = jnp.broadcast_to(prefix[blocks : blocks + 1, :], (8, 128))

    def state_copy(at, j, to):
        return remote(exch.at[at], exch.at[at], s_send.at[j - 1], s_recv.at[j - 1], to, head)

    for j in range(1, seqs):

        @pl.when(seq + j < seqs)
        def _():
            state_copy(seq, j, seq + j).start()

    @pl.loop(0, blocks)
    def _(b):
        at = pl.multiple_of(b * BLOCK, BLOCK)
        here = pl.ds(at, BLOCK)
        bc = raw[here, chans:wide]
        bc = bc * logistic(bc)
        scores = dotx(bc[:, NSTATE:], bc[:, :NSTATE], 1, 1)
        cum = cum_o[here, :]
        turned = cum.T
        for first_lane, end in lanes_of(chans):
            fed = halves(raw[here, scaled.start + first_lane : scaled.start + end])
            outs = [
                dot3(
                    halves(decay_of(cum, turned, lane // HEADDIM, causal) * scores), fed, 1, 0
                )
                for lane in range(first_lane, end, HEADDIM)
            ]
            out = outs[0]
            if len(outs) == 2:
                lane = lax.broadcasted_iota(jnp.int32, out.shape, 1)
                out = jnp.where(lane < HEADDIM, outs[0], outs[1])
            mixed_o[here, first_lane:end] = out

        @pl.when(b == 0)
        def _():
            cotan.relay(3, 0)

        @pl.when(b == blocks // 2)
        def _():
            cotan.relay(3, 1)

    run[...] = jnp.zeros_like(run)
    for earlier in range(seqs - 1):

        @pl.when(earlier < seq)
        def _():
            for j in range(1, seqs):

                @pl.when(seq - earlier == j)
                def _():
                    state_copy(earlier, j, lax.rem(seq + 1, seqs)).wait_recv()

            run[...] = (
                row_scale(exch[earlier, chans : chans + 1, :], expand) * run[...]
                + exch[earlier, 0:chans, :]
            )

    @pl.loop(0, blocks)
    def _(b):
        at = pl.multiple_of(b * BLOCK, BLOCK)
        here = pl.ds(at, BLOCK)
        state = enter[b] + row_scale(prefix[pl.ds(b, 1), :], expand) * run[...]
        state_o[b] = state
        conv = raw[here, convs]
        act = conv * logistic(conv)
        gate = pj[pl.ds(at + 8, BLOCK), 0:chans]
        carried = dotx(act[:, chans + NSTATE :], state, 1, 1)
        mixed = (
            mixed_o[here, :]
            + carried * spread(jnp.exp(cum_o[here, :]), expand)
            + chan_p[1:2, :] * act[:, :chans]
        )
        mixed_o[here, :] = mixed
        raw[here, scaled] = mixed * gate * logistic(gate)

    ones = jnp.ones((8, chans), F32)
    groups = tokens // 128

    def statistics(n):
        here = pl.ds(pl.multiple_of(n * 128, 128), 128)
        gated = raw[here, scaled]
        lows[pl.ds(n, 1), :] = dotx(ones, gated * gated, 1, 1)[0:1, :]
        lows[pl.ds(groups + n, 1), :] = dotx(
            ones, cross_o[here, :] * chan_p[0:1, :] * gated, 1, 1
        )[0:1, :]

    def consume(where):
        here = chunk_rows(where)
        for put in chunk_puts(where, hat_hi, hat_lo):
            put.wait()
        top, low = halves(cot_parts[where])
        hi[where] = top
        lo[where] = low
        cross_o[here, :] = dot3((top, low), (owh[...], owl[...]), 1, 0)
        for put in chunk_puts(where, cot_hi, cot_lo):
            put.start()
        if chunk == 128:
            statistics(where)

    for distance in range(cotan.outs + 1):
        cotan.use(distance, consume)

    if chunk != 128:

        @pl.loop(0, groups)
        def _(n):
            statistics(n)

    stat_all[head] = lows[...]
    sends = []
    for j in range(1, heads):
        sends.append(
            remote(
                stat_all.at[head],
                stat_all.at[head],
                t_send.at[j - 1],
                t_recv.at[j - 1],
                seq,
                lax.rem(head + j, heads),
            )
        )
        sends[-1].start()
    gather.finish()
    cotan.finish()
    for put in puts + [pj_put, conv_put]:
        put.wait()

    @pl.loop(0, heads)
    def _(where):
        for put in chunk_puts(where, cot_hi, cot_lo):
            put.wait()

    for j in range(1, seqs):

        @pl.when(seq + j < seqs)
        def _():
            state_copy(seq, j, seq + j).wait_send()

    for j in range(1, heads):
        came = lax.rem(head - j + heads, heads)
        remote(
            stat_all.at[came], stat_all.at[came], t_send.at[j - 1], t_recv.at[j - 1], seq, came
        ).wait_recv()
    total = stat_all[0]
    for j in range(1, heads):
        total = total + stat_all[j]
    stat_o[...] = total
    for copy in sends:
        copy.wait_send()


def front(
    resid, cot, gain, gate_w, inner_w, bc_w, step_w, out_w, conv_p, head_p, chan_p,
    seqs, heads,
):
    chunk, width = resid.shape
    chans = gate_w.shape[0]
    pad = 2 * chans + 2 * NSTATE + 128
    ins = inner_count(heads)
    outs = heads // ins
    tokens = chunk * heads
    wide = chans + 2 * NSTATE
    blocks = tokens // BLOCK
    groups = 2 * tokens // 128
    anywhere = pl.BlockSpec(memory_space=pl.ANY)
    local = pl.BlockSpec(memory_space=pltpu.VMEM)
    sems = pltpu.SemaphoreType.DMA
    shape = jax.ShapeDtypeStruct
    return pl.pallas_call(
        functools.partial(front_kernel, (seqs, heads, chunk, chans, pad)),
        out_shape=(
            shape((tokens, width), BF16),
            shape((tokens, width), BF16),
            shape((8 + tokens, pad), F32),
            shape((pad, width), BF16),
            shape((pad, width), BF16),
            shape((tokens, width), BF16),
            shape((tokens, width), BF16),
            shape((tokens, full_lanes(wide)), F32),
            shape((tokens, 128), F32),
            shape((tokens, 128), F32),
            shape((blocks, chans, NSTATE), F32),
            shape((tokens, chans), F32),
            shape((tokens, chans), F32),
            shape((groups, 128), F32),
        ),
        in_specs=[local] * 3 + [anywhere] * 2 + [local] * 2 + [anywhere] + [local] * 3,
        out_specs=(anywhere,) * 8 + (local,) * 6,
        scratch_shapes=[
            pltpu.VMEM((heads, chunk, width), F32),
            pltpu.VMEM((heads, chunk, width), F32),
            pltpu.VMEM((heads, chunk, width), BF16),
            pltpu.VMEM((heads, chunk, width), BF16),
            pltpu.VMEM((8 + tokens, pad), F32),
            pltpu.VMEM((max(pad, tokens), width), F32),
            pltpu.VMEM((pad, width), BF16),
            pltpu.VMEM((pad, width), BF16),
            pltpu.VMEM((width, pad), BF16),
            pltpu.VMEM((width, pad), BF16),
            pltpu.VMEM((width, chans), BF16),
            pltpu.VMEM((width, chans), BF16),
            pltpu.VMEM((blocks, chans, NSTATE), F32),
            pltpu.VMEM((8, 128), F32),
            pltpu.VMEM((chans, NSTATE), F32),
            pltpu.VMEM((seqs, chans + 8, NSTATE), F32),
            pltpu.VMEM((heads, groups, 128), F32),
            pltpu.VMEM((groups, 128), F32),
            *line_gather_sems(ins, outs),
            *line_gather_sems(ins, outs),
            sems((2,)),
            sems((4 + 2 * heads,)),
            sems,
            sems,
            sems((seqs - 1,)),
            sems((seqs - 1,)),
            sems((heads - 1,)),
            sems((heads - 1,)),
        ],
        compiler_params=pltpu.CompilerParams(
            collective_id=2, has_side_effects=True, vmem_limit_bytes=VMEM_LIMIT
        ),
        name="front",
    )(resid, cot, gain, gate_w, inner_w, bc_w, step_w, out_w, conv_p, head_p, chan_p)


class LineReduce:
    def __init__(self, parts, y_in, z_in, sems, seq, head, heads, partner, depth):
        self.depth = depth
        self.parts, self.y_in, self.z_in = parts, y_in, z_in
        self.y_send, self.y_recv, self.z_send, self.z_recv = sems
        self.seq, self.partner = seq, partner
        self.ins = inner_count(heads)
        self.outs = heads // self.ins
        self.half = parts.shape[1] // 2
        self.turns = 2 * self.outs
        self.at_out, self.at_in = head // self.ins, lax.rem(head, self.ins)
        self.upper = self.at_out // (self.outs // 2)
        self.mirrored = self.at_out + self.upper * (self.outs - 1 - 2 * self.at_out)

    def target(self, step):
        last = (step + 1) // self.outs
        far = self.outs - 1 - step
        far = far - (self.mirrored - far + self.outs) // self.outs
        far = far + self.upper * (self.outs - 1 - 2 * far)
        return far + last * (self.at_out - far)

    def rows(self, turn):
        return pl.ds(pl.multiple_of(lax.rem(turn, 2) * self.half, 8), self.half)

    def y_copy(self, turn, j):
        goal = self.target(turn // 2)
        to = lax.rem(self.at_in + 1 + j, self.ins)
        rows = self.rows(turn)
        return remote(
            self.parts.at[goal * self.ins + to, rows],
            self.y_in.at[goal * (self.ins - 1) + j, rows],
            self.y_send.at[turn, j],
            self.y_recv.at[turn, j],
            self.seq,
            self.at_out * self.ins + to,
        )

    def give(self, turn):
        for j in range(self.ins - 1):
            self.y_copy(turn, j).start()

    def take(self, turn, slot):
        rows = self.rows(turn)
        where = self.target(turn // 2) * self.ins + self.at_in
        remote(
            self.parts.at[0, rows],
            self.z_in.at[slot, rows],
            self.z_send.at[0],
            self.z_recv.at[slot, lax.rem(turn, 2)],
            self.partner,
            self.at_out * self.ins + self.at_in,
        ).wait_recv()
        self.parts[where, rows, :] = self.parts[where, rows, :] + self.z_in[slot, rows, :]

    def pass_on(self, turn, up):
        goal, rows = self.target(turn // 2), self.rows(turn)
        remote(
            self.parts.at[goal * self.ins + self.at_in, rows],
            self.z_in.at[goal + up, rows],
            self.z_send.at[turn],
            self.z_recv.at[goal + up, lax.rem(turn, 2)],
            self.seq,
            (self.at_out + 2 * up - 1) * self.ins + self.at_in,
        ).start()

    def across(self, turn):
        goal = self.target(turn // 2)
        rows = self.rows(turn)
        where = goal * self.ins + self.at_in
        for j in range(self.ins - 1):
            self.y_copy(turn, j).wait_recv()

        @pl.when(turn + self.depth < self.turns)
        def _():
            self.give(turn + self.depth)

        for j in range(self.ins - 1):
            self.parts[where, rows, :] = (
                self.parts[where, rows, :] + self.y_in[goal * (self.ins - 1) + j, rows, :]
            )

        @pl.when((goal > self.at_out) & (self.at_out == 0))
        def _():
            self.pass_on(turn, 1)

        @pl.when((goal < self.at_out) & (self.at_out == self.outs - 1))
        def _():
            self.pass_on(turn, 0)

    def along(self, turn):
        goal = self.target(turn // 2)

        @pl.when((goal >= self.at_out) & (self.at_out > 0))
        def _():
            self.take(turn, goal + 1)

        @pl.when((goal <= self.at_out) & (self.at_out < self.outs - 1))
        def _():
            self.take(turn, goal)

        @pl.when((goal > self.at_out) & (self.at_out > 0))
        def _():
            self.pass_on(turn, 1)

        @pl.when((goal < self.at_out) & (self.at_out < self.outs - 1))
        def _():
            self.pass_on(turn, 0)

    def reduce(self, turn):
        turn = jnp.int32(turn)
        self.across(turn)

        @pl.when(turn > 0)
        def _():
            self.along(turn - 1)

    def last(self):
        self.along(jnp.int32(self.turns - 1))

    def finish(self):
        @pl.loop(0, self.turns)
        def _(turn):
            for j in range(self.ins - 1):
                self.y_copy(turn, j).wait_send()

        @pl.loop(0, self.turns - 2)
        def _(turn):
            rows = pl.ds(0, self.half)
            remote(
                self.parts.at[0, rows],
                self.z_in.at[0, rows],
                self.z_send.at[turn],
                self.z_recv.at[0, 0],
                self.partner,
                self.at_out * self.ins + self.at_in,
            ).wait_send()


def line_reduce_sems(ins, outs):
    sems = pltpu.SemaphoreType.DMA
    return [
        sems((2 * outs, ins - 1)),
        sems((2 * outs, ins - 1)),
        sems((2 * outs,)),
        sems((outs + 1, 2)),
    ]


def backward_kernel(dims, *refs):
    seqs, heads, chunk, chans, pad = dims
    (
        proj, cot_hi, cot_lo, hat_hi, hat_lo, conv_in, cum_in, step_in, state_in, mixed_in, cross_in,
        stat_in, out_w, resid, conv_p, head_p, chan_p, gain,
        result_o, gp_hi, gp_lo, out_o, gate_o, wide_o, chan_o, head_o,
        pj, ngh, ngl, owh, owl, gmix, fedg, adj, run, exch, gconv,
        parts, y_in, z_in, chi, clo, oparts, columns, conv_buf, head_acc,
        keep_o, core_o, x_o, o_sems, keep_g, core_g, x_g, g_sems,
        y_send, y_recv, z_send, z_recv, load_sem, s_send, s_recv, e_send, e_recv, conv_sem,
    ) = refs
    tokens = chunk * heads
    blocks = tokens // BLOCK
    span = 2 * chans
    wide = chans + 2 * NSTATE
    split_at = resid.shape[1] // 2
    seq, head = lax.axis_index("seq"), lax.axis_index("head")
    side = lax.rem(seq, 2)
    partner = seq + 1 - 2 * side
    loads = [
        pltpu.make_async_copy(a, b, load_sem.at[n])
        for n, (a, b) in enumerate(
            (
                (proj, pj),
                (cot_hi.at[:, pl.ds(0, split_at)], chi),
                (cot_lo.at[:, pl.ds(0, split_at)], clo),
                (out_w, oparts),
            )
        )
    ]
    for load in loads:
        load.start()
    greet(seq, head, seqs, heads)
    loads[3].wait()
    owh[...], owl[...] = halves(oparts[...])
    expand = head_lanes(chans)
    tri_r = lax.broadcasted_iota(jnp.int32, (BLOCK, BLOCK), 0)
    tri_c = lax.broadcasted_iota(jnp.int32, (BLOCK, BLOCK), 1)
    anticausal = tri_r <= tri_c
    upper = anticausal.astype(F32)
    wide_o[...] = jnp.zeros_like(wide_o)
    chan_o[...] = jnp.zeros_like(chan_o)
    head_acc[...] = jnp.zeros_like(head_acc)
    run[...] = jnp.zeros_like(run)
    loads[0].wait()
    groups = tokens // 128
    turned_stats = stat_in[...].T
    inner_total = float(heads * chans)
    gain_row, skip_row = chan_p[0:1, :], chan_p[1:2, :]
    for n in range(groups):
        here = slice(n * 128, n * 128 + 128)
        scale = lax.rsqrt(turned_stats[:, n : n + 1] / inner_total + EPSILON)
        cross = turned_stats[:, groups + n : groups + n + 1]
        columns[here, 0:1] = scale
        columns[here, 1:2] = scale * scale * scale * (cross / inner_total)

    def conv_load(b, slot):
        return pltpu.make_async_copy(
            conv_in.at[pl.ds(pl.multiple_of(b * BLOCK, BLOCK), BLOCK)],
            conv_buf.at[slot],
            conv_sem.at[slot],
        )

    def conv_of(n, b, following):
        slot = lax.rem(n, 2)
        conv_load(b, slot).wait()
        conv_load(following, 1 - slot).start()
        return conv_buf[slot, :, :wide]

    conv_load(blocks - 1, 0).start()

    @pl.loop(0, blocks)
    def _(b):
        at = pl.multiple_of(b * BLOCK, BLOCK)
        here = pl.ds(at, BLOCK)
        gate = pj[pl.ds(at + 8, BLOCK), 0:chans]
        ngh[here, :], ngl[here, :] = halves(
            mixed_in[here, :] * (gate * logistic(gate)) * columns[here, 0:1] * gain_row
        )

    reduce = LineReduce(
        parts, y_in, z_in, (y_send, y_recv, z_send, z_recv), seq, head, heads, partner, 3
    )

    ins = reduce.ins

    def produce(step):
        first = reduce.target(step) * ins
        rows = pl.ds(pl.multiple_of(first * chunk, 8), ins * chunk)
        out = dot3((ngh[rows, :], ngl[rows, :]), (owh[...], owl[...]), 1, 0)
        for n in range(ins):
            parts[first + n] = out[n * chunk : (n + 1) * chunk]

    for load in loads[1:3]:
        load.wait()

    def weight_parts(left_hi, left_lo, hi, lo, then):
        for n in range(2):
            cols = pl.ds(n * split_at, split_at)
            oparts[:, n * split_at : (n + 1) * split_at] = dot3(
                (left_hi[...], left_lo[...]), (chi[...], clo[...]), 0, 0
            )
            source, cols = ((hi, lo), pl.ds(split_at, split_at)) if n == 0 else (then, None)
            if source is None:
                continue
            cols = pl.ds(split_at, split_at) if n == 0 else pl.ds(0, split_at)
            more = [
                pltpu.make_async_copy(a.at[:, cols], b, load_sem.at[1 + m])
                for m, (a, b) in enumerate(zip(source, (chi, clo)))
            ]
            for load in more:
                load.start()
            if n == 0:
                for load in more:
                    load.wait()
        return more

    hat_load = weight_parts(ngh, ngl, cot_hi, cot_lo, (hat_hi, hat_lo))
    out_sum = SeqSum(oparts, 0, keep_o, core_o, x_o, o_sems, out_o, seq, head, seqs)
    out_sum.begin()

    @pl.loop(0, reduce.outs)
    def _(step):
        produce(step)

        @pl.when(step == 0)
        def _():
            reduce.give(jnp.int32(0))

    out_sum.pair()
    reduce.give(jnp.int32(1))
    reduce.give(jnp.int32(2))

    def poll(n, base):
        @pl.when(lax.rem(n, pace) == pace - 1)
        def _():
            reduce.reduce(base + n // pace)

    pace = max(1, blocks // 2)

    @pl.loop(0, blocks)
    def _(back):
        b = blocks - 1 - back
        at = pl.multiple_of(b * BLOCK, BLOCK)
        here = pl.ds(at, BLOCK)
        scale = columns[here, 0:1]
        gate = pj[pl.ds(at + 8, BLOCK), 0:chans]
        sig = logistic(gate)
        gate_act = gate * sig
        mixed = mixed_in[here, :]
        gated = mixed * gate_act
        grad_ng = cross_in[here, :]
        grad_gated = scale * (grad_ng * gain_row) - gated * columns[here, 1:2]
        grad_mixed = grad_gated * gate_act
        gmix[here, :] = grad_mixed
        gp_hi[here, 0:chans], gp_lo[here, 0:chans] = halves(
            grad_gated * mixed * (sig * (1.0 + gate * (1.0 - sig)))
        )
        conv = conv_of(back, b, jnp.maximum(b - 1, 0))
        act = conv * logistic(conv)
        chan_o[0:1, :] = chan_o[0:1, :] + jnp.sum(grad_ng * (gated * scale), 0, keepdims=True)
        chan_o[1:2, :] = chan_o[1:2, :] + jnp.sum(grad_mixed * act[:, :chans], 0, keepdims=True)
        early = grad_mixed * spread(jnp.exp(cum_in[here, :]), expand)
        adj[b] = run[...]
        run[...] = row_scale(cum_in[pl.ds(at + BLOCK - 1, 1), :], expand) * run[...] + dotx(
            early, act[:, chans + NSTATE :], 0, 0
        )
        gconv[here, chans + NSTATE :] = dotx(early, state_in[b], 1, 0)
        poll(back, 0)

    total = jnp.zeros((1, 128), F32)
    for b in range(blocks):
        total = total + cum_in[(b + 1) * BLOCK - 1 : (b + 1) * BLOCK, :]
    exch[seq, 0:chans, :] = run[...]
    exch[seq, chans : chans + 8, :] = jnp.broadcast_to(total, (8, 128))

    def state_copy(at, j, to):
        return remote(exch.at[at], exch.at[at], s_send.at[j - 1], s_recv.at[j - 1], to, head)

    for j in range(1, seqs):

        @pl.when(seq - j >= 0)
        def _():
            state_copy(seq, j, seq - j).start()

    for load in hat_load:
        load.wait()
    weight_parts(gp_hi.at[:, 0:chans], gp_lo.at[:, 0:chans], hat_hi, hat_lo, None)
    oparts[...] = oparts[...] * gain[...]
    gate_sum = SeqSum(oparts, 0, keep_g, core_g, x_g, g_sems, gate_o, seq, head, seqs)
    gate_sum.begin()
    reduce.reduce(2)

    @pl.loop(0, blocks)
    def _(b):
        at = pl.multiple_of(b * BLOCK, BLOCK)
        here = pl.ds(at, BLOCK)
        conv = conv_of(b, b, lax.rem(b + 1, blocks))
        act = conv * logistic(conv)
        writes, reads = act[:, chans : chans + NSTATE], act[:, chans + NSTATE :]
        scores = dotx(writes, reads, 1, 1)
        cum = cum_in[here, :]
        turned = cum.T
        fed_all = act[:, :chans] * spread(step_in[here, :], expand)
        grad_scores = jnp.zeros((BLOCK, BLOCK), F32)
        for first_lane, end in lanes_of(chans):
            fed = fed_all[:, first_lane:end]
            grad = gmix[here, first_lane:end]
            grad_parts, grad_turned = halves(grad), halves(grad.T)
            lane = lax.broadcasted_iota(jnp.int32, fed.shape, 1)
            outs = []
            for start in range(first_lane, end, HEADDIM):
                decay = decay_turned(cum, turned, start // HEADDIM, anticausal)
                inside = (lane // HEADDIM) == (start - first_lane) // HEADDIM
                grad_scores = grad_scores + decay * dot3(
                    halves(jnp.where(inside, fed, 0.0)), grad_turned, 1, 0
                )
                outs.append(dot3(halves(decay * scores), grad_parts, 1, 0))
            out = outs[0]
            if len(outs) == 2:
                out = jnp.where(lane < HEADDIM, outs[0], outs[1])
            fedg[here, first_lane:end] = out
        gconv[here, chans : chans + NSTATE] = dotx(grad_scores, reads, 1, 0)
        gconv[here, chans + NSTATE :] = gconv[here, chans + NSTATE :] + dotx(grad_scores, writes, 0, 0)
        poll(b, 3)

        @pl.when(b == 0)
        def _():
            gate_sum.pair()


    run[...] = jnp.zeros_like(run)
    for back in range(seqs - 1):
        later = seqs - 1 - back

        @pl.when(later > seq)
        def _():
            for j in range(1, seqs):

                @pl.when(later - seq == j)
                def _():
                    state_copy(later, j, partner).wait_recv()

            run[...] = (
                row_scale(exch[later, chans : chans + 1, :], expand) * run[...]
                + exch[later, 0:chans, :]
            )

    for b in range(blocks - 1, -1, -1):
        adj[b] = adj[b] + run[...]
        run[...] = row_scale(cum_in[(b + 1) * BLOCK - 1 : (b + 1) * BLOCK, :], expand) * run[...]

    lane_ones = jnp.ones((8, NSTATE), F32)

    @pl.loop(0, blocks)
    def _(b):
        at = pl.multiple_of(b * BLOCK, BLOCK)
        here = pl.ds(at, BLOCK)
        conv = conv_of(b, b, lax.rem(b + 1, blocks))
        sig = logistic(conv)
        act = conv * sig
        slope = sig * (1.0 + conv * (1.0 - sig))
        inner, writes = act[:, :chans], act[:, chans : chans + NSTATE]
        cum = cum_in[here, :]
        step = step_in[here, :]
        last = cum[BLOCK - 1 : BLOCK, :]
        step_wide = spread(step, expand)
        tails = spread(jnp.exp(last - cum), expand)
        fed = inner * step_wide
        grad_state = adj[b]
        state_parts = halves(grad_state)
        from_state = tails * dot3(halves(writes), state_parts, 1, 1)
        grad_fed = fedg[here, :] + from_state
        grad_mixed = gmix[here, :]
        grad_writes = gconv[here, chans : chans + NSTATE] + dot3(halves(fed * tails), state_parts, 1, 0)
        direct = gather_heads(inner * grad_fed, expand)
        scanned = mixed_in[here, :] - skip_row * inner
        grad_cum = dotx(grad_mixed * scanned - fed * grad_fed, expand, 1, 1)
        kept = dotx(expand, grad_state * state_in[b], 1, 0)
        kept = dotx(lane_ones, kept, 1, 1)[0:1, :] * jnp.exp(last)
        grad_last = kept + jnp.sum(gather_heads(fed * from_state, expand), 0, keepdims=True)
        grad_log = dotx(upper, grad_cum, 1, 0) + grad_last
        rate = head_p[1:2, :]
        head_acc[1:2, :] = head_acc[1:2, :] + jnp.sum(step * grad_log, 0, keepdims=True) * rate
        arg = pj[pl.ds(at + 8, BLOCK), span + 2 * NSTATE : pad] + head_p[0:1, :]
        grad_arg = (direct + rate * grad_log) * logistic(arg) * head_p[2:3, :]
        head_acc[0:1, :] = head_acc[0:1, :] + jnp.sum(grad_arg, 0, keepdims=True)
        gp_hi[here, span + 2 * NSTATE : pad], gp_lo[here, span + 2 * NSTATE : pad] = halves(
            grad_arg
        )
        gconv[here, 0:chans] = (step_wide * grad_fed + skip_row * grad_mixed) * slope[:, :chans]
        gconv[here, chans : chans + NSTATE] = grad_writes * slope[:, chans : chans + NSTATE]
        gconv[here, chans + NSTATE :] = gconv[here, chans + NSTATE :] * slope[:, chans + NSTATE :]

        @pl.when(b == blocks // 2 - 1)
        def _():
            reduce.reduce(5)

    out_sum.total()
    edge = remote(
        gconv.at[pl.ds(0, 8)],
        gconv.at[pl.ds(tokens, 8)],
        e_send,
        e_recv,
        lax.rem(seq + seqs - 1, seqs),
        head,
    )
    edge.start()
    head_o[...] = head_acc[...]

    def conv_back(b):
        at = pl.multiple_of(b * BLOCK, BLOCK)
        here = pl.ds(at, BLOCK)
        before = pj[pl.ds(at + 8, BLOCK), chans : span + 2 * NSTATE]
        ahead = gconv[pl.ds(at, BLOCK + 8), :]
        grad = ahead[0:BLOCK, :]
        grad_pre = jnp.zeros((BLOCK, wide), F32)
        for k in range(WIDTH):
            later = ahead[3 - k : 3 - k + BLOCK, :]
            grad_pre = grad_pre + conv_p[k : k + 1, :] * later
            wide_o[k : k + 1, :] = wide_o[k : k + 1, :] + jnp.sum(
                later * before, 0, keepdims=True
            )
        wide_o[4:5, :] = wide_o[4:5, :] + jnp.sum(grad, 0, keepdims=True)
        (
            gp_hi[here, chans : span + 2 * NSTATE],
            gp_lo[here, chans : span + 2 * NSTATE],
        ) = halves(grad_pre)

    @pl.loop(0, blocks - 1)
    def _(b):
        conv_back(b)

    reduce.reduce(6)
    edge.wait()
    gconv[tokens : tokens + 8, :] = jnp.where(seq < seqs - 1, gconv[tokens : tokens + 8, :], 0.0)

    @pl.loop(blocks - 1, blocks)
    def _(b):
        conv_back(b)

    gate_sum.total()
    reduce.reduce(7)
    reduce.last()
    result_o[...] = resid[...] + parts[head]
    conv_load(0, 0).wait()
    reduce.finish()
    for j in range(1, seqs):

        @pl.when(seq - j >= 0)
        def _():
            state_copy(seq, j, seq - j).wait_send()

    out_sum.end()
    gate_sum.end()


def backward(proj, hat, kept, out_w, resid, conv_p, head_p, chan_p, gain, seqs, heads):
    (cot_hi, cot_lo, conv, cum, step, state, mixed, cross, stat) = kept
    tokens, pad = cum.shape[0], proj.shape[1]
    chunk, width = resid.shape
    chans = out_w.shape[0]
    ins = inner_count(heads)
    outs = heads // ins
    wide = chans + 2 * NSTATE
    blocks = tokens // BLOCK
    half = chans // 2
    rounds = (seqs // 2).bit_length() - 1
    anywhere = pl.BlockSpec(memory_space=pl.ANY)
    local = pl.BlockSpec(memory_space=pltpu.VMEM)
    sems = pltpu.SemaphoreType.DMA
    shape = jax.ShapeDtypeStruct
    return pl.pallas_call(
        functools.partial(backward_kernel, (seqs, heads, chunk, chans, pad)),
        out_shape=(
            shape((chunk, width), F32),
            shape((tokens, pad), BF16),
            shape((tokens, pad), BF16),
            shape((chans, width), F32),
            shape((chans, width), F32),
            shape((8, wide), F32),
            shape((8, chans), F32),
            shape((8, 128), F32),
        ),
        in_specs=[anywhere] * 6 + [local] * 6 + [anywhere] + [local] * 5,
        out_specs=(local, local, local, anywhere, anywhere, local, local, local),
        scratch_shapes=[
            pltpu.VMEM((8 + tokens, pad), F32),
            pltpu.VMEM((tokens, chans), BF16),
            pltpu.VMEM((tokens, chans), BF16),
            pltpu.VMEM((chans, width), BF16),
            pltpu.VMEM((chans, width), BF16),
            pltpu.VMEM((tokens, chans), F32),
            pltpu.VMEM((tokens, chans), F32),
            pltpu.VMEM((blocks, chans, NSTATE), F32),
            pltpu.VMEM((chans, NSTATE), F32),
            pltpu.VMEM((seqs, chans + 8, NSTATE), F32),
            pltpu.VMEM((tokens + 8, wide), F32),
            pltpu.VMEM((heads, chunk, width), F32),
            pltpu.VMEM((outs * (ins - 1), chunk, width), F32),
            pltpu.VMEM((outs + 1, chunk, width), F32),
            pltpu.VMEM((tokens, width // 2), BF16),
            pltpu.VMEM((tokens, width // 2), BF16),
            pltpu.VMEM((chans, width), F32),
            pltpu.VMEM((tokens, 128), F32),
            pltpu.VMEM((2, BLOCK, full_lanes(wide)), F32),
            pltpu.VMEM((8, 128), F32),
            *seq_sum_scratch(half, width, rounds),
            *seq_sum_scratch(half, width, rounds),
            *line_reduce_sems(ins, outs),
            sems((4,)),
            sems((seqs - 1,)),
            sems((seqs - 1,)),
            sems,
            sems,
            sems((2,)),
        ],
        compiler_params=pltpu.CompilerParams(
            collective_id=4, has_side_effects=True, vmem_limit_bytes=VMEM_LIMIT
        ),
        name="backward",
    )(
        proj, cot_hi, cot_lo, *hat, conv, cum, step, state, mixed, cross, stat,
        out_w, resid, conv_p, head_p, chan_p, gain,
    )


def on_device(
    residual_in,
    norm_gain,
    gate_weight,
    inner_weight,
    bc_weight,
    step_weight,
    conv_inner_weight,
    conv_inner_bias,
    conv_bc_weight,
    conv_bc_bias,
    step_bias,
    decay_log,
    skip_gain,
    gated_gain,
    out_weight,
    cotangent,
):
    seqs, heads = lax.axis_size("seq"), lax.axis_size("head")
    width = residual_in.shape[2]
    chans = gate_weight.shape[0]
    heads_here = step_weight.shape[0]
    spare = 128 - heads_here
    resid = residual_in.reshape(-1, width)
    cot = cotangent.reshape(-1, width)
    gain = norm_gain.reshape(1, width)

    def eight(part):
        return jnp.pad(part, ((0, 8 - part.shape[0]), (0, 0)))

    def by_head(*parts):
        return eight(jnp.pad(jnp.stack(parts), ((0, 0), (0, spare))))

    conv_p = eight(
        jnp.concatenate(
            [
                jnp.concatenate([conv_inner_weight, conv_bc_weight], 1),
                jnp.concatenate([conv_inner_bias, conv_bc_bias])[None],
            ],
            0,
        )
    )
    head_p = by_head(step_bias, -jnp.exp(decay_log), jnp.ones_like(step_bias))
    chan_p = eight(jnp.stack([gated_gain, jnp.repeat(skip_gain, HEADDIM)]))
    hat_hi, hat_lo, projected, weight_hi, weight_lo, *kept = front(
        resid,
        cot,
        gain,
        gate_weight,
        inner_weight,
        bc_weight,
        step_weight,
        out_weight,
        conv_p,
        head_p,
        chan_p,
        seqs,
        heads,
    )
    (
        result,
        grad_hi,
        grad_lo,
        out_weight_grad,
        gate_weight_grad,
        wide_sums,
        chan_sums,
        head_sums,
    ) = backward(
        projected,
        (hat_hi, hat_lo),
        kept,
        out_weight,
        resid,
        conv_p,
        head_p,
        chan_p,
        gain,
        seqs,
        heads,
    )

    residual_grad, inner_weight_grad, bc_pieces, sums, glob = tail(
        (grad_hi, grad_lo),
        (hat_hi, hat_lo),
        (weight_hi, weight_lo),
        (wide_sums, chan_sums, head_sums),
        resid,
        cot,
        gain,
        seqs,
        heads,
        chans,
    )
    across = width // bc_pieces.shape[2]
    bc_weight_grad = jnp.transpose(
        bc_pieces.reshape(2 * NSTATE // 8, across, 8, width // across), (1, 3, 0, 2)
    ).reshape(width, 2 * NSTATE)
    chan_at = full_lanes(chans + 2 * NSTATE)
    head_at = chan_at + full_lanes(chans)
    skip_wide = sums[1, 1, chan_at : chan_at + chans]
    return (
        result.reshape(residual_in.shape),
        residual_grad.reshape(residual_in.shape),
        glob[:4].reshape(width),
        gate_weight_grad,
        inner_weight_grad,
        bc_weight_grad,
        sums[0, :heads_here],
        sums[1, :WIDTH, :chans],
        sums[1, WIDTH, :chans],
        glob[8 : 8 + WIDTH, : 2 * NSTATE],
        glob[8 + WIDTH, : 2 * NSTATE],
        sums[1, 0, head_at : head_at + heads_here],
        sums[1, 1, head_at : head_at + heads_here],
        jnp.sum(skip_wide.reshape(heads_here, HEADDIM), axis=1),
        sums[1, 0, chan_at : chan_at + chans],
        out_weight_grad,
    )


def solution(mesh):
    placed = (
        P(None, ("seq", "head"), None),
        P(),
        P("head", None),
        P("head", None),
        P(),
        P("head", None),
        P(None, "head"),
        P("head"),
        P(),
        P(),
        P("head"),
        P("head"),
        P("head"),
        P("head"),
        P("head", None),
        P(None, ("seq", "head"), None),
    )
    return jax.shard_map(
        on_device,
        mesh=mesh,
        in_specs=placed,
        out_specs=(
            P(None, ("seq", "head"), None),
            P(None, ("seq", "head"), None),
            P(),
            P("head", None),
            P("head", None),
            P(),
            P("head", None),
            P(None, "head"),
            P("head"),
            P(),
            P(),
            P("head"),
            P("head"),
            P("head"),
            P("head"),
            P("head", None),
        ),
        check_vma=False,
    )
```

```python
import functools

import jax
import jax.numpy as jnp
from jax import lax
from jax.experimental import pallas as pl
from jax.experimental.pallas import tpu as pltpu
from jax.sharding import PartitionSpec as P

HEADDIM = 64
NSTATE = 128
WIDTH = 4
BLOCK = 256
EPSILON = 1e-05
EXACT = lax.Precision.HIGHEST
MESH = pl.DeviceIdType.MESH
F32 = jnp.float32
BF16 = jnp.bfloat16
VMEM_LIMIT = 66000000


def dot3(left, right, left_dim, right_dim):
    dims = (((left_dim,), (right_dim,)), ((), ()))
    one = functools.partial(lax.dot_general, dimension_numbers=dims, preferred_element_type=F32)
    return one(left[0], right[0]) + (one(left[0], right[1]) + one(left[1], right[0]))


def remote(source, target, send_sem, recv_sem, seq, head):
    return pltpu.make_async_remote_copy(
        src_ref=source,
        dst_ref=target,
        send_sem=send_sem,
        recv_sem=recv_sem,
        device_id=(seq, head),
        device_id_type=MESH,
    )


def greet(seq, head, seqs, heads):
    barrier = pltpu.get_barrier_semaphore()
    for j in range(1, seqs):
        pl.semaphore_signal(
            barrier, inc=1, device_id=(lax.rem(seq + j, seqs), head), device_id_type=MESH
        )
    for j in range(1, heads):
        pl.semaphore_signal(
            barrier, inc=1, device_id=(seq, lax.rem(head + j, heads)), device_id_type=MESH
        )
    pl.semaphore_wait(barrier, seqs + heads - 2)


def inner_count(heads):
    return 2 if heads <= 8 else 4


class SeqSum:
    def __init__(self, source, base, keep, core_in, x_in, sems, result, seq, head, seqs):
        self.source, self.base, self.keep, self.core_in, self.x_in = source, base, keep, core_in, x_in
        self.sems, self.result, self.seq, self.head = sems, result, seq, head
        self.rounds = (seqs // 2).bit_length() - 1
        self.half = keep.shape[0]
        self.side = lax.rem(seq, 2)
        self.partner = seq + 1 - 2 * self.side

    def rows(self, side, base):
        return pl.ds(pl.multiple_of(base + side * self.half, 8), self.half)

    def begin(self):
        self.keep[...] = self.source[self.rows(self.side, self.base), :]
        self.core = remote(
            self.source.at[self.rows(1 - self.side, self.base)],
            self.core_in,
            self.sems.at[0],
            self.sems.at[1],
            self.partner,
            self.head,
        )
        self.core.start()

    def cross(self, source, turn):
        away = 2 << turn
        far = self.seq + away - 2 * away * lax.rem(self.seq // away, 2)
        return remote(
            source,
            self.x_in.at[turn],
            self.sems.at[5 + 2 * turn],
            self.sems.at[6 + 2 * turn],
            far,
            self.head,
        )

    def pair(self):
        self.core.wait()
        self.keep[...] = self.keep[...] + self.core_in[...]

    def start(self):
        self.cross(self.keep, 0).start()

    def total(self):
        now, new = self.keep, self.core_in
        for turn in range(self.rounds):
            self.cross(now, turn).wait()
            new[...] = now[...] + self.x_in[turn]
            now, new = new, now
            if turn + 1 < self.rounds:
                self.cross(now, turn + 1).start()
        mine = self.result.at[self.rows(self.side, 0)]
        self.now = now
        self.put = pltpu.make_async_copy(now, mine, self.sems.at[2])
        self.put.start()
        self.final = remote(
            now, mine, self.sems.at[3], self.sems.at[4], self.partner, self.head
        )
        self.final.start()

    def end(self):
        self.final.wait_send()
        remote(
            self.now,
            self.result.at[self.rows(1 - self.side, 0)],
            self.sems.at[3],
            self.sems.at[4],
            self.partner,
            self.head,
        ).wait_recv()
        self.put.wait()


def seq_sum_scratch(half, width, rounds):
    return [
        pltpu.VMEM((half, width), F32),
        pltpu.VMEM((half, width), F32),
        pltpu.VMEM((rounds, half, width), F32),
        pltpu.SemaphoreType.DMA((5 + 2 * rounds,)),
    ]


def tail_kernel(dims, *refs):
    seqs, heads, chunk, chans, pad = dims
    (
        gp_hi, gp_lo, hat_hi, hat_lo, w_hi, w_lo, gate_half, wide_in, chan_in, head_in, resid, cot, gain,
        resid_grad, gate_out, inner_out, bc_out, small_out, glob_out,
        gph, gpl, hth, htl, wh, wl, parts, y_in, z_in, joined, keep, core_in, x_in, i_sems, keep_g, core_g, x_g, g_sems,
        bc_part, bc_half, bc_seq, bc_quart, bc_head, bc_full,
        small_mine, small_pair, small_far, glob_mine, glob_pair, glob_far, small_head, gain_sum,
        load_sem, y_send, y_recv, z_send, z_recv,
        a_sem, b_send, b_recv, c_send, c_recv, m_sem, h_send, h_recv, put_sem,
    ) = refs
    width = gain.shape[1]
    span = 2 * chans
    fars = seqs // 2
    seq, head = lax.axis_index("seq"), lax.axis_index("head")
    side, far = lax.rem(seq, 2), seq // 2
    partner = seq + 1 - 2 * side
    loads = [
        pltpu.make_async_copy(a, b, load_sem.at[n])
        for n, (a, b) in enumerate(
            ((gp_hi, gph), (w_hi, wh), (gp_lo, gpl), (w_lo, wl), (hat_hi, hth), (hat_lo, htl))
        )
    ]
    for load in loads:
        load.start()
    gate_load = pltpu.make_async_copy(gate_half, keep_g, load_sem.at[6])
    gate_load.start()
    greet(seq, head, seqs, heads)
    reduce = LineReduce(
        parts, y_in, z_in, (y_send, y_recv, z_send, z_recv), seq, head, heads, partner, 2
    )
    gate_load.wait()
    gate = SeqSum(None, 0, keep_g, core_g, x_g, g_sems, gate_out, seq, head, seqs)
    gate.start()
    for load in loads[:4]:
        load.wait()

    def chunk_rows(where):
        return pl.ds(pl.multiple_of(where * chunk, 8), chunk)

    ins = reduce.ins

    def produce(step):
        first = reduce.target(step) * ins
        rows = pl.ds(pl.multiple_of(first * chunk, 8), ins * chunk)
        out = dot3((gph[rows, :], gpl[rows, :]), (wh[...], wl[...]), 1, 0)
        for n in range(ins):
            parts[first + n] = out[n * chunk : (n + 1) * chunk]

    produce(jnp.int32(0))
    reduce.give(jnp.int32(0))
    gain_row = gain[...]
    for load in loads[4:]:
        load.wait()

    small_mine[...] = jnp.zeros_like(small_mine)
    offset = 0
    for block in (wide_in, chan_in, head_in):
        small_mine[1, :, offset : offset + block.shape[1]] = block[...]
        offset += full_lanes(block.shape[1])
    gain_sum[...] = jnp.zeros_like(gain_sum)

    def gain_part(step):
        first = reduce.target(step) * ins
        rows = pl.ds(pl.multiple_of(first * chunk, 8), ins * chunk)
        hat = hth[rows, :].astype(F32) + htl[rows, :].astype(F32)
        for n in range(ins):
            gain_sum[...] = gain_sum[...] + jnp.sum(
                parts[first + n] * hat[n * chunk : (n + 1) * chunk], 0, keepdims=True
            )

    gain_part(jnp.int32(0))

    joined[span:, :] = (
        dot3((gph[:, span:], gpl[:, span:]), (hth[...], htl[...]), 0, 0) * gain_row
    )
    pieces, _, lanes = bc_part.shape
    across = width // lanes
    for row in range(pieces // across):
        for col in range(across):
            bc_part[row * across + col] = joined[
                span + row * 8 : span + row * 8 + 8, col * lanes : (col + 1) * lanes
            ]
    mine = pl.ds(side * (pieces // 2), pieces // 2)
    theirs = pl.ds((1 - side) * (pieces // 2), pieces // 2)
    bc_core = remote(
        bc_part.at[theirs], bc_half, a_sem.at[0], a_sem.at[1], partner, head
    )
    bc_core.start()
    reduce.give(jnp.int32(1))

    @pl.loop(1, reduce.outs)
    def _(step):
        produce(step)
        gain_part(step)

    def others(make):
        copies = []
        for j in range(1, fars):
            copies.append(make(j, lax.rem(far + j, fars)))
            copies[-1].start()
        return copies

    bc_core.wait()
    bc_half[...] = bc_half[...] + bc_part[mine]
    cross_bc = others(
        lambda j, to: remote(
            bc_half.at[pl.ds(to * heads, heads)],
            bc_seq.at[j - 1],
            b_send.at[0, j - 1],
            b_recv.at[0, j - 1],
            2 * to + side,
            head,
        )
    )
    reduce.reduce(0)
    low = chans if chans % 128 == 0 else 0
    rows = dot3((gph[:, low:span], gpl[:, low:span]), (hth[...], htl[...]), 0, 0)
    joined[low:span, :] = rows * gain_row
    inner = SeqSum(
        joined, chans, keep, core_in, x_in, i_sems, inner_out, seq, head, seqs
    )
    inner.begin()
    small_mine[0] = joined[span + 2 * NSTATE : span + 2 * NSTATE + 8, :]
    glob_mine[...] = jnp.zeros_like(glob_mine)
    quarter = glob_mine.shape[1]
    for n in range(width // quarter):
        glob_mine[n : n + 1, :] = gain_sum[:, n * quarter : (n + 1) * quarter]
    glob_mine[8:16, 0 : 2 * NSTATE] = wide_in[:, chans:]
    reduce.reduce(1)
    for copy in cross_bc:
        copy.wait()
    quarter = bc_half[pl.ds(far * heads, heads)]
    for j in range(fars - 1):
        quarter = quarter + bc_seq[j]
    bc_quart[...] = quarter

    def to_heads(make):
        copies = []
        for j in range(1, heads):
            copies.append(make(j, lax.rem(head + j, heads)))
            copies[-1].start()
        return copies

    spread_bc = to_heads(
        lambda j, to: remote(
            bc_quart.at[to], bc_head.at[j - 1], c_send.at[0, j - 1], c_recv.at[0, j - 1], seq, to
        )
    )
    inner.pair()
    inner.start()
    small_core = [
        remote(small_mine, small_pair, a_sem.at[2], a_sem.at[3], partner, head),
        remote(glob_mine, glob_pair, a_sem.at[6], a_sem.at[7], partner, head),
    ]
    for copy in small_core:
        copy.start()
    reduce.reduce(2)
    for copy in small_core:
        copy.wait()
    small_far[far] = small_mine[...] + small_pair[...]
    glob_far[far] = glob_mine[...] + glob_pair[...]
    cross_small = others(
        lambda j, to: remote(
            small_far.at[far],
            small_far.at[far],
            m_sem.at[0, j - 1],
            m_sem.at[1, j - 1],
            2 * to + side,
            head,
        )
    ) + others(
        lambda j, to: remote(
            glob_far.at[far],
            glob_far.at[far],
            m_sem.at[2, j - 1],
            m_sem.at[3, j - 1],
            2 * to + side,
            head,
        )
    )
    reduce.reduce(3)
    for copy in spread_bc:
        copy.wait()
    piece = bc_quart[head]
    for j in range(heads - 1):
        piece = piece + bc_head[j]
    block = side * (pieces // 2) + far * heads
    bc_full[block + head] = piece
    gather_bc = to_heads(
        lambda j, to: remote(
            bc_full.at[block + head],
            bc_full.at[block + head],
            c_send.at[1, j - 1],
            c_recv.at[1, j - 1],
            seq,
            to,
        )
    )
    for j in range(1, fars):
        came = lax.rem(far - j + fars, fars)
        remote(
            small_far.at[came], small_far.at[came], m_sem.at[0, j - 1], m_sem.at[1, j - 1],
            partner, head,
        ).wait_recv()
        remote(
            glob_far.at[came], glob_far.at[came], m_sem.at[2, j - 1], m_sem.at[3, j - 1],
            partner, head,
        ).wait_recv()
    total, glob = small_far[0], glob_far[0]
    for j in range(1, fars):
        total = total + small_far[j]
        glob = glob + glob_far[j]
    small_out[...] = total
    small_head[head] = glob
    spread_small = to_heads(
        lambda j, to: remote(
            small_head.at[head], small_head.at[head], h_send.at[j - 1], h_recv.at[j - 1], seq, to
        )
    )
    reduce.reduce(4)
    reduce.reduce(5)
    for j in range(1, heads):
        came = lax.rem(head - j + heads, heads)
        remote(
            bc_full.at[block + came], bc_full.at[block + came],
            c_send.at[1, j - 1], c_recv.at[1, j - 1], partner, head,
        ).wait_recv()
    own_block = pl.ds(block, heads)
    join_bc = others(
        lambda j, to: remote(
            bc_full.at[own_block],
            bc_full.at[own_block],
            b_send.at[1, j - 1],
            b_recv.at[1, j - 1],
            2 * to + side,
            head,
        )
    )
    for j in range(1, heads):
        came = lax.rem(head - j + heads, heads)
        remote(
            small_head.at[came], small_head.at[came], h_send.at[j - 1], h_recv.at[j - 1], seq, came
        ).wait_recv()
    total = small_head[0]
    for j in range(1, heads):
        total = total + small_head[j]
    glob_out[...] = total
    reduce.reduce(6)
    for j in range(1, fars):
        came = side * (pieces // 2) + lax.rem(far - j + fars, fars) * heads
        came = pl.ds(came, heads)
        remote(
            bc_full.at[came], bc_full.at[came], b_send.at[1, j - 1], b_recv.at[1, j - 1],
            partner, head,
        ).wait_recv()
    join_core = remote(
        bc_full.at[mine], bc_full.at[mine], a_sem.at[4], a_sem.at[5], partner, head
    )
    join_core.start()
    gate.total()
    inner.total()
    reduce.reduce(7)
    reduce.last()
    grad_hat = parts[head] * gain_row
    values = resid[...]
    scale = lax.rsqrt(jnp.mean(values * values, axis=1, keepdims=True) + EPSILON)
    row_cross = jnp.sum(grad_hat * values, axis=1, keepdims=True)
    resid_grad[...] = (
        cot[...] + scale * grad_hat - values * (scale * scale * scale * (row_cross / width))
    )
    remote(
        bc_full.at[theirs], bc_full.at[theirs], a_sem.at[4], a_sem.at[5], partner, head
    ).wait_recv()
    bc_put = pltpu.make_async_copy(bc_full, bc_out, put_sem)
    bc_put.start()
    reduce.finish()
    for copy in gather_bc + cross_small + spread_small + join_bc + [join_core]:
        copy.wait_send()
    gate.end()
    inner.end()
    bc_put.wait()


def tail(gp, hat, weight, gate_half, sums, resid, cot, gain, seqs, heads, chans):
    tokens, width = hat[0].shape
    chunk = tokens // heads
    pad = gp[0].shape[1]
    ins = inner_count(heads)
    outs = heads // ins
    rounds = (seqs // 2).bit_length() - 1
    fars = seqs // 2
    lanes = 2 * NSTATE * width // (8 * seqs * heads)
    pieces = seqs * heads
    anywhere = pl.BlockSpec(memory_space=pl.ANY)
    local = pl.BlockSpec(memory_space=pltpu.VMEM)
    sems = pltpu.SemaphoreType.DMA
    return pl.pallas_call(
        functools.partial(tail_kernel, (seqs, heads, chunk, chans, pad)),
        out_shape=(
            jax.ShapeDtypeStruct((chunk, width), F32),
            jax.ShapeDtypeStruct((chans, width), F32),
            jax.ShapeDtypeStruct((chans, width), F32),
            jax.ShapeDtypeStruct((pieces, 8, lanes), F32),
            jax.ShapeDtypeStruct((2, 8, width), F32),
            jax.ShapeDtypeStruct((16, width // 4), F32),
        ),
        in_specs=[anywhere] * 7 + [local] * 6,
        out_specs=(local, anywhere, anywhere, anywhere, local, local),
        scratch_shapes=[
            pltpu.VMEM((tokens, pad), BF16),
            pltpu.VMEM((tokens, pad), BF16),
            pltpu.VMEM((tokens, width), BF16),
            pltpu.VMEM((tokens, width), BF16),
            pltpu.VMEM((pad, width), BF16),
            pltpu.VMEM((pad, width), BF16),
            pltpu.VMEM((heads, chunk, width), F32),
            pltpu.VMEM((outs * (ins - 1), chunk, width), F32),
            pltpu.VMEM((outs + 1, chunk, width), F32),
            pltpu.VMEM((pad, width), F32),
            *seq_sum_scratch(chans // 2, width, rounds),
            *seq_sum_scratch(chans // 2, width, rounds),
            pltpu.VMEM((pieces, 8, lanes), F32),
            pltpu.VMEM((pieces // 2, 8, lanes), F32),
            pltpu.VMEM((fars - 1, heads, 8, lanes), F32),
            pltpu.VMEM((heads, 8, lanes), F32),
            pltpu.VMEM((heads - 1, 8, lanes), F32),
            pltpu.VMEM((pieces, 8, lanes), F32),
            pltpu.VMEM((2, 8, width), F32),
            pltpu.VMEM((2, 8, width), F32),
            pltpu.VMEM((fars, 2, 8, width), F32),
            pltpu.VMEM((16, width // 4), F32),
            pltpu.VMEM((16, width // 4), F32),
            pltpu.VMEM((fars, 16, width // 4), F32),
            pltpu.VMEM((heads, 16, width // 4), F32),
            pltpu.VMEM((1, width), F32),
            sems((7,)),
            *line_reduce_sems(ins, outs),
            sems((8,)),
            sems((2, fars - 1)),
            sems((2, fars - 1)),
            sems((2, heads - 1)),
            sems((2, heads - 1)),
            sems((4, fars - 1)),
            sems((heads - 1,)),
            sems((heads - 1,)),
            sems,
        ],
        compiler_params=pltpu.CompilerParams(
            collective_id=1, has_side_effects=True, vmem_limit_bytes=VMEM_LIMIT
        ),
        name="tail",
    )(*gp, *hat, *weight, gate_half, *sums, resid, cot, gain)


def dotx(left, right, left_dim, right_dim):
    return lax.dot_general(
        left,
        right,
        (((left_dim,), (right_dim,)), ((), ())),
        precision=EXACT,
        preferred_element_type=F32,
    )


def dot3x(left, right, left_dim, right_dim):
    return dot3(halves(left), halves(right), left_dim, right_dim)


def halves(values):
    top = values.astype(BF16)
    return (top, (values - top.astype(F32)).astype(BF16))


def head_lanes(chans):
    row = lax.broadcasted_iota(jnp.int32, (128, chans), 0)
    col = lax.broadcasted_iota(jnp.int32, (128, chans), 1)
    return (row == col // HEADDIM).astype(F32)


def lanes_of(chans):
    return [(lo, min(lo + 2 * HEADDIM, chans)) for lo in range(0, chans, 2 * HEADDIM)]


def spread(values, expand):
    top, low = halves(values)
    expand = expand.astype(BF16)
    dims = (((1,), (0,)), ((), ()))
    one = functools.partial(lax.dot_general, dimension_numbers=dims, preferred_element_type=F32)
    return one(top, expand) + one(low, expand)


def gather_heads(values, expand):
    top, low = halves(values)
    expand = expand.astype(BF16)
    dims = (((1,), (1,)), ((), ()))
    one = functools.partial(lax.dot_general, dimension_numbers=dims, preferred_element_type=F32)
    return one(top, expand) + one(low, expand)


def row_scale(total_row, expand):
    top, low = halves(jnp.broadcast_to(jnp.exp(total_row), (128, 128)).T)
    expand = expand.astype(BF16)
    dims = (((0,), (0,)), ((), ()))
    one = functools.partial(lax.dot_general, dimension_numbers=dims, preferred_element_type=F32)
    return one(expand, top) + one(expand, low)


def logistic(values):
    return 1.0 / (1.0 + jnp.exp(-values))


def decay_of(cum, cum_turned, h, causal):
    return jnp.where(causal, jnp.exp(cum[:, h : h + 1] - cum_turned[h : h + 1, :]), 0.0)


def decay_turned(cum, cum_turned, h, anticausal):
    return jnp.where(anticausal, jnp.exp(cum_turned[h : h + 1, :] - cum[:, h : h + 1]), 0.0)


class LineGather:
    def __init__(self, parts, sems, seq, head, heads):
        self.parts, self.seq = parts, seq
        self.z_send, self.z_recv, self.y_send, self.y_recv = sems
        self.ins = inner_count(heads)
        self.outs = heads // self.ins
        self.at_out, self.at_in = head // self.ins, lax.rem(head, self.ins)
        chunk = parts.shape[1]
        half, early = chunk // 2, max(8, chunk // 8)
        self.halves = {0: pl.ds(0, half), self.ins: pl.ds(half, half)}
        self.sides = (pl.ds(0, half), pl.ds(chunk - early, early), pl.ds(half, half - early))

    def z_copy(self, place, j, up):
        where = place * self.ins + lax.rem(self.at_in + j, self.ins)
        piece = self.parts.at[where, self.halves.get(j, self.sides[1])]
        return remote(
            piece,
            piece,
            self.z_send.at[place, up, j],
            self.z_recv.at[place, j],
            self.seq,
            (self.at_out + 2 * up - 1) * self.ins + self.at_in,
        )

    def y_copy(self, where, j, part):
        place = where // self.ins
        piece = self.parts.at[where, self.sides[part]]
        return remote(
            piece,
            piece,
            self.y_send.at[place, j, part],
            self.y_recv.at[place, j, part],
            self.seq,
            self.at_out * self.ins + lax.rem(self.at_in + 1 + j, self.ins),
        )

    def onward(self, place, j, act):
        @pl.when((place >= self.at_out) & (self.at_out > 0))
        def _():
            act(self.z_copy(place, j, 0))

        @pl.when((place <= self.at_out) & (self.at_out < self.outs - 1))
        def _():
            act(self.z_copy(place, j, 1))

    def half(self, place, half):
        self.onward(place, half, lambda copy: copy.start())
        for j in range(self.ins - 1):
            self.y_copy(place * self.ins + self.at_in, j, 2 if half else 0).start()

    def start(self):
        for j in range(self.ins - 1):
            self.y_copy(self.at_out * self.ins + self.at_in, j, 1).start()
        self.half(self.at_out, 0)

    def second(self):
        self.half(self.at_out, self.ins)

    def early(self):
        for j in range(self.ins - 1):
            where = self.at_out * self.ins + lax.rem(self.at_in + self.ins - 1 - j, self.ins)
            self.y_copy(where, j, 1).wait_recv()
            self.onward(self.at_out, self.ins - 1 - j, lambda copy: copy.start())

    def relay(self, distance, part):
        for side in range(2):
            place = self.at_out + (2 * side - 1) * distance

            @pl.when((place >= 0) & (place < self.outs))
            def _():
                self.z_copy(place, part * self.ins, 0).wait_recv()
                self.half(place, part * self.ins)
                for j in range(1, self.ins if part else 1):
                    self.z_copy(place, j, 0).wait_recv()
                    self.onward(place, j, lambda copy: copy.start())

    def use(self, distance, consume):
        @pl.loop(0, 2 * self.ins)
        def _(n):
            side, j = n // self.ins, lax.rem(n, self.ins)
            late = (j + self.ins - 1) // self.ins
            away = distance - late
            place = self.at_out + (2 * side - 1) * away

            @pl.when(
                (place >= 0) & (place < self.outs) & (away >= 0) & (away + 1 - side > 0)
            )
            def _():
                where = place * self.ins + lax.rem(self.at_in + self.ins - j, self.ins)

                @pl.when(j > 0)
                def _():
                    self.y_copy(where, j - 1, 0).wait_recv()
                    self.y_copy(where, j - 1, 2).wait_recv()

                consume(where)

    def finish(self):
        mine = self.at_out * self.ins + self.at_in
        for place in range(self.outs):
            for j in range(self.ins + 1):
                self.onward(place, j, lambda copy: copy.wait_send())
            for j in range(self.ins - 1):
                self.y_copy(place * self.ins + self.at_in, j, 0).wait_send()
                self.y_copy(place * self.ins + self.at_in, j, 2).wait_send()
        for j in range(self.ins - 1):
            self.y_copy(mine, j, 1).wait_send()


def line_gather_sems(ins, outs):
    sems = pltpu.SemaphoreType.DMA
    return [
        sems((outs, 2, ins + 1)),
        sems((outs, ins + 1)),
        sems((outs, ins - 1, 3)),
        sems((outs, ins - 1, 3)),
    ]


def full_lanes(count):
    return -(-count // 128) * 128


def front_kernel(dims, *refs):
    seqs, heads, chunk, chans, pad = dims
    (
        rows, cot, gain, gate_w, inner_w, bc_w, step_w, out_w, conv_p, head_p, chan_p,
        hat_hi, hat_lo, pj_o, w_hi, w_lo,
        cot_hi, cot_lo, conv_hbm, cum_o, step_o, state_o, mixed_o, cross_o, stat_o,
        parts, cot_parts, hi, lo, pj, raw, wh, wl, wth, wtl, owh, owl,
        enter, prefix, run, exch, stat_all, lows,
        za_send, za_recv, ya_send, ya_recv, zb_send, zb_recv, yb_send, yb_recv,
        load_sem, put_sem, e_send, e_recv, s_send, s_recv, t_send, t_recv,
    ) = refs
    tokens = chunk * heads
    blocks = tokens // BLOCK
    span = 2 * chans
    wide = chans + 2 * NSTATE
    seq, head = lax.axis_index("seq"), lax.axis_index("head")
    convs = slice(0, wide)
    scaled = slice(768, 768 + chans)

    loads = [
        pltpu.make_async_copy(gate_w, raw.at[pl.ds(0, chans)], load_sem.at[0]),
        pltpu.make_async_copy(inner_w, raw.at[pl.ds(chans, chans)], load_sem.at[1]),
    ]
    for load in loads:
        load.start()
    values = rows[...]
    parts[head] = values * lax.rsqrt(
        jnp.mean(values * values, axis=1, keepdims=True) + EPSILON
    )
    cot_parts[head] = cot[...]
    greet(seq, head, seqs, heads)
    gather = LineGather(parts, (za_send, za_recv, ya_send, ya_recv), seq, head, heads)
    cotan = LineGather(cot_parts, (zb_send, zb_recv, yb_send, yb_recv), seq, head, heads)
    gather.start()

    raw[span : span + 2 * NSTATE, :] = bc_w[...].T
    raw[span + 2 * NSTATE :, :] = jnp.zeros((raw.shape[0] - span - 2 * NSTATE, raw.shape[1]), F32)
    raw[span + 2 * NSTATE : span + 2 * NSTATE + step_w.shape[0], :] = step_w[...]
    for load in loads:
        load.wait()
    gain_row = gain[...]

    def turn_weights(block):
        here = pl.ds(pl.multiple_of(block * 128, 128), 128)
        piece = raw[here, :]
        wh[here, :], wl[here, :] = halves(piece)
        wth[:, here], wtl[:, here] = halves((piece * gain_row).T)

    @pl.loop(0, pad // 256)
    def _(block):
        turn_weights(block)

    gather.second()
    gather.early()

    @pl.loop(pad // 256, pad // 128)
    def _(block):
        turn_weights(block)

    puts = [
        pltpu.make_async_copy(wh, w_hi, put_sem.at[0]),
        pltpu.make_async_copy(wl, w_lo, put_sem.at[1]),
    ]
    load_w = pltpu.make_async_copy(out_w, raw.at[pl.ds(0, chans)], load_sem.at[0])
    for copy in puts + [load_w]:
        copy.start()

    def chunk_rows(where):
        return pl.ds(pl.multiple_of(where * chunk, 8), chunk)

    def chunk_puts(where, top, low):
        here = chunk_rows(where)
        return [
            pltpu.make_async_copy(hi.at[where], top.at[here], put_sem.at[2 + 2 * where]),
            pltpu.make_async_copy(lo.at[where], low.at[here], put_sem.at[3 + 2 * where]),
        ]

    def project(where):
        top, low = halves(parts[where])
        hi[where] = top
        lo[where] = low
        here = pl.ds(pl.multiple_of(8 + where * chunk, 8), chunk)
        pj[here, :] = dot3((top, low), (wth[...], wtl[...]), 1, 0)
        for put in chunk_puts(where, hat_hi, hat_lo):
            put.start()

    assert gather.outs == 4
    gather.relay(1, 0)
    gather.use(0, project)
    load_w.wait()
    for lane, end in lanes_of(chans):
        owh[:, lane:end], owl[:, lane:end] = halves(raw[lane:end, :].T)
    gather.relay(1, 1)
    gather.relay(2, 0)
    expand = head_lanes(chans)
    gather.use(1, project)
    gather.relay(2, 1)
    gather.relay(3, 0)
    gather.use(2, project)
    gather.relay(3, 1)
    cotan.start()
    gather.use(3, project)
    cotan.second()
    cotan.early()
    gather.use(4, project)
    edge = remote(
        pj.at[pl.ds(tokens, 8)],
        pj.at[pl.ds(0, 8)],
        e_send,
        e_recv,
        lax.rem(seq + 1, seqs),
        head,
    )
    edge.start()
    cotan.relay(1, 0)
    edge.wait()
    pj[0:8, :] = jnp.where(seq > 0, pj[0:8, :], 0.0)
    pj_put = pltpu.make_async_copy(pj, pj_o, put_sem.at[2 + 2 * heads])
    pj_put.start()
    cotan.relay(1, 1)
    cotan.relay(2, 0)
    tri_r = lax.broadcasted_iota(jnp.int32, (BLOCK, BLOCK), 0)
    tri_c = lax.broadcasted_iota(jnp.int32, (BLOCK, BLOCK), 1)
    causal = tri_r >= tri_c
    lower = causal.astype(F32)
    run[...] = jnp.zeros_like(run)
    prefix[...] = jnp.zeros_like(prefix)

    @pl.loop(0, blocks)
    def _(b):
        at = pl.multiple_of(b * BLOCK, BLOCK)
        here = pl.ds(at, BLOCK)
        window = pj[pl.ds(at, BLOCK + 8), chans : span + 2 * NSTATE]
        conv = jnp.zeros((BLOCK, wide), F32) + conv_p[4:5, :]
        for k in range(WIDTH):
            conv = conv + conv_p[k : k + 1, :] * window[5 + k : 5 + k + BLOCK, :]
        raw[here, convs] = conv
        act = conv * logistic(conv)
        arg = pj[pl.ds(at + 8, BLOCK), span + 2 * NSTATE : pad] + head_p[0:1, :]
        step = jnp.maximum(arg, 0.0) + jnp.log1p(jnp.exp(-jnp.abs(arg)))
        cum = dotx(lower, step * head_p[1:2, :], 1, 0)
        last = cum[BLOCK - 1 : BLOCK, :]
        step_o[here, :] = step
        cum_o[here, :] = cum
        fed = act[:, :chans] * spread(step, expand)
        raw[here, scaled] = fed
        fresh = dot3x(
            fed * spread(jnp.exp(last - cum), expand), act[:, chans : chans + NSTATE], 0, 0
        )
        enter[b] = run[...]
        run[...] = row_scale(last, expand) * run[...] + fresh
        prefix[pl.ds(b + 1, 1), :] = prefix[pl.ds(b, 1), :] + last

        @pl.when(b == blocks // 2)
        def _():
            cotan.relay(2, 1)

    conv_put = pltpu.make_async_copy(
        raw.at[pl.ds(0, tokens), pl.ds(0, full_lanes(wide))], conv_hbm, put_sem.at[3 + 2 * heads]
    )
    conv_put.start()
    exch[seq, 0:chans, :] = run[...]
    exch[seq, chans : chans + 8, :] = jnp.broadcast_to(prefix[blocks : blocks + 1, :], (8, 128))

    def state_copy(at, j, to):
        return remote(exch.at[at], exch.at[at], s_send.at[j - 1], s_recv.at[j - 1], to, head)

    for j in range(1, seqs):

        @pl.when(seq + j < seqs)
        def _():
            state_copy(seq, j, seq + j).start()

    @pl.loop(0, blocks)
    def _(b):
        at = pl.multiple_of(b * BLOCK, BLOCK)
        here = pl.ds(at, BLOCK)
        bc = raw[here, chans:wide]
        bc = bc * logistic(bc)
        scores = dot3x(bc[:, NSTATE:], bc[:, :NSTATE], 1, 1)
        cum = cum_o[here, :]
        turned = cum.T
        for first_lane, end in lanes_of(chans):
            fed = halves(raw[here, scaled.start + first_lane : scaled.start + end])
            outs = [
                dot3(
                    halves(decay_of(cum, turned, lane // HEADDIM, causal) * scores), fed, 1, 0
                )
                for lane in range(first_lane, end, HEADDIM)
            ]
            out = outs[0]
            if len(outs) == 2:
                lane = lax.broadcasted_iota(jnp.int32, out.shape, 1)
                out = jnp.where(lane < HEADDIM, outs[0], outs[1])
            mixed_o[here, first_lane:end] = out

        @pl.when(b == 0)
        def _():
            cotan.relay(3, 0)

        @pl.when(b == blocks // 2)
        def _():
            cotan.relay(3, 1)

    run[...] = jnp.zeros_like(run)
    for earlier in range(seqs - 1):

        @pl.when(earlier < seq)
        def _():
            for j in range(1, seqs):

                @pl.when(seq - earlier == j)
                def _():
                    state_copy(earlier, j, lax.rem(seq + 1, seqs)).wait_recv()

            run[...] = (
                row_scale(exch[earlier, chans : chans + 1, :], expand) * run[...]
                + exch[earlier, 0:chans, :]
            )

    @pl.loop(0, blocks)
    def _(b):
        at = pl.multiple_of(b * BLOCK, BLOCK)
        here = pl.ds(at, BLOCK)
        state = enter[b] + row_scale(prefix[pl.ds(b, 1), :], expand) * run[...]
        state_o[b] = state
        conv = raw[here, convs]
        act = conv * logistic(conv)
        gate = pj[pl.ds(at + 8, BLOCK), 0:chans]
        carried = dot3x(act[:, chans + NSTATE :], state, 1, 1)
        mixed = (
            mixed_o[here, :]
            + carried * spread(jnp.exp(cum_o[here, :]), expand)
            + chan_p[1:2, :] * act[:, :chans]
        )
        mixed_o[here, :] = mixed
        raw[here, scaled] = mixed * gate * logistic(gate)

    ones = jnp.ones((8, chans), F32)
    groups = tokens // 128

    def statistics(n):
        here = pl.ds(pl.multiple_of(n * 128, 128), 128)
        gated = raw[here, scaled]
        lows[pl.ds(n, 1), :] = dotx(ones, gated * gated, 1, 1)[0:1, :]
        lows[pl.ds(groups + n, 1), :] = dotx(
            ones, cross_o[here, :] * chan_p[0:1, :] * gated, 1, 1
        )[0:1, :]

    def consume(where):
        here = chunk_rows(where)
        for put in chunk_puts(where, hat_hi, hat_lo):
            put.wait()
        top, low = halves(cot_parts[where])
        hi[where] = top
        lo[where] = low
        cross_o[here, :] = dot3((top, low), (owh[...], owl[...]), 1, 0)
        for put in chunk_puts(where, cot_hi, cot_lo):
            put.start()
        if chunk == 128:
            statistics(where)

    for distance in range(cotan.outs + 1):
        cotan.use(distance, consume)

    if chunk != 128:

        @pl.loop(0, groups)
        def _(n):
            statistics(n)

    stat_all[head] = lows[...]
    sends = []
    for j in range(1, heads):
        sends.append(
            remote(
                stat_all.at[head],
                stat_all.at[head],
                t_send.at[j - 1],
                t_recv.at[j - 1],
                seq,
                lax.rem(head + j, heads),
            )
        )
        sends[-1].start()
    gather.finish()
    cotan.finish()
    for put in puts + [pj_put, conv_put]:
        put.wait()

    @pl.loop(0, heads)
    def _(where):
        for put in chunk_puts(where, cot_hi, cot_lo):
            put.wait()

    for j in range(1, seqs):

        @pl.when(seq + j < seqs)
        def _():
            state_copy(seq, j, seq + j).wait_send()

    for j in range(1, heads):
        came = lax.rem(head - j + heads, heads)
        remote(
            stat_all.at[came], stat_all.at[came], t_send.at[j - 1], t_recv.at[j - 1], seq, came
        ).wait_recv()
    total = stat_all[0]
    for j in range(1, heads):
        total = total + stat_all[j]
    stat_o[...] = total
    for copy in sends:
        copy.wait_send()


def front(
    resid, cot, gain, gate_w, inner_w, bc_w, step_w, out_w, conv_p, head_p, chan_p,
    seqs, heads,
):
    chunk, width = resid.shape
    chans = gate_w.shape[0]
    pad = 2 * chans + 2 * NSTATE + 128
    ins = inner_count(heads)
    outs = heads // ins
    tokens = chunk * heads
    wide = chans + 2 * NSTATE
    blocks = tokens // BLOCK
    groups = 2 * tokens // 128
    anywhere = pl.BlockSpec(memory_space=pl.ANY)
    local = pl.BlockSpec(memory_space=pltpu.VMEM)
    sems = pltpu.SemaphoreType.DMA
    shape = jax.ShapeDtypeStruct
    return pl.pallas_call(
        functools.partial(front_kernel, (seqs, heads, chunk, chans, pad)),
        out_shape=(
            shape((tokens, width), BF16),
            shape((tokens, width), BF16),
            shape((8 + tokens, pad), F32),
            shape((pad, width), BF16),
            shape((pad, width), BF16),
            shape((tokens, width), BF16),
            shape((tokens, width), BF16),
            shape((tokens, full_lanes(wide)), F32),
            shape((tokens, 128), F32),
            shape((tokens, 128), F32),
            shape((blocks, chans, NSTATE), F32),
            shape((tokens, chans), F32),
            shape((tokens, chans), F32),
            shape((groups, 128), F32),
        ),
        in_specs=[local] * 3 + [anywhere] * 2 + [local] * 2 + [anywhere] + [local] * 3,
        out_specs=(anywhere,) * 8 + (local,) * 6,
        scratch_shapes=[
            pltpu.VMEM((heads, chunk, width), F32),
            pltpu.VMEM((heads, chunk, width), F32),
            pltpu.VMEM((heads, chunk, width), BF16),
            pltpu.VMEM((heads, chunk, width), BF16),
            pltpu.VMEM((8 + tokens, pad), F32),
            pltpu.VMEM((max(pad, tokens), width), F32),
            pltpu.VMEM((pad, width), BF16),
            pltpu.VMEM((pad, width), BF16),
            pltpu.VMEM((width, pad), BF16),
            pltpu.VMEM((width, pad), BF16),
            pltpu.VMEM((width, chans), BF16),
            pltpu.VMEM((width, chans), BF16),
            pltpu.VMEM((blocks, chans, NSTATE), F32),
            pltpu.VMEM((8, 128), F32),
            pltpu.VMEM((chans, NSTATE), F32),
            pltpu.VMEM((seqs, chans + 8, NSTATE), F32),
            pltpu.VMEM((heads, groups, 128), F32),
            pltpu.VMEM((groups, 128), F32),
            *line_gather_sems(ins, outs),
            *line_gather_sems(ins, outs),
            sems((2,)),
            sems((4 + 2 * heads,)),
            sems,
            sems,
            sems((seqs - 1,)),
            sems((seqs - 1,)),
            sems((heads - 1,)),
            sems((heads - 1,)),
        ],
        compiler_params=pltpu.CompilerParams(
            collective_id=2, has_side_effects=True, vmem_limit_bytes=VMEM_LIMIT
        ),
        name="front",
    )(resid, cot, gain, gate_w, inner_w, bc_w, step_w, out_w, conv_p, head_p, chan_p)


class LineReduce:
    def __init__(self, parts, y_in, z_in, sems, seq, head, heads, partner, depth):
        self.depth = depth
        self.parts, self.y_in, self.z_in = parts, y_in, z_in
        self.y_send, self.y_recv, self.z_send, self.z_recv = sems
        self.seq, self.partner = seq, partner
        self.ins = inner_count(heads)
        self.outs = heads // self.ins
        self.half = parts.shape[1] // 2
        self.turns = 2 * self.outs
        self.at_out, self.at_in = head // self.ins, lax.rem(head, self.ins)
        self.upper = self.at_out // (self.outs // 2)
        self.mirrored = self.at_out + self.upper * (self.outs - 1 - 2 * self.at_out)

    def target(self, step):
        last = (step + 1) // self.outs
        far = self.outs - 1 - step
        far = far - (self.mirrored - far + self.outs) // self.outs
        far = far + self.upper * (self.outs - 1 - 2 * far)
        return far + last * (self.at_out - far)

    def rows(self, turn):
        return pl.ds(pl.multiple_of(lax.rem(turn, 2) * self.half, 8), self.half)

    def y_copy(self, turn, j):
        goal = self.target(turn // 2)
        to = lax.rem(self.at_in + 1 + j, self.ins)
        rows = self.rows(turn)
        return remote(
            self.parts.at[goal * self.ins + to, rows],
            self.y_in.at[goal * (self.ins - 1) + j, rows],
            self.y_send.at[turn, j],
            self.y_recv.at[turn, j],
            self.seq,
            self.at_out * self.ins + to,
        )

    def give(self, turn):
        for j in range(self.ins - 1):
            self.y_copy(turn, j).start()

    def take(self, turn, slot):
        rows = self.rows(turn)
        where = self.target(turn // 2) * self.ins + self.at_in
        remote(
            self.parts.at[0, rows],
            self.z_in.at[slot, rows],
            self.z_send.at[0],
            self.z_recv.at[slot, lax.rem(turn, 2)],
            self.partner,
            self.at_out * self.ins + self.at_in,
        ).wait_recv()
        self.parts[where, rows, :] = self.parts[where, rows, :] + self.z_in[slot, rows, :]

    def pass_on(self, turn, up):
        goal, rows = self.target(turn // 2), self.rows(turn)
        remote(
            self.parts.at[goal * self.ins + self.at_in, rows],
            self.z_in.at[goal + up, rows],
            self.z_send.at[turn],
            self.z_recv.at[goal + up, lax.rem(turn, 2)],
            self.seq,
            (self.at_out + 2 * up - 1) * self.ins + self.at_in,
        ).start()

    def across(self, turn):
        goal = self.target(turn // 2)
        rows = self.rows(turn)
        where = goal * self.ins + self.at_in
        for j in range(self.ins - 1):
            self.y_copy(turn, j).wait_recv()

        @pl.when(turn + self.depth < self.turns)
        def _():
            self.give(turn + self.depth)

        for j in range(self.ins - 1):
            self.parts[where, rows, :] = (
                self.parts[where, rows, :] + self.y_in[goal * (self.ins - 1) + j, rows, :]
            )

        @pl.when((goal > self.at_out) & (self.at_out == 0))
        def _():
            self.pass_on(turn, 1)

        @pl.when((goal < self.at_out) & (self.at_out == self.outs - 1))
        def _():
            self.pass_on(turn, 0)

    def along(self, turn):
        goal = self.target(turn // 2)

        @pl.when((goal >= self.at_out) & (self.at_out > 0))
        def _():
            self.take(turn, goal + 1)

        @pl.when((goal <= self.at_out) & (self.at_out < self.outs - 1))
        def _():
            self.take(turn, goal)

        @pl.when((goal > self.at_out) & (self.at_out > 0))
        def _():
            self.pass_on(turn, 1)

        @pl.when((goal < self.at_out) & (self.at_out < self.outs - 1))
        def _():
            self.pass_on(turn, 0)

    def reduce(self, turn):
        turn = jnp.int32(turn)
        self.across(turn)

        @pl.when(turn > 0)
        def _():
            self.along(turn - 1)

    def last(self):
        self.along(jnp.int32(self.turns - 1))

    def finish(self):
        @pl.loop(0, self.turns)
        def _(turn):
            for j in range(self.ins - 1):
                self.y_copy(turn, j).wait_send()

        @pl.loop(0, self.turns - 2)
        def _(turn):
            rows = pl.ds(0, self.half)
            remote(
                self.parts.at[0, rows],
                self.z_in.at[0, rows],
                self.z_send.at[turn],
                self.z_recv.at[0, 0],
                self.partner,
                self.at_out * self.ins + self.at_in,
            ).wait_send()


def line_reduce_sems(ins, outs):
    sems = pltpu.SemaphoreType.DMA
    return [
        sems((2 * outs, ins - 1)),
        sems((2 * outs, ins - 1)),
        sems((2 * outs,)),
        sems((outs + 1, 2)),
    ]


def backward_kernel(dims, *refs):
    seqs, heads, chunk, chans, pad = dims
    (
        proj, cot_hi, cot_lo, hat_hi, hat_lo, conv_in, cum_in, step_in, state_in, mixed_in, cross_in,
        stat_in, out_w, resid, conv_p, head_p, chan_p, gain,
        result_o, gp_hi, gp_lo, out_o, gate_o, wide_o, chan_o, head_o,
        pj, ngh, ngl, owh, owl, gmix, fedg, adj, run, exch, gconv,
        parts, y_in, z_in, chi, clo, oparts, columns, conv_buf, head_acc,
        keep_o, core_o, x_o, o_sems, keep_g, core_g, g_sems, gate_sem,
        y_send, y_recv, z_send, z_recv, load_sem, s_send, s_recv, e_send, e_recv, conv_sem,
    ) = refs
    tokens = chunk * heads
    blocks = tokens // BLOCK
    span = 2 * chans
    wide = chans + 2 * NSTATE
    split_at = resid.shape[1] // 2
    seq, head = lax.axis_index("seq"), lax.axis_index("head")
    side = lax.rem(seq, 2)
    partner = seq + 1 - 2 * side
    loads = [
        pltpu.make_async_copy(a, b, load_sem.at[n])
        for n, (a, b) in enumerate(
            (
                (proj, pj),
                (cot_hi.at[:, pl.ds(0, split_at)], chi),
                (cot_lo.at[:, pl.ds(0, split_at)], clo),
                (out_w, oparts),
            )
        )
    ]
    for load in loads:
        load.start()
    greet(seq, head, seqs, heads)
    loads[3].wait()
    owh[...], owl[...] = halves(oparts[...])
    expand = head_lanes(chans)
    tri_r = lax.broadcasted_iota(jnp.int32, (BLOCK, BLOCK), 0)
    tri_c = lax.broadcasted_iota(jnp.int32, (BLOCK, BLOCK), 1)
    anticausal = tri_r <= tri_c
    upper = anticausal.astype(F32)
    wide_o[...] = jnp.zeros_like(wide_o)
    chan_o[...] = jnp.zeros_like(chan_o)
    head_acc[...] = jnp.zeros_like(head_acc)
    run[...] = jnp.zeros_like(run)
    loads[0].wait()
    groups = tokens // 128
    turned_stats = stat_in[...].T
    inner_total = float(heads * chans)
    gain_row, skip_row = chan_p[0:1, :], chan_p[1:2, :]
    for n in range(groups):
        here = slice(n * 128, n * 128 + 128)
        scale = lax.rsqrt(turned_stats[:, n : n + 1] / inner_total + EPSILON)
        cross = turned_stats[:, groups + n : groups + n + 1]
        columns[here, 0:1] = scale
        columns[here, 1:2] = scale * scale * scale * (cross / inner_total)

    def conv_load(b, slot):
        return pltpu.make_async_copy(
            conv_in.at[pl.ds(pl.multiple_of(b * BLOCK, BLOCK), BLOCK)],
            conv_buf.at[slot],
            conv_sem.at[slot],
        )

    def conv_of(n, b, following):
        slot = lax.rem(n, 2)
        conv_load(b, slot).wait()
        conv_load(following, 1 - slot).start()
        return conv_buf[slot, :, :wide]

    conv_load(blocks - 1, 0).start()

    @pl.loop(0, blocks)
    def _(b):
        at = pl.multiple_of(b * BLOCK, BLOCK)
        here = pl.ds(at, BLOCK)
        gate = pj[pl.ds(at + 8, BLOCK), 0:chans]
        ngh[here, :], ngl[here, :] = halves(
            mixed_in[here, :] * (gate * logistic(gate)) * columns[here, 0:1] * gain_row
        )

    reduce = LineReduce(
        parts, y_in, z_in, (y_send, y_recv, z_send, z_recv), seq, head, heads, partner, 3
    )

    ins = reduce.ins

    def produce(step):
        first = reduce.target(step) * ins
        rows = pl.ds(pl.multiple_of(first * chunk, 8), ins * chunk)
        out = dot3((ngh[rows, :], ngl[rows, :]), (owh[...], owl[...]), 1, 0)
        for n in range(ins):
            parts[first + n] = out[n * chunk : (n + 1) * chunk]

    @pl.loop(0, reduce.outs)
    def _(step):
        produce(step)

        @pl.when(step == 0)
        def _():
            reduce.give(jnp.int32(0))

    for load in loads[1:3]:
        load.wait()

    def weight_parts(left_hi, left_lo, hi, lo, then):
        for n in range(2):
            cols = pl.ds(n * split_at, split_at)
            oparts[:, n * split_at : (n + 1) * split_at] = dot3(
                (left_hi[...], left_lo[...]), (chi[...], clo[...]), 0, 0
            )
            source, cols = ((hi, lo), pl.ds(split_at, split_at)) if n == 0 else (then, None)
            if source is None:
                continue
            cols = pl.ds(split_at, split_at) if n == 0 else pl.ds(0, split_at)
            more = [
                pltpu.make_async_copy(a.at[:, cols], b, load_sem.at[1 + m])
                for m, (a, b) in enumerate(zip(source, (chi, clo)))
            ]
            for load in more:
                load.start()
            if n == 0:
                for load in more:
                    load.wait()
        return more

    reduce.give(jnp.int32(1))
    hat_load = weight_parts(ngh, ngl, cot_hi, cot_lo, (hat_hi, hat_lo))
    out_sum = SeqSum(oparts, 0, keep_o, core_o, x_o, o_sems, out_o, seq, head, seqs)
    out_sum.begin()
    reduce.give(jnp.int32(2))

    out_sum.pair()
    out_sum.start()

    def poll(n, base):
        @pl.when(lax.rem(n, pace) == pace - 1)
        def _():
            reduce.reduce(base + n // pace)

    pace = max(1, blocks // 2)

    @pl.loop(0, blocks)
    def _(back):
        b = blocks - 1 - back
        at = pl.multiple_of(b * BLOCK, BLOCK)
        here = pl.ds(at, BLOCK)
        scale = columns[here, 0:1]
        gate = pj[pl.ds(at + 8, BLOCK), 0:chans]
        sig = logistic(gate)
        gate_act = gate * sig
        mixed = mixed_in[here, :]
        gated = mixed * gate_act
        grad_ng = cross_in[here, :]
        grad_gated = scale * (grad_ng * gain_row) - gated * columns[here, 1:2]
        grad_mixed = grad_gated * gate_act
        gmix[here, :] = grad_mixed
        gp_hi[here, 0:chans], gp_lo[here, 0:chans] = halves(
            grad_gated * mixed * (sig * (1.0 + gate * (1.0 - sig)))
        )
        conv = conv_of(back, b, jnp.maximum(b - 1, 0))
        act = conv * logistic(conv)
        chan_o[0:1, :] = chan_o[0:1, :] + jnp.sum(grad_ng * (gated * scale), 0, keepdims=True)
        chan_o[1:2, :] = chan_o[1:2, :] + jnp.sum(grad_mixed * act[:, :chans], 0, keepdims=True)
        early = grad_mixed * spread(jnp.exp(cum_in[here, :]), expand)
        adj[b] = run[...]
        run[...] = row_scale(cum_in[pl.ds(at + BLOCK - 1, 1), :], expand) * run[...] + dot3x(
            early, act[:, chans + NSTATE :], 0, 0
        )
        gconv[here, chans + NSTATE :] = dot3x(early, state_in[b], 1, 0)
        poll(back, 0)

    total = jnp.zeros((1, 128), F32)
    for b in range(blocks):
        total = total + cum_in[(b + 1) * BLOCK - 1 : (b + 1) * BLOCK, :]
    exch[seq, 0:chans, :] = run[...]
    exch[seq, chans : chans + 8, :] = jnp.broadcast_to(total, (8, 128))

    def state_copy(at, j, to):
        return remote(exch.at[at], exch.at[at], s_send.at[j - 1], s_recv.at[j - 1], to, head)

    for j in range(1, seqs):

        @pl.when(seq - j >= 0)
        def _():
            state_copy(seq, j, seq - j).start()

    for load in hat_load:
        load.wait()
    weight_parts(gp_hi.at[:, 0:chans], gp_lo.at[:, 0:chans], hat_hi, hat_lo, None)
    oparts[...] = oparts[...] * gain[...]
    gate_sum = SeqSum(oparts, 0, keep_g, core_g, None, g_sems, None, seq, head, seqs)
    gate_sum.begin()
    gate_put = pltpu.make_async_copy(keep_g, gate_o, gate_sem)
    reduce.reduce(2)

    @pl.loop(0, blocks)
    def _(b):
        at = pl.multiple_of(b * BLOCK, BLOCK)
        here = pl.ds(at, BLOCK)
        conv = conv_of(b, b, lax.rem(b + 1, blocks))
        act = conv * logistic(conv)
        writes, reads = act[:, chans : chans + NSTATE], act[:, chans + NSTATE :]
        scores = dot3x(writes, reads, 1, 1)
        cum = cum_in[here, :]
        turned = cum.T
        fed_all = act[:, :chans] * spread(step_in[here, :], expand)
        grad_scores = jnp.zeros((BLOCK, BLOCK), F32)
        for first_lane, end in lanes_of(chans):
            fed = fed_all[:, first_lane:end]
            grad = gmix[here, first_lane:end]
            grad_parts, grad_turned = halves(grad), halves(grad.T)
            lane = lax.broadcasted_iota(jnp.int32, fed.shape, 1)
            outs = []
            for start in range(first_lane, end, HEADDIM):
                decay = decay_turned(cum, turned, start // HEADDIM, anticausal)
                inside = (lane // HEADDIM) == (start - first_lane) // HEADDIM
                grad_scores = grad_scores + decay * dot3(
                    halves(jnp.where(inside, fed, 0.0)), grad_turned, 1, 0
                )
                outs.append(dot3(halves(decay * scores), grad_parts, 1, 0))
            out = outs[0]
            if len(outs) == 2:
                out = jnp.where(lane < HEADDIM, outs[0], outs[1])
            fedg[here, first_lane:end] = out
        score_parts = halves(grad_scores)
        gconv[here, chans : chans + NSTATE] = dot3(score_parts, halves(reads), 1, 0)
        gconv[here, chans + NSTATE :] = gconv[here, chans + NSTATE :] + dot3(score_parts, halves(writes), 0, 0)
        poll(b, 3)

        @pl.when(b == 0)
        def _():
            gate_sum.pair()
            gate_put.start()


    run[...] = jnp.zeros_like(run)
    for back in range(seqs - 1):
        later = seqs - 1 - back

        @pl.when(later > seq)
        def _():
            for j in range(1, seqs):

                @pl.when(later - seq == j)
                def _():
                    state_copy(later, j, partner).wait_recv()

            run[...] = (
                row_scale(exch[later, chans : chans + 1, :], expand) * run[...]
                + exch[later, 0:chans, :]
            )

    for b in range(blocks - 1, -1, -1):
        adj[b] = adj[b] + run[...]
        run[...] = row_scale(cum_in[(b + 1) * BLOCK - 1 : (b + 1) * BLOCK, :], expand) * run[...]

    lane_ones = jnp.ones((8, NSTATE), F32)

    @pl.loop(0, blocks)
    def _(b):
        at = pl.multiple_of(b * BLOCK, BLOCK)
        here = pl.ds(at, BLOCK)
        conv = conv_of(b, b, lax.rem(b + 1, blocks))
        sig = logistic(conv)
        act = conv * sig
        slope = sig * (1.0 + conv * (1.0 - sig))
        inner, writes = act[:, :chans], act[:, chans : chans + NSTATE]
        cum = cum_in[here, :]
        step = step_in[here, :]
        last = cum[BLOCK - 1 : BLOCK, :]
        step_wide = spread(step, expand)
        tails = spread(jnp.exp(last - cum), expand)
        fed = inner * step_wide
        grad_state = adj[b]
        state_parts = halves(grad_state)
        from_state = tails * dot3(halves(writes), state_parts, 1, 1)
        grad_fed = fedg[here, :] + from_state
        grad_mixed = gmix[here, :]
        grad_writes = gconv[here, chans : chans + NSTATE] + dot3(halves(fed * tails), state_parts, 1, 0)
        direct = gather_heads(inner * grad_fed, expand)
        scanned = mixed_in[here, :] - skip_row * inner
        grad_cum = dotx(grad_mixed * scanned - fed * grad_fed, expand, 1, 1)
        kept = dotx(expand, grad_state * state_in[b], 1, 0)
        kept = dotx(lane_ones, kept, 1, 1)[0:1, :] * jnp.exp(last)
        grad_last = kept + jnp.sum(gather_heads(fed * from_state, expand), 0, keepdims=True)
        grad_log = dotx(upper, grad_cum, 1, 0) + grad_last
        rate = head_p[1:2, :]
        head_acc[1:2, :] = head_acc[1:2, :] + jnp.sum(step * grad_log, 0, keepdims=True) * rate
        arg = pj[pl.ds(at + 8, BLOCK), span + 2 * NSTATE : pad] + head_p[0:1, :]
        grad_arg = (direct + rate * grad_log) * logistic(arg) * head_p[2:3, :]
        head_acc[0:1, :] = head_acc[0:1, :] + jnp.sum(grad_arg, 0, keepdims=True)
        gp_hi[here, span + 2 * NSTATE : pad], gp_lo[here, span + 2 * NSTATE : pad] = halves(
            grad_arg
        )
        gconv[here, 0:chans] = (step_wide * grad_fed + skip_row * grad_mixed) * slope[:, :chans]
        gconv[here, chans : chans + NSTATE] = grad_writes * slope[:, chans : chans + NSTATE]
        gconv[here, chans + NSTATE :] = gconv[here, chans + NSTATE :] * slope[:, chans + NSTATE :]

        @pl.when(b == blocks // 2 - 1)
        def _():
            reduce.reduce(5)

    out_sum.total()
    edge = remote(
        gconv.at[pl.ds(0, 8)],
        gconv.at[pl.ds(tokens, 8)],
        e_send,
        e_recv,
        lax.rem(seq + seqs - 1, seqs),
        head,
    )
    edge.start()
    head_o[...] = head_acc[...]

    def conv_back(b):
        at = pl.multiple_of(b * BLOCK, BLOCK)
        here = pl.ds(at, BLOCK)
        before = pj[pl.ds(at + 8, BLOCK), chans : span + 2 * NSTATE]
        ahead = gconv[pl.ds(at, BLOCK + 8), :]
        grad = ahead[0:BLOCK, :]
        grad_pre = jnp.zeros((BLOCK, wide), F32)
        for k in range(WIDTH):
            later = ahead[3 - k : 3 - k + BLOCK, :]
            grad_pre = grad_pre + conv_p[k : k + 1, :] * later
            wide_o[k : k + 1, :] = wide_o[k : k + 1, :] + jnp.sum(
                later * before, 0, keepdims=True
            )
        wide_o[4:5, :] = wide_o[4:5, :] + jnp.sum(grad, 0, keepdims=True)
        (
            gp_hi[here, chans : span + 2 * NSTATE],
            gp_lo[here, chans : span + 2 * NSTATE],
        ) = halves(grad_pre)

    @pl.loop(0, blocks - 1)
    def _(b):
        conv_back(b)

    reduce.reduce(6)
    edge.wait()
    gconv[tokens : tokens + 8, :] = jnp.where(seq < seqs - 1, gconv[tokens : tokens + 8, :], 0.0)

    @pl.loop(blocks - 1, blocks)
    def _(b):
        conv_back(b)

    reduce.reduce(7)
    reduce.last()
    result_o[...] = resid[...] + parts[head]
    conv_load(0, 0).wait()
    reduce.finish()
    for j in range(1, seqs):

        @pl.when(seq - j >= 0)
        def _():
            state_copy(seq, j, seq - j).wait_send()

    out_sum.end()
    gate_put.wait()


def backward(proj, hat, kept, out_w, resid, conv_p, head_p, chan_p, gain, seqs, heads):
    (cot_hi, cot_lo, conv, cum, step, state, mixed, cross, stat) = kept
    tokens, pad = cum.shape[0], proj.shape[1]
    chunk, width = resid.shape
    chans = out_w.shape[0]
    ins = inner_count(heads)
    outs = heads // ins
    wide = chans + 2 * NSTATE
    blocks = tokens // BLOCK
    half = chans // 2
    rounds = (seqs // 2).bit_length() - 1
    anywhere = pl.BlockSpec(memory_space=pl.ANY)
    local = pl.BlockSpec(memory_space=pltpu.VMEM)
    sems = pltpu.SemaphoreType.DMA
    shape = jax.ShapeDtypeStruct
    return pl.pallas_call(
        functools.partial(backward_kernel, (seqs, heads, chunk, chans, pad)),
        out_shape=(
            shape((chunk, width), F32),
            shape((tokens, pad), BF16),
            shape((tokens, pad), BF16),
            shape((chans, width), F32),
            shape((half, width), F32),
            shape((8, wide), F32),
            shape((8, chans), F32),
            shape((8, 128), F32),
        ),
        in_specs=[anywhere] * 6 + [local] * 6 + [anywhere] + [local] * 5,
        out_specs=(local, local, local, anywhere, anywhere, local, local, local),
        scratch_shapes=[
            pltpu.VMEM((8 + tokens, pad), F32),
            pltpu.VMEM((tokens, chans), BF16),
            pltpu.VMEM((tokens, chans), BF16),
            pltpu.VMEM((chans, width), BF16),
            pltpu.VMEM((chans, width), BF16),
            pltpu.VMEM((tokens, chans), F32),
            pltpu.VMEM((tokens, chans), F32),
            pltpu.VMEM((blocks, chans, NSTATE), F32),
            pltpu.VMEM((chans, NSTATE), F32),
            pltpu.VMEM((seqs, chans + 8, NSTATE), F32),
            pltpu.VMEM((tokens + 8, wide), F32),
            pltpu.VMEM((heads, chunk, width), F32),
            pltpu.VMEM((outs * (ins - 1), chunk, width), F32),
            pltpu.VMEM((outs + 1, chunk, width), F32),
            pltpu.VMEM((tokens, width // 2), BF16),
            pltpu.VMEM((tokens, width // 2), BF16),
            pltpu.VMEM((chans, width), F32),
            pltpu.VMEM((tokens, 128), F32),
            pltpu.VMEM((2, BLOCK, full_lanes(wide)), F32),
            pltpu.VMEM((8, 128), F32),
            *seq_sum_scratch(half, width, rounds),
            pltpu.VMEM((half, width), F32),
            pltpu.VMEM((half, width), F32),
            sems((2,)),
            sems,
            *line_reduce_sems(ins, outs),
            sems((4,)),
            sems((seqs - 1,)),
            sems((seqs - 1,)),
            sems,
            sems,
            sems((2,)),
        ],
        compiler_params=pltpu.CompilerParams(
            collective_id=4, has_side_effects=True, vmem_limit_bytes=VMEM_LIMIT
        ),
        name="backward",
    )(
        proj, cot_hi, cot_lo, *hat, conv, cum, step, state, mixed, cross, stat,
        out_w, resid, conv_p, head_p, chan_p, gain,
    )


def on_device(
    residual_in,
    norm_gain,
    gate_weight,
    inner_weight,
    bc_weight,
    step_weight,
    conv_inner_weight,
    conv_inner_bias,
    conv_bc_weight,
    conv_bc_bias,
    step_bias,
    decay_log,
    skip_gain,
    gated_gain,
    out_weight,
    cotangent,
):
    seqs, heads = lax.axis_size("seq"), lax.axis_size("head")
    width = residual_in.shape[2]
    chans = gate_weight.shape[0]
    heads_here = step_weight.shape[0]
    spare = 128 - heads_here
    resid = residual_in.reshape(-1, width)
    cot = cotangent.reshape(-1, width)
    gain = norm_gain.reshape(1, width)

    def eight(part):
        return jnp.pad(part, ((0, 8 - part.shape[0]), (0, 0)))

    def by_head(*parts):
        return eight(jnp.pad(jnp.stack(parts), ((0, 0), (0, spare))))

    conv_p = eight(
        jnp.concatenate(
            [
                jnp.concatenate([conv_inner_weight, conv_bc_weight], 1),
                jnp.concatenate([conv_inner_bias, conv_bc_bias])[None],
            ],
            0,
        )
    )
    head_p = by_head(step_bias, -jnp.exp(decay_log), jnp.ones_like(step_bias))
    chan_p = eight(jnp.stack([gated_gain, jnp.repeat(skip_gain, HEADDIM)]))
    hat_hi, hat_lo, projected, weight_hi, weight_lo, *kept = front(
        resid,
        cot,
        gain,
        gate_weight,
        inner_weight,
        bc_weight,
        step_weight,
        out_weight,
        conv_p,
        head_p,
        chan_p,
        seqs,
        heads,
    )
    (
        result,
        grad_hi,
        grad_lo,
        out_weight_grad,
        gate_half,
        wide_sums,
        chan_sums,
        head_sums,
    ) = backward(
        projected,
        (hat_hi, hat_lo),
        kept,
        out_weight,
        resid,
        conv_p,
        head_p,
        chan_p,
        gain,
        seqs,
        heads,
    )

    residual_grad, gate_weight_grad, inner_weight_grad, bc_pieces, sums, glob = tail(
        (grad_hi, grad_lo),
        (hat_hi, hat_lo),
        (weight_hi, weight_lo),
        gate_half,
        (wide_sums, chan_sums, head_sums),
        resid,
        cot,
        gain,
        seqs,
        heads,
        chans,
    )
    across = width // bc_pieces.shape[2]
    bc_weight_grad = jnp.transpose(
        bc_pieces.reshape(2 * NSTATE // 8, across, 8, width // across), (1, 3, 0, 2)
    ).reshape(width, 2 * NSTATE)
    chan_at = full_lanes(chans + 2 * NSTATE)
    head_at = chan_at + full_lanes(chans)
    skip_wide = sums[1, 1, chan_at : chan_at + chans]
    return (
        result.reshape(residual_in.shape),
        residual_grad.reshape(residual_in.shape),
        glob[:4].reshape(width),
        gate_weight_grad,
        inner_weight_grad,
        bc_weight_grad,
        sums[0, :heads_here],
        sums[1, :WIDTH, :chans],
        sums[1, WIDTH, :chans],
        glob[8 : 8 + WIDTH, : 2 * NSTATE],
        glob[8 + WIDTH, : 2 * NSTATE],
        sums[1, 0, head_at : head_at + heads_here],
        sums[1, 1, head_at : head_at + heads_here],
        jnp.sum(skip_wide.reshape(heads_here, HEADDIM), axis=1),
        sums[1, 0, chan_at : chan_at + chans],
        out_weight_grad,
    )


def solution(mesh):
    placed = (
        P(None, ("seq", "head"), None),
        P(),
        P("head", None),
        P("head", None),
        P(),
        P("head", None),
        P(None, "head"),
        P("head"),
        P(),
        P(),
        P("head"),
        P("head"),
        P("head"),
        P("head"),
        P("head", None),
        P(None, ("seq", "head"), None),
    )
    return jax.shard_map(
        on_device,
        mesh=mesh,
        in_specs=placed,
        out_specs=(
            P(None, ("seq", "head"), None),
            P(None, ("seq", "head"), None),
            P(),
            P("head", None),
            P("head", None),
            P(),
            P("head", None),
            P(None, "head"),
            P("head"),
            P(),
            P(),
            P("head"),
            P("head"),
            P("head"),
            P("head"),
            P("head", None),
        ),
        check_vma=False,
    )
```

```python
import functools

import jax
import jax.numpy as jnp
from jax import lax
from jax.experimental import pallas as pl
from jax.experimental.pallas import tpu as pltpu
from jax.sharding import PartitionSpec as P

HEADDIM = 64
NSTATE = 128
WIDTH = 4
BLOCK = 256
EPSILON = 1e-05
EXACT = lax.Precision.HIGHEST
MESH = pl.DeviceIdType.MESH
F32 = jnp.float32
BF16 = jnp.bfloat16
VMEM_LIMIT = 66000000


def dot3(left, right, left_dim, right_dim):
    dims = (((left_dim,), (right_dim,)), ((), ()))
    one = functools.partial(lax.dot_general, dimension_numbers=dims, preferred_element_type=F32)
    return one(left[0], right[0]) + (one(left[0], right[1]) + one(left[1], right[0]))


def remote(source, target, send_sem, recv_sem, seq, head):
    return pltpu.make_async_remote_copy(
        src_ref=source,
        dst_ref=target,
        send_sem=send_sem,
        recv_sem=recv_sem,
        device_id=(seq, head),
        device_id_type=MESH,
    )


def greet(seq, head, seqs, heads):
    barrier = pltpu.get_barrier_semaphore()
    for j in range(1, seqs):
        pl.semaphore_signal(
            barrier, inc=1, device_id=(lax.rem(seq + j, seqs), head), device_id_type=MESH
        )
    for j in range(1, heads):
        pl.semaphore_signal(
            barrier, inc=1, device_id=(seq, lax.rem(head + j, heads)), device_id_type=MESH
        )
    pl.semaphore_wait(barrier, seqs + heads - 2)


def inner_count(heads):
    return 2 if heads <= 8 else 4


class SeqSum:
    def __init__(self, source, base, keep, core_in, x_in, sems, result, seq, head, seqs):
        self.source, self.base, self.keep, self.core_in, self.x_in = source, base, keep, core_in, x_in
        self.sems, self.result, self.seq, self.head = sems, result, seq, head
        self.rounds = (seqs // 2).bit_length() - 1
        self.half = keep.shape[0]
        self.side = lax.rem(seq, 2)
        self.partner = seq + 1 - 2 * self.side

    def rows(self, side, base):
        return pl.ds(pl.multiple_of(base + side * self.half, 8), self.half)

    def begin(self):
        self.keep[...] = self.source[self.rows(self.side, self.base), :]
        self.core = remote(
            self.source.at[self.rows(1 - self.side, self.base)],
            self.core_in,
            self.sems.at[0],
            self.sems.at[1],
            self.partner,
            self.head,
        )
        self.core.start()

    def cross(self, source, turn):
        away = 2 << turn
        far = self.seq + away - 2 * away * lax.rem(self.seq // away, 2)
        return remote(
            source,
            self.x_in.at[turn],
            self.sems.at[5 + 2 * turn],
            self.sems.at[6 + 2 * turn],
            far,
            self.head,
        )

    def pair(self):
        self.core.wait()
        self.keep[...] = self.keep[...] + self.core_in[...]

    def start(self):
        self.cross(self.keep, 0).start()

    def total(self):
        now, new = self.keep, self.core_in
        for turn in range(self.rounds):
            self.cross(now, turn).wait()
            new[...] = now[...] + self.x_in[turn]
            now, new = new, now
            if turn + 1 < self.rounds:
                self.cross(now, turn + 1).start()
        mine = self.result.at[self.rows(self.side, 0)]
        self.now = now
        self.put = pltpu.make_async_copy(now, mine, self.sems.at[2])
        self.put.start()
        self.final = remote(
            now, mine, self.sems.at[3], self.sems.at[4], self.partner, self.head
        )
        self.final.start()

    def end(self):
        self.final.wait_send()
        remote(
            self.now,
            self.result.at[self.rows(1 - self.side, 0)],
            self.sems.at[3],
            self.sems.at[4],
            self.partner,
            self.head,
        ).wait_recv()
        self.put.wait()


def seq_sum_scratch(half, width, rounds):
    return [
        pltpu.VMEM((half, width), F32),
        pltpu.VMEM((half, width), F32),
        pltpu.VMEM((rounds, half, width), F32),
        pltpu.SemaphoreType.DMA((5 + 2 * rounds,)),
    ]


def tail_kernel(dims, *refs):
    seqs, heads, chunk, chans, pad = dims
    (
        gp_hi, gp_lo, hat_hi, hat_lo, w_hi, w_lo, gate_half, wide_in, chan_in, head_in, resid, cot, gain,
        resid_grad, gate_out, inner_out, bc_out, small_out, glob_out,
        gph, gpl, hth, htl, wh, wl, parts, y_in, z_in, joined, keep, core_in, x_in, i_sems, keep_g, core_g, x_g, g_sems,
        bc_part, bc_half, bc_seq, bc_quart, bc_head, bc_full,
        small_mine, small_pair, small_far, glob_mine, glob_pair, glob_far, small_head, gain_sum,
        load_sem, y_send, y_recv, z_send, z_recv,
        a_sem, b_send, b_recv, c_send, c_recv, m_sem, h_send, h_recv, put_sem,
    ) = refs
    width = gain.shape[1]
    span = 2 * chans
    fars = seqs // 2
    seq, head = lax.axis_index("seq"), lax.axis_index("head")
    side, far = lax.rem(seq, 2), seq // 2
    partner = seq + 1 - 2 * side
    loads = [
        pltpu.make_async_copy(a, b, load_sem.at[n])
        for n, (a, b) in enumerate(
            ((gp_hi, gph), (w_hi, wh), (gp_lo, gpl), (w_lo, wl), (hat_hi, hth), (hat_lo, htl))
        )
    ]
    for load in loads:
        load.start()
    gate_load = pltpu.make_async_copy(gate_half, keep_g, load_sem.at[6])
    gate_load.start()
    greet(seq, head, seqs, heads)
    reduce = LineReduce(
        parts, y_in, z_in, (y_send, y_recv, z_send, z_recv), seq, head, heads, partner, 2
    )
    gate_load.wait()
    gate = SeqSum(None, 0, keep_g, core_g, x_g, g_sems, gate_out, seq, head, seqs)
    gate.start()
    for load in loads[:4]:
        load.wait()

    def chunk_rows(where):
        return pl.ds(pl.multiple_of(where * chunk, 8), chunk)

    ins = reduce.ins

    def produce(step):
        first = reduce.target(step) * ins
        rows = pl.ds(pl.multiple_of(first * chunk, 8), ins * chunk)
        out = dot3((gph[rows, :], gpl[rows, :]), (wh[...], wl[...]), 1, 0)
        for n in range(ins):
            parts[first + n] = out[n * chunk : (n + 1) * chunk]

    produce(jnp.int32(0))
    reduce.give(jnp.int32(0))
    gain_row = gain[...]
    for load in loads[4:]:
        load.wait()

    small_mine[...] = jnp.zeros_like(small_mine)
    offset = 0
    for block in (wide_in, chan_in, head_in):
        small_mine[1, :, offset : offset + block.shape[1]] = block[...]
        offset += full_lanes(block.shape[1])
    gain_sum[...] = jnp.zeros_like(gain_sum)

    def gain_part(step):
        first = reduce.target(step) * ins
        rows = pl.ds(pl.multiple_of(first * chunk, 8), ins * chunk)
        hat = hth[rows, :].astype(F32) + htl[rows, :].astype(F32)
        for n in range(ins):
            gain_sum[...] = gain_sum[...] + jnp.sum(
                parts[first + n] * hat[n * chunk : (n + 1) * chunk], 0, keepdims=True
            )

    gain_part(jnp.int32(0))

    joined[span:, :] = (
        dot3((gph[:, span:], gpl[:, span:]), (hth[...], htl[...]), 0, 0) * gain_row
    )
    pieces, _, lanes = bc_part.shape
    across = width // lanes
    for row in range(pieces // across):
        for col in range(across):
            bc_part[row * across + col] = joined[
                span + row * 8 : span + row * 8 + 8, col * lanes : (col + 1) * lanes
            ]
    mine = pl.ds(side * (pieces // 2), pieces // 2)
    theirs = pl.ds((1 - side) * (pieces // 2), pieces // 2)
    bc_core = remote(
        bc_part.at[theirs], bc_half, a_sem.at[0], a_sem.at[1], partner, head
    )
    bc_core.start()
    reduce.give(jnp.int32(1))

    @pl.loop(1, reduce.outs)
    def _(step):
        produce(step)
        gain_part(step)

    def others(make):
        copies = []
        for j in range(1, fars):
            copies.append(make(j, lax.rem(far + j, fars)))
            copies[-1].start()
        return copies

    bc_core.wait()
    bc_half[...] = bc_half[...] + bc_part[mine]
    cross_bc = others(
        lambda j, to: remote(
            bc_half.at[pl.ds(to * heads, heads)],
            bc_seq.at[j - 1],
            b_send.at[0, j - 1],
            b_recv.at[0, j - 1],
            2 * to + side,
            head,
        )
    )
    reduce.reduce(0)
    low = chans if chans % 128 == 0 else 0
    rows = dot3((gph[:, low:span], gpl[:, low:span]), (hth[...], htl[...]), 0, 0)
    joined[low:span, :] = rows * gain_row
    inner = SeqSum(
        joined, chans, keep, core_in, x_in, i_sems, inner_out, seq, head, seqs
    )
    inner.begin()
    small_mine[0] = joined[span + 2 * NSTATE : span + 2 * NSTATE + 8, :]
    glob_mine[...] = jnp.zeros_like(glob_mine)
    quarter = glob_mine.shape[1]
    for n in range(width // quarter):
        glob_mine[n : n + 1, :] = gain_sum[:, n * quarter : (n + 1) * quarter]
    glob_mine[8:16, 0 : 2 * NSTATE] = wide_in[:, chans:]
    reduce.reduce(1)
    for copy in cross_bc:
        copy.wait()
    quarter = bc_half[pl.ds(far * heads, heads)]
    for j in range(fars - 1):
        quarter = quarter + bc_seq[j]
    bc_quart[...] = quarter

    def to_heads(make):
        copies = []
        for j in range(1, heads):
            copies.append(make(j, lax.rem(head + j, heads)))
            copies[-1].start()
        return copies

    spread_bc = to_heads(
        lambda j, to: remote(
            bc_quart.at[to], bc_head.at[j - 1], c_send.at[0, j - 1], c_recv.at[0, j - 1], seq, to
        )
    )
    inner.pair()
    inner.start()
    small_core = [
        remote(small_mine, small_pair, a_sem.at[2], a_sem.at[3], partner, head),
        remote(glob_mine, glob_pair, a_sem.at[6], a_sem.at[7], partner, head),
    ]
    for copy in small_core:
        copy.start()
    reduce.reduce(2)
    for copy in small_core:
        copy.wait()
    small_far[far] = small_mine[...] + small_pair[...]
    glob_far[far] = glob_mine[...] + glob_pair[...]
    cross_small = others(
        lambda j, to: remote(
            small_far.at[far],
            small_far.at[far],
            m_sem.at[0, j - 1],
            m_sem.at[1, j - 1],
            2 * to + side,
            head,
        )
    ) + others(
        lambda j, to: remote(
            glob_far.at[far],
            glob_far.at[far],
            m_sem.at[2, j - 1],
            m_sem.at[3, j - 1],
            2 * to + side,
            head,
        )
    )
    reduce.reduce(3)
    for copy in spread_bc:
        copy.wait()
    piece = bc_quart[head]
    for j in range(heads - 1):
        piece = piece + bc_head[j]
    block = side * (pieces // 2) + far * heads
    bc_full[block + head] = piece
    gather_bc = to_heads(
        lambda j, to: remote(
            bc_full.at[block + head],
            bc_full.at[block + head],
            c_send.at[1, j - 1],
            c_recv.at[1, j - 1],
            seq,
            to,
        )
    )
    for j in range(1, fars):
        came = lax.rem(far - j + fars, fars)
        remote(
            small_far.at[came], small_far.at[came], m_sem.at[0, j - 1], m_sem.at[1, j - 1],
            partner, head,
        ).wait_recv()
        remote(
            glob_far.at[came], glob_far.at[came], m_sem.at[2, j - 1], m_sem.at[3, j - 1],
            partner, head,
        ).wait_recv()
    total, glob = small_far[0], glob_far[0]
    for j in range(1, fars):
        total = total + small_far[j]
        glob = glob + glob_far[j]
    small_out[...] = total
    small_head[head] = glob
    spread_small = to_heads(
        lambda j, to: remote(
            small_head.at[head], small_head.at[head], h_send.at[j - 1], h_recv.at[j - 1], seq, to
        )
    )
    reduce.reduce(4)
    reduce.reduce(5)
    for j in range(1, heads):
        came = lax.rem(head - j + heads, heads)
        remote(
            bc_full.at[block + came], bc_full.at[block + came],
            c_send.at[1, j - 1], c_recv.at[1, j - 1], partner, head,
        ).wait_recv()
    own_block = pl.ds(block, heads)
    join_bc = others(
        lambda j, to: remote(
            bc_full.at[own_block],
            bc_full.at[own_block],
            b_send.at[1, j - 1],
            b_recv.at[1, j - 1],
            2 * to + side,
            head,
        )
    )
    for j in range(1, heads):
        came = lax.rem(head - j + heads, heads)
        remote(
            small_head.at[came], small_head.at[came], h_send.at[j - 1], h_recv.at[j - 1], seq, came
        ).wait_recv()
    total = small_head[0]
    for j in range(1, heads):
        total = total + small_head[j]
    glob_out[...] = total
    reduce.reduce(6)
    for j in range(1, fars):
        came = side * (pieces // 2) + lax.rem(far - j + fars, fars) * heads
        came = pl.ds(came, heads)
        remote(
            bc_full.at[came], bc_full.at[came], b_send.at[1, j - 1], b_recv.at[1, j - 1],
            partner, head,
        ).wait_recv()
    join_core = remote(
        bc_full.at[mine], bc_full.at[mine], a_sem.at[4], a_sem.at[5], partner, head
    )
    join_core.start()
    gate.total()
    inner.total()
    reduce.reduce(7)
    reduce.last()
    grad_hat = parts[head] * gain_row
    values = resid[...]
    scale = lax.rsqrt(jnp.mean(values * values, axis=1, keepdims=True) + EPSILON)
    row_cross = jnp.sum(grad_hat * values, axis=1, keepdims=True)
    resid_grad[...] = (
        cot[...] + scale * grad_hat - values * (scale * scale * scale * (row_cross / width))
    )
    remote(
        bc_full.at[theirs], bc_full.at[theirs], a_sem.at[4], a_sem.at[5], partner, head
    ).wait_recv()
    bc_put = pltpu.make_async_copy(bc_full, bc_out, put_sem)
    bc_put.start()
    reduce.finish()
    for copy in gather_bc + cross_small + spread_small + join_bc + [join_core]:
        copy.wait_send()
    gate.end()
    inner.end()
    bc_put.wait()


def tail(gp, hat, weight, gate_half, sums, resid, cot, gain, seqs, heads, chans):
    tokens, width = hat[0].shape
    chunk = tokens // heads
    pad = gp[0].shape[1]
    ins = inner_count(heads)
    outs = heads // ins
    rounds = (seqs // 2).bit_length() - 1
    fars = seqs // 2
    lanes = 2 * NSTATE * width // (8 * seqs * heads)
    pieces = seqs * heads
    anywhere = pl.BlockSpec(memory_space=pl.ANY)
    local = pl.BlockSpec(memory_space=pltpu.VMEM)
    sems = pltpu.SemaphoreType.DMA
    return pl.pallas_call(
        functools.partial(tail_kernel, (seqs, heads, chunk, chans, pad)),
        out_shape=(
            jax.ShapeDtypeStruct((chunk, width), F32),
            jax.ShapeDtypeStruct((chans, width), F32),
            jax.ShapeDtypeStruct((chans, width), F32),
            jax.ShapeDtypeStruct((pieces, 8, lanes), F32),
            jax.ShapeDtypeStruct((2, 8, width), F32),
            jax.ShapeDtypeStruct((16, width // 4), F32),
        ),
        in_specs=[anywhere] * 7 + [local] * 6,
        out_specs=(local, anywhere, anywhere, anywhere, local, local),
        scratch_shapes=[
            pltpu.VMEM((tokens, pad), BF16),
            pltpu.VMEM((tokens, pad), BF16),
            pltpu.VMEM((tokens, width), BF16),
            pltpu.VMEM((tokens, width), BF16),
            pltpu.VMEM((pad, width), BF16),
            pltpu.VMEM((pad, width), BF16),
            pltpu.VMEM((heads, chunk, width), F32),
            pltpu.VMEM((outs * (ins - 1), chunk, width), F32),
            pltpu.VMEM((outs + 1, chunk, width), F32),
            pltpu.VMEM((pad, width), F32),
            *seq_sum_scratch(chans // 2, width, rounds),
            *seq_sum_scratch(chans // 2, width, rounds),
            pltpu.VMEM((pieces, 8, lanes), F32),
            pltpu.VMEM((pieces // 2, 8, lanes), F32),
            pltpu.VMEM((fars - 1, heads, 8, lanes), F32),
            pltpu.VMEM((heads, 8, lanes), F32),
            pltpu.VMEM((heads - 1, 8, lanes), F32),
            pltpu.VMEM((pieces, 8, lanes), F32),
            pltpu.VMEM((2, 8, width), F32),
            pltpu.VMEM((2, 8, width), F32),
            pltpu.VMEM((fars, 2, 8, width), F32),
            pltpu.VMEM((16, width // 4), F32),
            pltpu.VMEM((16, width // 4), F32),
            pltpu.VMEM((fars, 16, width // 4), F32),
            pltpu.VMEM((heads, 16, width // 4), F32),
            pltpu.VMEM((1, width), F32),
            sems((7,)),
            *line_reduce_sems(ins, outs),
            sems((8,)),
            sems((2, fars - 1)),
            sems((2, fars - 1)),
            sems((2, heads - 1)),
            sems((2, heads - 1)),
            sems((4, fars - 1)),
            sems((heads - 1,)),
            sems((heads - 1,)),
            sems,
        ],
        compiler_params=pltpu.CompilerParams(
            collective_id=1, has_side_effects=True, vmem_limit_bytes=VMEM_LIMIT
        ),
        name="tail",
    )(*gp, *hat, *weight, gate_half, *sums, resid, cot, gain)


def dotx(left, right, left_dim, right_dim):
    return lax.dot_general(
        left,
        right,
        (((left_dim,), (right_dim,)), ((), ())),
        precision=EXACT,
        preferred_element_type=F32,
    )


def dot3x(left, right, left_dim, right_dim):
    return dot3(halves(left), halves(right), left_dim, right_dim)


def halves(values):
    top = values.astype(BF16)
    return (top, (values - top.astype(F32)).astype(BF16))


def head_lanes(chans):
    row = lax.broadcasted_iota(jnp.int32, (128, chans), 0)
    col = lax.broadcasted_iota(jnp.int32, (128, chans), 1)
    return (row == col // HEADDIM).astype(F32)


def lanes_of(chans):
    return [(lo, min(lo + 2 * HEADDIM, chans)) for lo in range(0, chans, 2 * HEADDIM)]


def spread(values, expand):
    top, low = halves(values)
    expand = expand.astype(BF16)
    dims = (((1,), (0,)), ((), ()))
    one = functools.partial(lax.dot_general, dimension_numbers=dims, preferred_element_type=F32)
    return one(top, expand) + one(low, expand)


def gather_heads(values, expand):
    top, low = halves(values)
    expand = expand.astype(BF16)
    dims = (((1,), (1,)), ((), ()))
    one = functools.partial(lax.dot_general, dimension_numbers=dims, preferred_element_type=F32)
    return one(top, expand) + one(low, expand)


def row_scale(total_row, expand):
    top, low = halves(jnp.broadcast_to(jnp.exp(total_row), (128, 128)).T)
    expand = expand.astype(BF16)
    dims = (((0,), (0,)), ((), ()))
    one = functools.partial(lax.dot_general, dimension_numbers=dims, preferred_element_type=F32)
    return one(expand, top) + one(expand, low)


def logistic(values):
    return 1.0 / (1.0 + jnp.exp(-values))


def decay_of(cum, cum_turned, h, causal):
    return jnp.where(causal, jnp.exp(cum[:, h : h + 1] - cum_turned[h : h + 1, :]), 0.0)


def decay_turned(cum, cum_turned, h, anticausal):
    return jnp.where(anticausal, jnp.exp(cum_turned[h : h + 1, :] - cum[:, h : h + 1]), 0.0)


class LineGather:
    def __init__(self, parts, sems, seq, head, heads):
        self.parts, self.seq = parts, seq
        self.z_send, self.z_recv, self.y_send, self.y_recv = sems
        self.ins = inner_count(heads)
        self.outs = heads // self.ins
        self.at_out, self.at_in = head // self.ins, lax.rem(head, self.ins)
        chunk = parts.shape[1]
        half, early = chunk // 2, max(8, chunk // 8)
        self.halves = {0: pl.ds(0, half), self.ins: pl.ds(half, half)}
        self.sides = (pl.ds(0, half), pl.ds(chunk - early, early), pl.ds(half, half - early))

    def z_copy(self, place, j, up):
        where = place * self.ins + lax.rem(self.at_in + j, self.ins)
        piece = self.parts.at[where, self.halves.get(j, self.sides[1])]
        return remote(
            piece,
            piece,
            self.z_send.at[place, up, j],
            self.z_recv.at[place, j],
            self.seq,
            (self.at_out + 2 * up - 1) * self.ins + self.at_in,
        )

    def y_copy(self, where, j, part):
        place = where // self.ins
        piece = self.parts.at[where, self.sides[part]]
        return remote(
            piece,
            piece,
            self.y_send.at[place, j, part],
            self.y_recv.at[place, j, part],
            self.seq,
            self.at_out * self.ins + lax.rem(self.at_in + 1 + j, self.ins),
        )

    def onward(self, place, j, act):
        @pl.when((place >= self.at_out) & (self.at_out > 0))
        def _():
            act(self.z_copy(place, j, 0))

        @pl.when((place <= self.at_out) & (self.at_out < self.outs - 1))
        def _():
            act(self.z_copy(place, j, 1))

    def half(self, place, half):
        self.onward(place, half, lambda copy: copy.start())
        for j in range(self.ins - 1):
            self.y_copy(place * self.ins + self.at_in, j, 2 if half else 0).start()

    def start(self):
        for j in range(self.ins - 1):
            self.y_copy(self.at_out * self.ins + self.at_in, j, 1).start()
        self.half(self.at_out, 0)

    def second(self):
        self.half(self.at_out, self.ins)

    def early(self):
        for j in range(self.ins - 1):
            where = self.at_out * self.ins + lax.rem(self.at_in + self.ins - 1 - j, self.ins)
            self.y_copy(where, j, 1).wait_recv()
            self.onward(self.at_out, self.ins - 1 - j, lambda copy: copy.start())

    def relay(self, distance, part):
        for side in range(2):
            place = self.at_out + (2 * side - 1) * distance

            @pl.when((place >= 0) & (place < self.outs))
            def _():
                self.z_copy(place, part * self.ins, 0).wait_recv()
                self.half(place, part * self.ins)
                for j in range(1, self.ins if part else 1):
                    self.z_copy(place, j, 0).wait_recv()
                    self.onward(place, j, lambda copy: copy.start())

    def use(self, distance, consume):
        @pl.loop(0, 2 * self.ins)
        def _(n):
            side, j = n // self.ins, lax.rem(n, self.ins)
            late = (j + self.ins - 1) // self.ins
            away = distance - late
            place = self.at_out + (2 * side - 1) * away

            @pl.when(
                (place >= 0) & (place < self.outs) & (away >= 0) & (away + 1 - side > 0)
            )
            def _():
                where = place * self.ins + lax.rem(self.at_in + self.ins - j, self.ins)

                @pl.when(j > 0)
                def _():
                    self.y_copy(where, j - 1, 0).wait_recv()
                    self.y_copy(where, j - 1, 2).wait_recv()

                consume(where)

    def finish(self):
        mine = self.at_out * self.ins + self.at_in
        for place in range(self.outs):
            for j in range(self.ins + 1):
                self.onward(place, j, lambda copy: copy.wait_send())
            for j in range(self.ins - 1):
                self.y_copy(place * self.ins + self.at_in, j, 0).wait_send()
                self.y_copy(place * self.ins + self.at_in, j, 2).wait_send()
        for j in range(self.ins - 1):
            self.y_copy(mine, j, 1).wait_send()


def line_gather_sems(ins, outs):
    sems = pltpu.SemaphoreType.DMA
    return [
        sems((outs, 2, ins + 1)),
        sems((outs, ins + 1)),
        sems((outs, ins - 1, 3)),
        sems((outs, ins - 1, 3)),
    ]


def full_lanes(count):
    return -(-count // 128) * 128


def front_kernel(dims, *refs):
    seqs, heads, chunk, chans, pad = dims
    (
        rows, cot, gain, gate_w, inner_w, bc_w, step_w, out_w, conv_p, head_p, chan_p,
        hat_hi, hat_lo, pj_o, w_hi, w_lo,
        cot_hi, cot_lo, conv_hbm, cum_o, step_o, state_o, mixed_o, cross_o, stat_o,
        parts, cot_parts, hi, lo, pj, raw, wh, wl, wth, wtl, owh, owl,
        enter, prefix, run, exch, stat_all, lows,
        za_send, za_recv, ya_send, ya_recv, zb_send, zb_recv, yb_send, yb_recv,
        load_sem, put_sem, e_send, e_recv, s_send, s_recv, t_send, t_recv,
    ) = refs
    tokens = chunk * heads
    blocks = tokens // BLOCK
    span = 2 * chans
    wide = chans + 2 * NSTATE
    seq, head = lax.axis_index("seq"), lax.axis_index("head")
    convs = slice(0, wide)
    scaled = slice(768, 768 + chans)

    loads = [
        pltpu.make_async_copy(gate_w, raw.at[pl.ds(0, chans)], load_sem.at[0]),
        pltpu.make_async_copy(inner_w, raw.at[pl.ds(chans, chans)], load_sem.at[1]),
    ]
    for load in loads:
        load.start()
    values = rows[...]
    parts[head] = values * lax.rsqrt(
        jnp.mean(values * values, axis=1, keepdims=True) + EPSILON
    )
    cot_parts[head] = cot[...]
    greet(seq, head, seqs, heads)
    gather = LineGather(parts, (za_send, za_recv, ya_send, ya_recv), seq, head, heads)
    cotan = LineGather(cot_parts, (zb_send, zb_recv, yb_send, yb_recv), seq, head, heads)
    gather.start()

    raw[span : span + 2 * NSTATE, :] = bc_w[...].T
    raw[span + 2 * NSTATE :, :] = jnp.zeros((raw.shape[0] - span - 2 * NSTATE, raw.shape[1]), F32)
    raw[span + 2 * NSTATE : span + 2 * NSTATE + step_w.shape[0], :] = step_w[...]
    for load in loads:
        load.wait()
    gain_row = gain[...]

    def turn_weights(block):
        here = pl.ds(pl.multiple_of(block * 128, 128), 128)
        piece = raw[here, :]
        wh[here, :], wl[here, :] = halves(piece)
        wth[:, here], wtl[:, here] = halves((piece * gain_row).T)

    @pl.loop(0, pad // 256)
    def _(block):
        turn_weights(block)

    gather.second()
    gather.early()

    @pl.loop(pad // 256, pad // 128)
    def _(block):
        turn_weights(block)

    puts = [
        pltpu.make_async_copy(wh, w_hi, put_sem.at[0]),
        pltpu.make_async_copy(wl, w_lo, put_sem.at[1]),
    ]
    load_w = pltpu.make_async_copy(out_w, raw.at[pl.ds(0, chans)], load_sem.at[0])
    for copy in puts + [load_w]:
        copy.start()

    def chunk_rows(where):
        return pl.ds(pl.multiple_of(where * chunk, 8), chunk)

    def chunk_puts(where, top, low):
        here = chunk_rows(where)
        return [
            pltpu.make_async_copy(hi.at[where], top.at[here], put_sem.at[2 + 2 * where]),
            pltpu.make_async_copy(lo.at[where], low.at[here], put_sem.at[3 + 2 * where]),
        ]

    def project(where):
        top, low = halves(parts[where])
        hi[where] = top
        lo[where] = low
        here = pl.ds(pl.multiple_of(8 + where * chunk, 8), chunk)
        pj[here, :] = dot3((top, low), (wth[...], wtl[...]), 1, 0)
        for put in chunk_puts(where, hat_hi, hat_lo):
            put.start()

    assert gather.outs == 4
    expand = head_lanes(chans)

    @pl.loop(0, 5)
    def _(distance):
        @pl.when(distance == 0)
        def _():
            gather.relay(1, 0)

        @pl.when(distance == 1)
        def _():
            load_w.wait()
            for lane, end in lanes_of(chans):
                owh[:, lane:end], owl[:, lane:end] = halves(raw[lane:end, :].T)
            gather.relay(1, 1)
            gather.relay(2, 0)

        @pl.when(distance == 2)
        def _():
            gather.relay(2, 1)
            gather.relay(3, 0)

        @pl.when(distance == 3)
        def _():
            gather.relay(3, 1)
            cotan.start()

        @pl.when(distance == 4)
        def _():
            cotan.second()
            cotan.early()

        gather.use(distance, project)

    edge = remote(
        pj.at[pl.ds(tokens, 8)],
        pj.at[pl.ds(0, 8)],
        e_send,
        e_recv,
        lax.rem(seq + 1, seqs),
        head,
    )
    edge.start()
    cotan.relay(1, 0)
    edge.wait()
    pj[0:8, :] = jnp.where(seq > 0, pj[0:8, :], 0.0)
    pj_put = pltpu.make_async_copy(pj, pj_o, put_sem.at[2 + 2 * heads])
    pj_put.start()
    cotan.relay(1, 1)
    cotan.relay(2, 0)
    tri_r = lax.broadcasted_iota(jnp.int32, (BLOCK, BLOCK), 0)
    tri_c = lax.broadcasted_iota(jnp.int32, (BLOCK, BLOCK), 1)
    causal = tri_r >= tri_c
    lower = causal.astype(F32)
    run[...] = jnp.zeros_like(run)
    prefix[...] = jnp.zeros_like(prefix)

    @pl.loop(0, blocks)
    def _(b):
        at = pl.multiple_of(b * BLOCK, BLOCK)
        here = pl.ds(at, BLOCK)
        window = pj[pl.ds(at, BLOCK + 8), chans : span + 2 * NSTATE]
        conv = jnp.zeros((BLOCK, wide), F32) + conv_p[4:5, :]
        for k in range(WIDTH):
            conv = conv + conv_p[k : k + 1, :] * window[5 + k : 5 + k + BLOCK, :]
        raw[here, convs] = conv
        act = conv * logistic(conv)
        arg = pj[pl.ds(at + 8, BLOCK), span + 2 * NSTATE : pad] + head_p[0:1, :]
        step = jnp.maximum(arg, 0.0) + jnp.log1p(jnp.exp(-jnp.abs(arg)))
        cum = dotx(lower, step * head_p[1:2, :], 1, 0)
        last = cum[BLOCK - 1 : BLOCK, :]
        step_o[here, :] = step
        cum_o[here, :] = cum
        fed = act[:, :chans] * spread(step, expand)
        raw[here, scaled] = fed
        fresh = dot3x(
            fed * spread(jnp.exp(last - cum), expand), act[:, chans : chans + NSTATE], 0, 0
        )
        enter[b] = run[...]
        run[...] = row_scale(last, expand) * run[...] + fresh
        prefix[pl.ds(b + 1, 1), :] = prefix[pl.ds(b, 1), :] + last

        @pl.when(b == blocks // 2)
        def _():
            cotan.relay(2, 1)

    conv_put = pltpu.make_async_copy(
        raw.at[pl.ds(0, tokens), pl.ds(0, full_lanes(wide))], conv_hbm, put_sem.at[3 + 2 * heads]
    )
    conv_put.start()
    exch[seq, 0:chans, :] = run[...]
    exch[seq, chans : chans + 8, :] = jnp.broadcast_to(prefix[blocks : blocks + 1, :], (8, 128))

    def state_copy(at, j, to):
        return remote(exch.at[at], exch.at[at], s_send.at[j - 1], s_recv.at[j - 1], to, head)

    for j in range(1, seqs):

        @pl.when(seq + j < seqs)
        def _():
            state_copy(seq, j, seq + j).start()

    @pl.loop(0, blocks)
    def _(b):
        at = pl.multiple_of(b * BLOCK, BLOCK)
        here = pl.ds(at, BLOCK)
        bc = raw[here, chans:wide]
        bc = bc * logistic(bc)
        scores = dot3x(bc[:, NSTATE:], bc[:, :NSTATE], 1, 1)
        cum = cum_o[here, :]
        turned = cum.T
        for first_lane, end in lanes_of(chans):
            fed = halves(raw[here, scaled.start + first_lane : scaled.start + end])
            outs = [
                dot3(
                    halves(decay_of(cum, turned, lane // HEADDIM, causal) * scores), fed, 1, 0
                )
                for lane in range(first_lane, end, HEADDIM)
            ]
            out = outs[0]
            if len(outs) == 2:
                lane = lax.broadcasted_iota(jnp.int32, out.shape, 1)
                out = jnp.where(lane < HEADDIM, outs[0], outs[1])
            mixed_o[here, first_lane:end] = out

        @pl.when(b == 0)
        def _():
            cotan.relay(3, 0)

        @pl.when(b == blocks // 2)
        def _():
            cotan.relay(3, 1)

    run[...] = jnp.zeros_like(run)
    for earlier in range(seqs - 1):

        @pl.when(earlier < seq)
        def _():
            for j in range(1, seqs):

                @pl.when(seq - earlier == j)
                def _():
                    state_copy(earlier, j, lax.rem(seq + 1, seqs)).wait_recv()

            run[...] = (
                row_scale(exch[earlier, chans : chans + 1, :], expand) * run[...]
                + exch[earlier, 0:chans, :]
            )

    @pl.loop(0, blocks)
    def _(b):
        at = pl.multiple_of(b * BLOCK, BLOCK)
        here = pl.ds(at, BLOCK)
        state = enter[b] + row_scale(prefix[pl.ds(b, 1), :], expand) * run[...]
        state_o[b] = state
        conv = raw[here, convs]
        act = conv * logistic(conv)
        gate = pj[pl.ds(at + 8, BLOCK), 0:chans]
        carried = dot3x(act[:, chans + NSTATE :], state, 1, 1)
        mixed = (
            mixed_o[here, :]
            + carried * spread(jnp.exp(cum_o[here, :]), expand)
            + chan_p[1:2, :] * act[:, :chans]
        )
        mixed_o[here, :] = mixed
        raw[here, scaled] = mixed * gate * logistic(gate)

    ones = jnp.ones((8, chans), F32)
    groups = tokens // 128

    def statistics(n):
        here = pl.ds(pl.multiple_of(n * 128, 128), 128)
        gated = raw[here, scaled]
        lows[pl.ds(n, 1), :] = dotx(ones, gated * gated, 1, 1)[0:1, :]
        lows[pl.ds(groups + n, 1), :] = dotx(
            ones, cross_o[here, :] * chan_p[0:1, :] * gated, 1, 1
        )[0:1, :]

    def consume(where):
        here = chunk_rows(where)
        for put in chunk_puts(where, hat_hi, hat_lo):
            put.wait()
        top, low = halves(cot_parts[where])
        hi[where] = top
        lo[where] = low
        cross_o[here, :] = dot3((top, low), (owh[...], owl[...]), 1, 0)
        for put in chunk_puts(where, cot_hi, cot_lo):
            put.start()
        if chunk == 128:
            statistics(where)

    @pl.loop(0, cotan.outs + 1)
    def _(distance):
        cotan.use(distance, consume)

    if chunk != 128:

        @pl.loop(0, groups)
        def _(n):
            statistics(n)

    stat_all[head] = lows[...]
    sends = []
    for j in range(1, heads):
        sends.append(
            remote(
                stat_all.at[head],
                stat_all.at[head],
                t_send.at[j - 1],
                t_recv.at[j - 1],
                seq,
                lax.rem(head + j, heads),
            )
        )
        sends[-1].start()
    gather.finish()
    cotan.finish()
    for put in puts + [pj_put, conv_put]:
        put.wait()

    @pl.loop(0, heads)
    def _(where):
        for put in chunk_puts(where, cot_hi, cot_lo):
            put.wait()

    for j in range(1, seqs):

        @pl.when(seq + j < seqs)
        def _():
            state_copy(seq, j, seq + j).wait_send()

    for j in range(1, heads):
        came = lax.rem(head - j + heads, heads)
        remote(
            stat_all.at[came], stat_all.at[came], t_send.at[j - 1], t_recv.at[j - 1], seq, came
        ).wait_recv()
    total = stat_all[0]
    for j in range(1, heads):
        total = total + stat_all[j]
    stat_o[...] = total
    for copy in sends:
        copy.wait_send()


def front(
    resid, cot, gain, gate_w, inner_w, bc_w, step_w, out_w, conv_p, head_p, chan_p,
    seqs, heads,
):
    chunk, width = resid.shape
    chans = gate_w.shape[0]
    pad = 2 * chans + 2 * NSTATE + 128
    ins = inner_count(heads)
    outs = heads // ins
    tokens = chunk * heads
    wide = chans + 2 * NSTATE
    blocks = tokens // BLOCK
    groups = 2 * tokens // 128
    anywhere = pl.BlockSpec(memory_space=pl.ANY)
    local = pl.BlockSpec(memory_space=pltpu.VMEM)
    sems = pltpu.SemaphoreType.DMA
    shape = jax.ShapeDtypeStruct
    return pl.pallas_call(
        functools.partial(front_kernel, (seqs, heads, chunk, chans, pad)),
        out_shape=(
            shape((tokens, width), BF16),
            shape((tokens, width), BF16),
            shape((8 + tokens, pad), F32),
            shape((pad, width), BF16),
            shape((pad, width), BF16),
            shape((tokens, width), BF16),
            shape((tokens, width), BF16),
            shape((tokens, full_lanes(wide)), F32),
            shape((tokens, 128), F32),
            shape((tokens, 128), F32),
            shape((blocks, chans, NSTATE), F32),
            shape((tokens, chans), F32),
            shape((tokens, chans), F32),
            shape((groups, 128), F32),
        ),
        in_specs=[local] * 3 + [anywhere] * 2 + [local] * 2 + [anywhere] + [local] * 3,
        out_specs=(anywhere,) * 8 + (local,) * 6,
        scratch_shapes=[
            pltpu.VMEM((heads, chunk, width), F32),
            pltpu.VMEM((heads, chunk, width), F32),
            pltpu.VMEM((heads, chunk, width), BF16),
            pltpu.VMEM((heads, chunk, width), BF16),
            pltpu.VMEM((8 + tokens, pad), F32),
            pltpu.VMEM((max(pad, tokens), width), F32),
            pltpu.VMEM((pad, width), BF16),
            pltpu.VMEM((pad, width), BF16),
            pltpu.VMEM((width, pad), BF16),
            pltpu.VMEM((width, pad), BF16),
            pltpu.VMEM((width, chans), BF16),
            pltpu.VMEM((width, chans), BF16),
            pltpu.VMEM((blocks, chans, NSTATE), F32),
            pltpu.VMEM((8, 128), F32),
            pltpu.VMEM((chans, NSTATE), F32),
            pltpu.VMEM((seqs, chans + 8, NSTATE), F32),
            pltpu.VMEM((heads, groups, 128), F32),
            pltpu.VMEM((groups, 128), F32),
            *line_gather_sems(ins, outs),
            *line_gather_sems(ins, outs),
            sems((2,)),
            sems((4 + 2 * heads,)),
            sems,
            sems,
            sems((seqs - 1,)),
            sems((seqs - 1,)),
            sems((heads - 1,)),
            sems((heads - 1,)),
        ],
        compiler_params=pltpu.CompilerParams(
            collective_id=2, has_side_effects=True, vmem_limit_bytes=VMEM_LIMIT
        ),
        name="front",
    )(resid, cot, gain, gate_w, inner_w, bc_w, step_w, out_w, conv_p, head_p, chan_p)


class LineReduce:
    def __init__(self, parts, y_in, z_in, sems, seq, head, heads, partner, depth):
        self.depth = depth
        self.parts, self.y_in, self.z_in = parts, y_in, z_in
        self.y_send, self.y_recv, self.z_send, self.z_recv = sems
        self.seq, self.partner = seq, partner
        self.ins = inner_count(heads)
        self.outs = heads // self.ins
        self.half = parts.shape[1] // 2
        self.turns = 2 * self.outs
        self.at_out, self.at_in = head // self.ins, lax.rem(head, self.ins)
        self.upper = self.at_out // (self.outs // 2)
        self.mirrored = self.at_out + self.upper * (self.outs - 1 - 2 * self.at_out)

    def target(self, step):
        last = (step + 1) // self.outs
        far = self.outs - 1 - step
        far = far - (self.mirrored - far + self.outs) // self.outs
        far = far + self.upper * (self.outs - 1 - 2 * far)
        return far + last * (self.at_out - far)

    def rows(self, turn):
        return pl.ds(pl.multiple_of(lax.rem(turn, 2) * self.half, 8), self.half)

    def y_copy(self, turn, j):
        goal = self.target(turn // 2)
        to = lax.rem(self.at_in + 1 + j, self.ins)
        rows = self.rows(turn)
        return remote(
            self.parts.at[goal * self.ins + to, rows],
            self.y_in.at[goal * (self.ins - 1) + j, rows],
            self.y_send.at[turn, j],
            self.y_recv.at[turn, j],
            self.seq,
            self.at_out * self.ins + to,
        )

    def give(self, turn):
        for j in range(self.ins - 1):
            self.y_copy(turn, j).start()

    def add(self, where, turn, source, slot):
        @pl.loop(0, self.half // 16)
        def _(n):
            first = lax.rem(turn, 2) * self.half + n * 16
            rows = pl.ds(pl.multiple_of(first, 8), 16)
            self.parts[where, rows, :] = self.parts[where, rows, :] + source[slot, rows, :]

    def take(self, turn, slot):
        rows = self.rows(turn)
        where = self.target(turn // 2) * self.ins + self.at_in
        remote(
            self.parts.at[0, rows],
            self.z_in.at[slot, rows],
            self.z_send.at[0],
            self.z_recv.at[slot, lax.rem(turn, 2)],
            self.partner,
            self.at_out * self.ins + self.at_in,
        ).wait_recv()
        self.add(where, turn, self.z_in, slot)

    def pass_on(self, turn, up):
        goal, rows = self.target(turn // 2), self.rows(turn)
        remote(
            self.parts.at[goal * self.ins + self.at_in, rows],
            self.z_in.at[goal + up, rows],
            self.z_send.at[turn],
            self.z_recv.at[goal + up, lax.rem(turn, 2)],
            self.seq,
            (self.at_out + 2 * up - 1) * self.ins + self.at_in,
        ).start()

    def across(self, turn):
        goal = self.target(turn // 2)
        where = goal * self.ins + self.at_in
        for j in range(self.ins - 1):
            self.y_copy(turn, j).wait_recv()

        @pl.when(turn + self.depth < self.turns)
        def _():
            self.give(turn + self.depth)

        for j in range(self.ins - 1):
            self.add(where, turn, self.y_in, goal * (self.ins - 1) + j)

        @pl.when((goal > self.at_out) & (self.at_out == 0))
        def _():
            self.pass_on(turn, 1)

        @pl.when((goal < self.at_out) & (self.at_out == self.outs - 1))
        def _():
            self.pass_on(turn, 0)

    def along(self, turn):
        goal = self.target(turn // 2)

        @pl.when((goal >= self.at_out) & (self.at_out > 0))
        def _():
            self.take(turn, goal + 1)

        @pl.when((goal <= self.at_out) & (self.at_out < self.outs - 1))
        def _():
            self.take(turn, goal)

        @pl.when((goal > self.at_out) & (self.at_out > 0))
        def _():
            self.pass_on(turn, 1)

        @pl.when((goal < self.at_out) & (self.at_out < self.outs - 1))
        def _():
            self.pass_on(turn, 0)

    def reduce(self, turn):
        turn = jnp.int32(turn)
        self.across(turn)

        @pl.when(turn > 0)
        def _():
            self.along(turn - 1)

    def last(self):
        self.along(jnp.int32(self.turns - 1))

    def finish(self):
        @pl.loop(0, self.turns)
        def _(turn):
            for j in range(self.ins - 1):
                self.y_copy(turn, j).wait_send()

        @pl.loop(0, self.turns - 2)
        def _(turn):
            rows = pl.ds(0, self.half)
            remote(
                self.parts.at[0, rows],
                self.z_in.at[0, rows],
                self.z_send.at[turn],
                self.z_recv.at[0, 0],
                self.partner,
                self.at_out * self.ins + self.at_in,
            ).wait_send()


def line_reduce_sems(ins, outs):
    sems = pltpu.SemaphoreType.DMA
    return [
        sems((2 * outs, ins - 1)),
        sems((2 * outs, ins - 1)),
        sems((2 * outs,)),
        sems((outs + 1, 2)),
    ]


def backward_kernel(dims, *refs):
    seqs, heads, chunk, chans, pad = dims
    (
        proj, cot_hi, cot_lo, hat_hi, hat_lo, conv_in, cum_in, step_in, state_in, mixed_in, cross_in,
        stat_in, out_w, resid, conv_p, head_p, chan_p, gain,
        result_o, gp_hi, gp_lo, out_o, gate_o, wide_o, chan_o, head_o,
        pj, ngh, ngl, owh, owl, gmix, fedg, adj, run, exch, gconv,
        parts, y_in, z_in, chi, clo, oparts, columns, conv_buf, head_acc,
        keep_o, core_o, x_o, o_sems, keep_g, core_g, g_sems, gate_sem,
        y_send, y_recv, z_send, z_recv, load_sem, s_send, s_recv, e_send, e_recv, conv_sem,
    ) = refs
    tokens = chunk * heads
    blocks = tokens // BLOCK
    span = 2 * chans
    wide = chans + 2 * NSTATE
    split_at = resid.shape[1] // 2
    seq, head = lax.axis_index("seq"), lax.axis_index("head")
    side = lax.rem(seq, 2)
    partner = seq + 1 - 2 * side
    loads = [
        pltpu.make_async_copy(a, b, load_sem.at[n])
        for n, (a, b) in enumerate(
            (
                (proj, pj),
                (cot_hi.at[:, pl.ds(0, split_at)], chi),
                (cot_lo.at[:, pl.ds(0, split_at)], clo),
                (out_w, oparts),
            )
        )
    ]
    for load in loads:
        load.start()
    greet(seq, head, seqs, heads)
    loads[3].wait()
    owh[...], owl[...] = halves(oparts[...])
    expand = head_lanes(chans)
    tri_r = lax.broadcasted_iota(jnp.int32, (BLOCK, BLOCK), 0)
    tri_c = lax.broadcasted_iota(jnp.int32, (BLOCK, BLOCK), 1)
    anticausal = tri_r <= tri_c
    upper = anticausal.astype(F32)
    wide_o[...] = jnp.zeros_like(wide_o)
    chan_o[...] = jnp.zeros_like(chan_o)
    head_acc[...] = jnp.zeros_like(head_acc)
    run[...] = jnp.zeros_like(run)
    loads[0].wait()
    groups = tokens // 128
    turned_stats = stat_in[...].T
    inner_total = float(heads * chans)
    gain_row, skip_row = chan_p[0:1, :], chan_p[1:2, :]
    for n in range(groups):
        here = slice(n * 128, n * 128 + 128)
        scale = lax.rsqrt(turned_stats[:, n : n + 1] / inner_total + EPSILON)
        cross = turned_stats[:, groups + n : groups + n + 1]
        columns[here, 0:1] = scale
        columns[here, 1:2] = scale * scale * scale * (cross / inner_total)

    def conv_load(b, slot):
        return pltpu.make_async_copy(
            conv_in.at[pl.ds(pl.multiple_of(b * BLOCK, BLOCK), BLOCK)],
            conv_buf.at[slot],
            conv_sem.at[slot],
        )

    def conv_of(n, b, following):
        slot = lax.rem(n, 2)
        conv_load(b, slot).wait()
        conv_load(following, 1 - slot).start()
        return conv_buf[slot, :, :wide]

    conv_load(blocks - 1, 0).start()

    @pl.loop(0, blocks)
    def _(b):
        at = pl.multiple_of(b * BLOCK, BLOCK)
        here = pl.ds(at, BLOCK)
        gate = pj[pl.ds(at + 8, BLOCK), 0:chans]
        ngh[here, :], ngl[here, :] = halves(
            mixed_in[here, :] * (gate * logistic(gate)) * columns[here, 0:1] * gain_row
        )

    reduce = LineReduce(
        parts, y_in, z_in, (y_send, y_recv, z_send, z_recv), seq, head, heads, partner, 3
    )

    ins = reduce.ins

    def produce(step):
        first = reduce.target(step) * ins
        rows = pl.ds(pl.multiple_of(first * chunk, 8), ins * chunk)
        out = dot3((ngh[rows, :], ngl[rows, :]), (owh[...], owl[...]), 1, 0)
        for n in range(ins):
            parts[first + n] = out[n * chunk : (n + 1) * chunk]

    @pl.loop(0, reduce.outs)
    def _(step):
        produce(step)

        @pl.when(step == 0)
        def _():
            reduce.give(jnp.int32(0))

    for load in loads[1:3]:
        load.wait()

    def weight_parts(left_hi, left_lo, hi, lo, then):
        def halves_of(source, first):
            return [
                pltpu.make_async_copy(a.at[:, pl.ds(first, split_at)], b, load_sem.at[1 + m])
                for m, (a, b) in enumerate(zip(source, (chi, clo)))
            ]

        second = halves_of((hi, lo), split_at)

        @pl.loop(0, 2)
        def _(n):
            cols = pl.ds(pl.multiple_of(n * split_at, 128), split_at)
            oparts[:, cols] = dot3((left_hi[...], left_lo[...]), (chi[...], clo[...]), 0, 0)

            @pl.when(n == 0)
            def _():
                for load in second:
                    load.start()
                for load in second:
                    load.wait()

        if then is None:
            return None
        following = halves_of(then, 0)
        for load in following:
            load.start()
        return following

    reduce.give(jnp.int32(1))
    hat_load = weight_parts(ngh, ngl, cot_hi, cot_lo, (hat_hi, hat_lo))
    out_sum = SeqSum(oparts, 0, keep_o, core_o, x_o, o_sems, out_o, seq, head, seqs)
    out_sum.begin()
    reduce.give(jnp.int32(2))

    out_sum.pair()
    out_sum.start()

    def poll(n, base):
        @pl.when(lax.rem(n, pace) == pace - 1)
        def _():
            reduce.reduce(base + n // pace)

    pace = max(1, blocks // 2)

    @pl.loop(0, blocks)
    def _(back):
        b = blocks - 1 - back
        at = pl.multiple_of(b * BLOCK, BLOCK)
        here = pl.ds(at, BLOCK)
        scale = columns[here, 0:1]
        gate = pj[pl.ds(at + 8, BLOCK), 0:chans]
        sig = logistic(gate)
        gate_act = gate * sig
        mixed = mixed_in[here, :]
        gated = mixed * gate_act
        grad_ng = cross_in[here, :]
        grad_gated = scale * (grad_ng * gain_row) - gated * columns[here, 1:2]
        grad_mixed = grad_gated * gate_act
        gmix[here, :] = grad_mixed
        gp_hi[here, 0:chans], gp_lo[here, 0:chans] = halves(
            grad_gated * mixed * (sig * (1.0 + gate * (1.0 - sig)))
        )
        conv = conv_of(back, b, jnp.maximum(b - 1, 0))
        act = conv * logistic(conv)
        chan_o[0:1, :] = chan_o[0:1, :] + jnp.sum(grad_ng * (gated * scale), 0, keepdims=True)
        chan_o[1:2, :] = chan_o[1:2, :] + jnp.sum(grad_mixed * act[:, :chans], 0, keepdims=True)
        early = grad_mixed * spread(jnp.exp(cum_in[here, :]), expand)
        adj[b] = run[...]
        run[...] = row_scale(cum_in[pl.ds(at + BLOCK - 1, 1), :], expand) * run[...] + dot3x(
            early, act[:, chans + NSTATE :], 0, 0
        )
        gconv[here, chans + NSTATE :] = dot3x(early, state_in[b], 1, 0)
        poll(back, 0)

    total = jnp.zeros((1, 128), F32)
    for b in range(blocks):
        total = total + cum_in[(b + 1) * BLOCK - 1 : (b + 1) * BLOCK, :]
    exch[seq, 0:chans, :] = run[...]
    exch[seq, chans : chans + 8, :] = jnp.broadcast_to(total, (8, 128))

    def state_copy(at, j, to):
        return remote(exch.at[at], exch.at[at], s_send.at[j - 1], s_recv.at[j - 1], to, head)

    for j in range(1, seqs):

        @pl.when(seq - j >= 0)
        def _():
            state_copy(seq, j, seq - j).start()

    for load in hat_load:
        load.wait()
    weight_parts(gp_hi.at[:, 0:chans], gp_lo.at[:, 0:chans], hat_hi, hat_lo, None)
    oparts[...] = oparts[...] * gain[...]
    gate_sum = SeqSum(oparts, 0, keep_g, core_g, None, g_sems, None, seq, head, seqs)
    gate_sum.begin()
    gate_put = pltpu.make_async_copy(keep_g, gate_o, gate_sem)
    reduce.reduce(2)

    @pl.loop(0, blocks)
    def _(b):
        at = pl.multiple_of(b * BLOCK, BLOCK)
        here = pl.ds(at, BLOCK)
        conv = conv_of(b, b, lax.rem(b + 1, blocks))
        act = conv * logistic(conv)
        writes, reads = act[:, chans : chans + NSTATE], act[:, chans + NSTATE :]
        scores = dot3x(writes, reads, 1, 1)
        cum = cum_in[here, :]
        turned = cum.T
        fed_all = act[:, :chans] * spread(step_in[here, :], expand)
        grad_scores = jnp.zeros((BLOCK, BLOCK), F32)
        for first_lane, end in lanes_of(chans):
            fed = fed_all[:, first_lane:end]
            grad = gmix[here, first_lane:end]
            grad_parts, grad_turned = halves(grad), halves(grad.T)
            lane = lax.broadcasted_iota(jnp.int32, fed.shape, 1)
            outs = []
            for start in range(first_lane, end, HEADDIM):
                decay = decay_turned(cum, turned, start // HEADDIM, anticausal)
                inside = (lane // HEADDIM) == (start - first_lane) // HEADDIM
                grad_scores = grad_scores + decay * dot3(
                    halves(jnp.where(inside, fed, 0.0)), grad_turned, 1, 0
                )
                outs.append(dot3(halves(decay * scores), grad_parts, 1, 0))
            out = outs[0]
            if len(outs) == 2:
                out = jnp.where(lane < HEADDIM, outs[0], outs[1])
            fedg[here, first_lane:end] = out
        score_parts = halves(grad_scores)
        gconv[here, chans : chans + NSTATE] = dot3(score_parts, halves(reads), 1, 0)
        gconv[here, chans + NSTATE :] = gconv[here, chans + NSTATE :] + dot3(score_parts, halves(writes), 0, 0)
        poll(b, 3)

        @pl.when(b == 0)
        def _():
            gate_sum.pair()
            gate_put.start()


    run[...] = jnp.zeros_like(run)
    for back in range(seqs - 1):
        later = seqs - 1 - back

        @pl.when(later > seq)
        def _():
            for j in range(1, seqs):

                @pl.when(later - seq == j)
                def _():
                    state_copy(later, j, partner).wait_recv()

            run[...] = (
                row_scale(exch[later, chans : chans + 1, :], expand) * run[...]
                + exch[later, 0:chans, :]
            )

    @pl.loop(0, blocks)
    def _(back):
        b = blocks - 1 - back
        adj[b] = adj[b] + run[...]
        run[...] = row_scale(cum_in[pl.ds((b + 1) * BLOCK - 1, 1), :], expand) * run[...]

    lane_ones = jnp.ones((8, NSTATE), F32)

    @pl.loop(0, blocks)
    def _(b):
        at = pl.multiple_of(b * BLOCK, BLOCK)
        here = pl.ds(at, BLOCK)
        conv = conv_of(b, b, lax.rem(b + 1, blocks))
        sig = logistic(conv)
        act = conv * sig
        slope = sig * (1.0 + conv * (1.0 - sig))
        inner, writes = act[:, :chans], act[:, chans : chans + NSTATE]
        cum = cum_in[here, :]
        step = step_in[here, :]
        last = cum[BLOCK - 1 : BLOCK, :]
        step_wide = spread(step, expand)
        tails = spread(jnp.exp(last - cum), expand)
        fed = inner * step_wide
        grad_state = adj[b]
        state_parts = halves(grad_state)
        from_state = tails * dot3(halves(writes), state_parts, 1, 1)
        grad_fed = fedg[here, :] + from_state
        grad_mixed = gmix[here, :]
        grad_writes = gconv[here, chans : chans + NSTATE] + dot3(halves(fed * tails), state_parts, 1, 0)
        direct = gather_heads(inner * grad_fed, expand)
        scanned = mixed_in[here, :] - skip_row * inner
        grad_cum = dotx(grad_mixed * scanned - fed * grad_fed, expand, 1, 1)
        kept = dotx(expand, grad_state * state_in[b], 1, 0)
        kept = dotx(lane_ones, kept, 1, 1)[0:1, :] * jnp.exp(last)
        grad_last = kept + jnp.sum(gather_heads(fed * from_state, expand), 0, keepdims=True)
        grad_log = dotx(upper, grad_cum, 1, 0) + grad_last
        rate = head_p[1:2, :]
        head_acc[1:2, :] = head_acc[1:2, :] + jnp.sum(step * grad_log, 0, keepdims=True) * rate
        arg = pj[pl.ds(at + 8, BLOCK), span + 2 * NSTATE : pad] + head_p[0:1, :]
        grad_arg = (direct + rate * grad_log) * logistic(arg) * head_p[2:3, :]
        head_acc[0:1, :] = head_acc[0:1, :] + jnp.sum(grad_arg, 0, keepdims=True)
        gp_hi[here, span + 2 * NSTATE : pad], gp_lo[here, span + 2 * NSTATE : pad] = halves(
            grad_arg
        )
        gconv[here, 0:chans] = (step_wide * grad_fed + skip_row * grad_mixed) * slope[:, :chans]
        gconv[here, chans : chans + NSTATE] = grad_writes * slope[:, chans : chans + NSTATE]
        gconv[here, chans + NSTATE :] = gconv[here, chans + NSTATE :] * slope[:, chans + NSTATE :]

        @pl.when(b == blocks // 2 - 1)
        def _():
            reduce.reduce(5)

    out_sum.total()
    edge = remote(
        gconv.at[pl.ds(0, 8)],
        gconv.at[pl.ds(tokens, 8)],
        e_send,
        e_recv,
        lax.rem(seq + seqs - 1, seqs),
        head,
    )
    edge.start()
    head_o[...] = head_acc[...]

    def conv_back(b):
        at = pl.multiple_of(b * BLOCK, BLOCK)
        here = pl.ds(at, BLOCK)
        before = pj[pl.ds(at + 8, BLOCK), chans : span + 2 * NSTATE]
        ahead = gconv[pl.ds(at, BLOCK + 8), :]
        grad = ahead[0:BLOCK, :]
        grad_pre = jnp.zeros((BLOCK, wide), F32)
        for k in range(WIDTH):
            later = ahead[3 - k : 3 - k + BLOCK, :]
            grad_pre = grad_pre + conv_p[k : k + 1, :] * later
            wide_o[k : k + 1, :] = wide_o[k : k + 1, :] + jnp.sum(
                later * before, 0, keepdims=True
            )
        wide_o[4:5, :] = wide_o[4:5, :] + jnp.sum(grad, 0, keepdims=True)
        (
            gp_hi[here, chans : span + 2 * NSTATE],
            gp_lo[here, chans : span + 2 * NSTATE],
        ) = halves(grad_pre)

    @pl.loop(0, blocks)
    def _(b):
        @pl.when(b == blocks - 1)
        def _():
            reduce.reduce(6)
            edge.wait()
            gconv[tokens : tokens + 8, :] = jnp.where(
                seq < seqs - 1, gconv[tokens : tokens + 8, :], 0.0
            )

        conv_back(b)

    reduce.reduce(7)
    reduce.last()
    result_o[...] = resid[...] + parts[head]
    conv_load(0, 0).wait()
    reduce.finish()
    for j in range(1, seqs):

        @pl.when(seq - j >= 0)
        def _():
            state_copy(seq, j, seq - j).wait_send()

    out_sum.end()
    gate_put.wait()


def backward(proj, hat, kept, out_w, resid, conv_p, head_p, chan_p, gain, seqs, heads):
    (cot_hi, cot_lo, conv, cum, step, state, mixed, cross, stat) = kept
    tokens, pad = cum.shape[0], proj.shape[1]
    chunk, width = resid.shape
    chans = out_w.shape[0]
    ins = inner_count(heads)
    outs = heads // ins
    wide = chans + 2 * NSTATE
    blocks = tokens // BLOCK
    half = chans // 2
    rounds = (seqs // 2).bit_length() - 1
    anywhere = pl.BlockSpec(memory_space=pl.ANY)
    local = pl.BlockSpec(memory_space=pltpu.VMEM)
    sems = pltpu.SemaphoreType.DMA
    shape = jax.ShapeDtypeStruct
    return pl.pallas_call(
        functools.partial(backward_kernel, (seqs, heads, chunk, chans, pad)),
        out_shape=(
            shape((chunk, width), F32),
            shape((tokens, pad), BF16),
            shape((tokens, pad), BF16),
            shape((chans, width), F32),
            shape((half, width), F32),
            shape((8, wide), F32),
            shape((8, chans), F32),
            shape((8, 128), F32),
        ),
        in_specs=[anywhere] * 6 + [local] * 6 + [anywhere] + [local] * 5,
        out_specs=(local, local, local, anywhere, anywhere, local, local, local),
        scratch_shapes=[
            pltpu.VMEM((8 + tokens, pad), F32),
            pltpu.VMEM((tokens, chans), BF16),
            pltpu.VMEM((tokens, chans), BF16),
            pltpu.VMEM((chans, width), BF16),
            pltpu.VMEM((chans, width), BF16),
            pltpu.VMEM((tokens, chans), F32),
            pltpu.VMEM((tokens, chans), F32),
            pltpu.VMEM((blocks, chans, NSTATE), F32),
            pltpu.VMEM((chans, NSTATE), F32),
            pltpu.VMEM((seqs, chans + 8, NSTATE), F32),
            pltpu.VMEM((tokens + 8, wide), F32),
            pltpu.VMEM((heads, chunk, width), F32),
            pltpu.VMEM((outs * (ins - 1), chunk, width), F32),
            pltpu.VMEM((outs + 1, chunk, width), F32),
            pltpu.VMEM((tokens, width // 2), BF16),
            pltpu.VMEM((tokens, width // 2), BF16),
            pltpu.VMEM((chans, width), F32),
            pltpu.VMEM((tokens, 128), F32),
            pltpu.VMEM((2, BLOCK, full_lanes(wide)), F32),
            pltpu.VMEM((8, 128), F32),
            *seq_sum_scratch(half, width, rounds),
            pltpu.VMEM((half, width), F32),
            pltpu.VMEM((half, width), F32),
            sems((2,)),
            sems,
            *line_reduce_sems(ins, outs),
            sems((4,)),
            sems((seqs - 1,)),
            sems((seqs - 1,)),
            sems,
            sems,
            sems((2,)),
        ],
        compiler_params=pltpu.CompilerParams(
            collective_id=4, has_side_effects=True, vmem_limit_bytes=VMEM_LIMIT
        ),
        name="backward",
    )(
        proj, cot_hi, cot_lo, *hat, conv, cum, step, state, mixed, cross, stat,
        out_w, resid, conv_p, head_p, chan_p, gain,
    )


def on_device(
    residual_in,
    norm_gain,
    gate_weight,
    inner_weight,
    bc_weight,
    step_weight,
    conv_inner_weight,
    conv_inner_bias,
    conv_bc_weight,
    conv_bc_bias,
    step_bias,
    decay_log,
    skip_gain,
    gated_gain,
    out_weight,
    cotangent,
):
    seqs, heads = lax.axis_size("seq"), lax.axis_size("head")
    width = residual_in.shape[2]
    chans = gate_weight.shape[0]
    heads_here = step_weight.shape[0]
    spare = 128 - heads_here
    resid = residual_in.reshape(-1, width)
    cot = cotangent.reshape(-1, width)
    gain = norm_gain.reshape(1, width)

    def eight(part):
        return jnp.pad(part, ((0, 8 - part.shape[0]), (0, 0)))

    def by_head(*parts):
        return eight(jnp.pad(jnp.stack(parts), ((0, 0), (0, spare))))

    conv_p = eight(
        jnp.concatenate(
            [
                jnp.concatenate([conv_inner_weight, conv_bc_weight], 1),
                jnp.concatenate([conv_inner_bias, conv_bc_bias])[None],
            ],
            0,
        )
    )
    head_p = by_head(step_bias, -jnp.exp(decay_log), jnp.ones_like(step_bias))
    chan_p = eight(jnp.stack([gated_gain, jnp.repeat(skip_gain, HEADDIM)]))
    hat_hi, hat_lo, projected, weight_hi, weight_lo, *kept = front(
        resid,
        cot,
        gain,
        gate_weight,
        inner_weight,
        bc_weight,
        step_weight,
        out_weight,
        conv_p,
        head_p,
        chan_p,
        seqs,
        heads,
    )
    (
        result,
        grad_hi,
        grad_lo,
        out_weight_grad,
        gate_half,
        wide_sums,
        chan_sums,
        head_sums,
    ) = backward(
        projected,
        (hat_hi, hat_lo),
        kept,
        out_weight,
        resid,
        conv_p,
        head_p,
        chan_p,
        gain,
        seqs,
        heads,
    )

    residual_grad, gate_weight_grad, inner_weight_grad, bc_pieces, sums, glob = tail(
        (grad_hi, grad_lo),
        (hat_hi, hat_lo),
        (weight_hi, weight_lo),
        gate_half,
        (wide_sums, chan_sums, head_sums),
        resid,
        cot,
        gain,
        seqs,
        heads,
        chans,
    )
    across = width // bc_pieces.shape[2]
    bc_weight_grad = jnp.transpose(
        bc_pieces.reshape(2 * NSTATE // 8, across, 8, width // across), (1, 3, 0, 2)
    ).reshape(width, 2 * NSTATE)
    chan_at = full_lanes(chans + 2 * NSTATE)
    head_at = chan_at + full_lanes(chans)
    skip_wide = sums[1, 1, chan_at : chan_at + chans]
    return (
        result.reshape(residual_in.shape),
        residual_grad.reshape(residual_in.shape),
        glob[:4].reshape(width),
        gate_weight_grad,
        inner_weight_grad,
        bc_weight_grad,
        sums[0, :heads_here],
        sums[1, :WIDTH, :chans],
        sums[1, WIDTH, :chans],
        glob[8 : 8 + WIDTH, : 2 * NSTATE],
        glob[8 + WIDTH, : 2 * NSTATE],
        sums[1, 0, head_at : head_at + heads_here],
        sums[1, 1, head_at : head_at + heads_here],
        jnp.sum(skip_wide.reshape(heads_here, HEADDIM), axis=1),
        sums[1, 0, chan_at : chan_at + chans],
        out_weight_grad,
    )


def solution(mesh):
    placed = (
        P(None, ("seq", "head"), None),
        P(),
        P("head", None),
        P("head", None),
        P(),
        P("head", None),
        P(None, "head"),
        P("head"),
        P(),
        P(),
        P("head"),
        P("head"),
        P("head"),
        P("head"),
        P("head", None),
        P(None, ("seq", "head"), None),
    )
    return jax.shard_map(
        on_device,
        mesh=mesh,
        in_specs=placed,
        out_specs=(
            P(None, ("seq", "head"), None),
            P(None, ("seq", "head"), None),
            P(),
            P("head", None),
            P("head", None),
            P(),
            P("head", None),
            P(None, "head"),
            P("head"),
            P(),
            P(),
            P("head"),
            P("head"),
            P("head"),
            P("head"),
            P("head", None),
        ),
        check_vma=False,
    )
```
